512 devices in a mesh: grp: 2 (over y), gx: 16 (over z), gy: 8 (over x), gz: 2 (over core).
Axes of the slice: x: 8, y: 2, z: 16, core: 2. Of those that a mesh axis runs over, the one named last changes fastest.
The devices are a block of a 8x8x16 slice.
Arguments:
- design: int32 [64, 64, 256], P(('grp', 'gx'), 'gy', 'gz'), parts along dimension 0, may hold values from 0 to 15
- supports: int32 [64, 64, 256], P(('grp', 'gx'), 'gy', 'gz'), parts along dimension 0, may hold values 0 or 1
- body_load: float32 [12, 3, 32, 64, 256], P('grp', None, 'gx', 'gy', 'gz'), parts along dimension 0, may hold values from -6 to 6
- start: float32 [12, 3, 32, 64, 256], P('grp', None, 'gx', 'gy', 'gz'), parts along dimension 0, may hold values from -1.8 to 1.8
- load_nodes: int32 [12, 16], P('grp'), parts along dimension 0, may hold values from 0 to 524287
- load_values: float32 [12, 16, 3], P('grp'), parts along dimension 0, may hold values from -24 to 24
Outputs:
- solution: float32 [12, 3, 32, 64, 256], P('grp', None, 'gx', 'gy', 'gz'), parts along dimension 0
- residual: float32 [12, 3, 32, 64, 256], P('grp', None, 'gx', 'gy', 'gz'), parts along dimension 0
The draws below stay inside these ranges and needn't reach their ends.
There are 2 independent parts, one for each index of `grp`. The reference program is written for one: setup_inputs(seed, part) draws one part's arguments, and reference() takes and returns one part's arrays. A program takes and returns all parts, laid end to end along the dimension named above; each array names one. Nothing has to cross between parts.
Inputs may be any that keep to these rules, and one draw needn't show every extreme that they name: `supports`: 1 where all three displacements of the node are held fixed. `load_nodes`: flat index (i * 64 + j) * 256 + k of a loaded node; a node may be named several times.
All inputs are finite; a program needn't handle non-finite values. No bound on the sum of `supports` on one device may be relied on, other than what follows from the above.
Results may differ from the reference program's by a relative error of at most 0.0003.
Values sent between devices are 32-bit elements; how exact they have to be, the bound alone decides.
A program may use at most 64 MiB of HBM per device.

```python
import jax
import jax.numpy as jnp
import numpy as np
from jax import lax

CASES = 6
LOADS = 16
LEVELS = 16
ITERS = 2
NX = 32
NY = 64
NZ = 256


def plant(values, key, low, largest):
    place = [jax.random.randint(jax.random.fold_in(key, axis), (), 0, length) for axis, length in enumerate(values.shape)]
    main_axis = values.shape.index(max(values.shape))
    neighbour = place[:main_axis] + [(place[main_axis] + 1) % values.shape[main_axis]] + place[main_axis + 1:]
    return values.at[tuple(place)].set(low).at[tuple(neighbour)].set(largest)


def block_scale(own_key, shape, shards, smallest, top_value):
    gain = 1.0
    for dim, parts in shards:
        heights = jax.random.uniform(jax.random.fold_in(jax.random.fold_in(own_key, 6), dim), (parts,), jnp.float32, smallest / len(shards), top_value / len(shards))
        gain = gain * jnp.repeat(jnp.exp(heights), shape[dim] // parts).reshape((-1,) + (1,) * (len(shape) - 1 - dim))
    return gain


def centred(rng, shape, scale, reach, pieces=(), kind=jnp.bfloat16):
    result = jax.random.normal(rng, shape, jnp.float32) * scale
    if len(pieces) > 0:
        result = block_scale(rng, shape, pieces, -0.22, 0.18) * result
    return jnp.clip(result, min=-reach, max=reach).astype(kind)


def setup_inputs(seed: int = 0, part: int = 0) -> dict:
    key_of = jax.random.split(jax.random.key(seed), 7)
    part_keys = jax.random.split(jax.random.fold_in(key_of[6], part), 7)
    return {
        "design": plant(jax.random.randint(part_keys[0], (NX, NY, NZ), 0, LEVELS), jax.random.fold_in(part_keys[0], 1), 0, LEVELS - 1).astype(jnp.int32),
        "supports": plant((jax.random.randint(part_keys[1], (NX, NY, NZ), 0, 16) < 1).astype(jnp.int32), jax.random.fold_in(part_keys[1], 1), 0, 1),
        "body_load": centred(part_keys[2], (CASES, 3, NX, NY, NZ), 1.0, 6.0, ((2, 16), (3, 8), (4, 2)), jnp.float32),
        "start": centred(part_keys[3], (CASES, 3, NX, NY, NZ), 0.3, 1.8, ((2, 16), (3, 8), (4, 2)), jnp.float32),
        "load_nodes": plant(jax.random.randint(part_keys[4], (CASES, LOADS), 0, NX * NY * NZ), jax.random.fold_in(part_keys[4], 1), 0, (NX * NY * NZ) - 1).astype(jnp.int32),
        "load_values": centred(part_keys[5], (CASES, LOADS, 3), 4.0, 24.0, (), jnp.float32),
    }


soft_modulus = 0.05
poisson_ratio = 0.3
highest = lax.Precision.HIGHEST

def corner_list():
    return [(first, second, third) for first in (0, 1) for second in (0, 1) for third in (0, 1)]

def element_matrix():
    ratio = poisson_ratio
    lame_first = ratio / ((1.0 + ratio) * (1.0 - 2.0 * ratio))
    shear_modulus = 1.0 / (2.0 * (1.0 + ratio))
    elastic = np.zeros((6, 6))
    elastic[:3, :3] = lame_first
    for axis_dim in range(3):
        elastic[axis_dim, axis_dim] += 2.0 * shear_modulus
        elastic[3 + axis_dim, 3 + axis_dim] = shear_modulus
    gauss_points = [0.5 - 0.5 / np.sqrt(3.0), 0.5 + 0.5 / np.sqrt(3.0)]
    corners = corner_list()
    matrix_total = np.zeros((24, 24))
    for first_point in gauss_points:
        for second_point in gauss_points:
            for third_point in gauss_points:
                points = (first_point, second_point, third_point)
                strain = np.zeros((6, 24))
                for number, corner in enumerate(corners):
                    values = [points[axis_dim] if corner[axis_dim] else 1.0 - points[axis_dim] for axis_dim in range(3)]
                    slopes = [1.0 if corner[axis_dim] else -1.0 for axis_dim in range(3)]
                    grad_first = slopes[0] * values[1] * values[2]
                    grad_second = values[0] * slopes[1] * values[2]
                    grad_third = values[0] * values[1] * slopes[2]
                    column = 3 * number
                    strain[0, column] = grad_first
                    strain[1, column + 1] = grad_second
                    strain[2, column + 2] = grad_third
                    strain[3, column] = grad_second
                    strain[3, column + 1] = grad_first
                    strain[4, column + 1] = grad_third
                    strain[4, column + 2] = grad_second
                    strain[5, column] = grad_third
                    strain[5, column + 2] = grad_first
                matrix_total = matrix_total + strain.T @ elastic @ strain / 8.0
    return jnp.asarray(matrix_total, dtype=jnp.float32)

def stiffness_of(design):
    density = (design.astype(jnp.float32) + 1.0) / LEVELS
    return soft_modulus + (1.0 - soft_modulus) * density * density * density

def crop(array, width):
    return array[..., width:array.shape[-3] - width, width:array.shape[-2] - width, width:array.shape[-1] - width]

def pad_grid(array):
    widths = [(0, 0)] * (array.ndim - 3) + [(1, 1)] * 3
    return jnp.pad(array, widths)

def stiff_apply(padded, moduli, element_stiffness):
    span_first, span_second, span_third = padded.shape[-3:]
    corners = corner_list()
    results = []
    for member in range(padded.shape[0]):
        single = padded[member]
        stacked = jnp.concatenate([single[:, corner[0]:span_first - 1 + corner[0], corner[1]:span_second - 1 + corner[1], corner[2]:span_third - 1 + corner[2]] for corner in corners], axis=0)
        forces = jnp.einsum('ij,jxyz->ixyz', element_stiffness, stacked, precision=highest)
        forces = forces * moduli[None, :span_first - 1, :span_second - 1, :span_third - 1]
        accumulated = jnp.zeros((3, span_first - 2, span_second - 2, span_third - 2), jnp.float32)
        for number, corner in enumerate(corners):
            accumulated = accumulated + forces[3 * number:3 * number + 3, 1 - corner[0]:span_first - 1 - corner[0], 1 - corner[1]:span_second - 1 - corner[1], 1 - corner[2]:span_third - 1 - corner[2]]
        results.append(accumulated)
    return jnp.stack(results)

def operate(padded, moduli, movable_pad, element_stiffness):
    forces = stiff_apply(padded * movable_pad, moduli, element_stiffness)
    inner = crop(movable_pad, 1)
    return inner * forces + (1.0 - inner) * crop(padded, 1)

def inverse_diagonal(moduli, movable_inner, element_stiffness):
    span_first, span_second, span_third = moduli.shape
    adjacent = jnp.zeros((span_first - 2, span_second - 2, span_third - 2), jnp.float32)
    for corner in corner_list():
        adjacent = adjacent + moduli[1 - corner[0]:span_first - 1 - corner[0], 1 - corner[1]:span_second - 1 - corner[1], 1 - corner[2]:span_third - 1 - corner[2]]
    guarded = jnp.where(movable_inner > 0, adjacent, 1.0)
    return movable_inner / (element_stiffness[0, 0] * guarded) + (1.0 - movable_inner)

def gram_matrix(first, second):
    return jnp.einsum('iaxyz,jaxyz->ij', first, second, precision=highest)

def combine(fields, coeffs):
    return jnp.einsum('jaxyz,ji->iaxyz', fields, coeffs, precision=highest)

def small_solve(matrix, right):
    factor = jnp.linalg.cholesky(matrix)
    middle = lax.linalg.triangular_solve(factor, right, left_side=True, lower=True)
    return lax.linalg.triangular_solve(factor, middle, left_side=True, lower=True, transpose_a=True)

def add_points(plane, nodes, values):
    return plane.at[:, nodes].add(values.T)

def reference(design, supports, body_load, start, load_nodes, load_values):
    element_stiffness = element_matrix()
    stiffness = stiffness_of(design)
    movable = 1.0 - supports.astype(jnp.float32)
    moduli = pad_grid(stiffness)
    movable_pad = pad_grid(movable)
    flat = body_load.reshape(body_load.shape[0], 3, -1)
    loaded = jax.vmap(add_points)(flat, load_nodes, load_values).reshape(body_load.shape)
    loading = movable * loaded
    residual = loading - operate(pad_grid(start), moduli, movable_pad, element_stiffness)
    scaling = inverse_diagonal(moduli, movable, element_stiffness)
    direction = scaling * residual
    solution = start
    for turn_index in range(ITERS):
        applied = operate(pad_grid(direction), moduli, movable_pad, element_stiffness)
        curvature = gram_matrix(direction, applied)
        projection = gram_matrix(direction, residual)
        step_size = small_solve(curvature, projection)
        solution = solution + combine(direction, step_size)
        updated = residual - combine(applied, step_size)
        if turn_index + 1 < ITERS:
            scaled = scaling * updated
            coupling = gram_matrix(applied, scaled)
            direction = scaled + combine(direction, -small_solve(curvature, coupling))
        residual = updated
    return (solution, residual)
```

```python
import functools

import jax
import jax.numpy as jnp
from jax import lax
from jax.experimental import pallas as pl
from jax.experimental.pallas import tpu as pltpu
from jax.sharding import PartitionSpec as P

LEVELS = 16
CASES = 6
LOADS = 16
HALF = 3
soft_modulus = 0.05
poisson_ratio = 0.3
LAM = poisson_ratio / ((1.0 + poisson_ratio) * (1.0 - 2.0 * poisson_ratio))
MU = 1.0 / (2.0 * (1.0 + poisson_ratio))
C11 = LAM + 2.0 * MU
RHO = LAM / MU
KAP = C11 / MU + 1.0
K00 = (C11 + 2.0 * MU) / 9.0
MESH = pl.DeviceIdType.MESH
ANY = pl.ANY
f32 = jnp.float32


def masks():
    lane = lax.broadcasted_iota(jnp.int32, (8, 128), 1)
    sub = lax.broadcasted_iota(jnp.int32, (8, 128), 0)
    return lane, sub


def z_up(v, lane, sub):
    nd = v.ndim
    sh = pltpu.roll(v, 127, axis=nd - 1)
    fx = pltpu.roll(sh, 4, axis=nd - 2)
    return jnp.where(lane == 127, jnp.where(sub < 4, fx, 0.0), sh)


def z_dn(v, lane, sub):
    nd = v.ndim
    sh = pltpu.roll(v, 1, axis=nd - 1)
    fx = pltpu.roll(sh, 4, axis=nd - 2)
    return jnp.where(lane == 0, jnp.where(sub >= 4, fx, 0.0), sh)


def modal(a, em):
    X, Y, Z = 0, 1, 2
    g = {}
    tr = RHO * (a[X, 1, 0, 0] + a[Y, 0, 1, 0] + a[Z, 0, 0, 1])
    for key in ((X, 1, 0, 0), (Y, 0, 1, 0), (Z, 0, 0, 1)):
        g[key] = em * (a[key] + a[key] + tr)
    for p, q in (
        ((X, 0, 1, 0), (Y, 1, 0, 0)),
        ((X, 0, 0, 1), (Z, 1, 0, 0)),
        ((Y, 0, 0, 1), (Z, 0, 1, 0)),
    ):
        g[p] = g[q] = em * (a[p] + a[q])
    e2 = em * (1.0 / 3.0)
    ek = em * (KAP / 3.0)
    er = em * (RHO / 3.0)
    for p, q in (
        ((X, 1, 1, 0), (Z, 0, 1, 1)),
        ((X, 1, 0, 1), (Y, 0, 1, 1)),
        ((Y, 1, 1, 0), (Z, 1, 0, 1)),
    ):
        g[p] = ek * a[p] + er * a[q]
        g[q] = ek * a[q] + er * a[p]
    three = ((X, 0, 1, 1), (Y, 1, 0, 1), (Z, 1, 1, 0))
    total = a[three[0]] + a[three[1]] + a[three[2]]
    for key in three:
        g[key] = e2 * (a[key] + total)
    e3 = em * ((C11 / MU + 2.0) / 9.0)
    for c in range(3):
        g[c, 1, 1, 1] = e3 * a[c, 1, 1, 1]
    return g


def apply_k(node_row, em_row, emit, lane, sub):
    prev_z = None
    prev_hi = None
    for r in range(10):
        zs = []
        for c in range(3):
            v = node_row(c, r)
            w = z_up(v, lane, sub)
            zs.append((v + w, w - v))
        if r > 0:
            a = {}
            for c in range(3):
                for z in (0, 1):
                    lo, hi = prev_z[c][z], zs[c][z]
                    for y, f in ((0, lo + hi), (1, hi - lo)):
                        a[c, 1, y, z] = f[1:4] - f[0:3]
                        if y or z:
                            a[c, 0, y, z] = f[0:3] + f[1:4]
            g = modal(a, em_row(r - 1))
            lows, highs = [], []
            for c in range(3):
                h = {}
                for y in (0, 1):
                    for z in (0, 1):
                        gd = g[c, 1, y, z]
                        t = gd[0:2] - gd[1:3]
                        if y or z:
                            gs = g[c, 0, y, z]
                            t = t + (gs[0:2] + gs[1:3])
                        h[y, z] = t
                lows.append([h[0, z] - h[1, z] for z in (0, 1)])
                highs.append([h[0, z] + h[1, z] for z in (0, 1)])
            if r > 1:
                out = []
                for c in range(3):
                    ks = prev_hi[c][0] + lows[c][0]
                    kd = prev_hi[c][1] + lows[c][1]
                    out.append((ks - kd) + z_dn(ks + kd, lane, sub))
                emit(r - 2, out)
            prev_hi = highs
        prev_z = zs


def cyc1(v, sub):
    return jnp.where(sub % 4 == 2, pltpu.roll(v, 2, axis=v.ndim - 2), pltpu.roll(v, 7, axis=v.ndim - 2))


def cyc2(v, sub):
    return jnp.where(sub % 4 == 0, pltpu.roll(v, 6, axis=v.ndim - 2), pltpu.roll(v, 1, axis=v.ndim - 2))


def pair_products(own_x, other_x, own_y, sub):
    return [
        own_x * own_y,
        cyc1(own_x, sub) * own_y,
        other_x * own_y,
        cyc1(other_x, sub) * own_y,
        cyc2(other_x, sub) * own_y,
    ]


def cholesky(m, n):
    low = {}
    inv = {}
    for j in range(n):
        s = m[j, j]
        for k in range(j):
            s = s - low[j, k] * low[j, k]
        inv[j] = 1.0 / jnp.sqrt(s)
        for i in range(j + 1, n):
            t = m[i, j]
            for k in range(j):
                t = t - low[i, k] * low[j, k]
            low[i, j] = t * inv[j]
    return low, inv


def forward(low, inv, rhs, n):
    out = []
    for i in range(n):
        t = rhs[i]
        for k in range(i):
            t = t - low[i, k] * out[k]
        out.append(t * inv[i])
    return out


def backward(low, inv, rhs, n):
    out = [None] * n
    for i in reversed(range(n)):
        t = rhs[i]
        for k in range(i + 1, n):
            t = t - low[k, i] * out[k]
        out[i] = t * inv[i]
    return out


def kernel(
    nx, ny,
    nodes, vals, x_hbm, b_hbm, d_hbm, s_hbm,
    xo_hbm, ro_hbm,
    xin, bin_, din, sin, xm, ysend, esend, qs,
    nat, yrow, enat, ey, qnat,
    u0, u1, u2, em, mob, scl, rb, ib, yb, ga, ag, bg, xout, rout,
    in_sem, out_sem, ss, rs,
):
    grp, gx, gy, gz = (lax.axis_index(a) for a in ("grp", "gx", "gy", "gz"))
    oz = 1 - gz
    lane, sub = masks()
    valid = sub % 4 < 3
    counter = [0]
    pending = []

    loads = [
        pltpu.make_async_copy(src, dst, in_sem.at[i])
        for i, (src, dst) in enumerate(((d_hbm, din), (s_hbm, sin), (x_hbm, xin), (b_hbm, bin_)))
    ]
    for load in loads:
        load.start()

    barrier = pltpu.get_barrier_semaphore()

    def greet(cx, cy, cz):
        pl.semaphore_signal(barrier, inc=1, device_id=(grp, cx, cy, cz), device_id_type=MESH)

    exists = {}
    for dx in (-1, 0, 1):
        for dy in (-1, 0, 1):
            conds = []
            if dx:
                conds.append(gx > 0 if dx < 0 else gx < nx - 1)
            if dy:
                conds.append(gy > 0 if dy < 0 else gy < ny - 1)
            if conds:
                exists[dx, dy] = functools.reduce(jnp.logical_and, conds)

    greet(gx, gy, oz)
    for d in range(1, ny):
        for core in (0, 1):
            greet(gx, lax.rem(gy + d, ny), core)
    for d in range(1, nx):
        greet(lax.rem(gx + d, nx), gy, gz)
    expected = 1 + 2 * (ny - 1) + (nx - 1)
    extra = 0
    for (dx, dy), here in exists.items():
        cores = ()
        if dx and dy:
            cores = (0, 1)
        elif dx:
            cores = (oz,)
        if cores:

            @pl.when(here)
            def _(dx=dx, dy=dy, cores=cores):
                for core in cores:
                    greet(gx + dx, gy + dy, core)

            extra = extra + len(cores) * here.astype(jnp.int32)

    def clear(ref, *index):
        ref[index] = jnp.zeros(ref[index].shape, f32)

    full = slice(None)

    @pl.when(gx == 0)
    def _():
        clear(nat, pl.ds(0, 3))
        clear(enat, full, 0)
        clear(ey, full, 0)
        for side in (0, 4):
            clear(yrow, side)
        for u in (u1, u2):
            clear(u, full, 0)

    @pl.when(gx == nx - 1)
    def _():
        clear(nat, pl.ds(9, 3))
        for side in (0, 4):
            clear(yrow, side + 3)
        for u in (u1, u2):
            clear(u, full, 3)

    @pl.when(gy == 0)
    def _():
        clear(yrow, pl.ds(0, 4))
        clear(ey)
        for u in (u1, u2):
            clear(u, full, full, 0)

    @pl.when(gy == ny - 1)
    def _():
        clear(yrow, pl.ds(4, 4))
        for u in (u1, u2):
            clear(u, full, full, 9)

    loads[0].wait()
    loads[1].wait()
    mnat = []
    for p in range(2):
        density = (din[p].astype(f32) + 1.0) * (1.0 / LEVELS)
        modulus = soft_modulus + (1.0 - soft_modulus) * density * density * density
        movable = 1.0 - sin[p].astype(f32)
        esend[p] = modulus
        esend[2 + p] = movable
        enat[gz, 1 + p] = modulus
        enat[gz, 3 + p] = movable
        mnat.append(movable)
    loads[2].wait()
    for side in range(2):
        for core in range(2):
            for p in range(2):
                ysend[side, core, p, 8:16] = jnp.zeros((8, 128), f32)
    for case in range(CASES):
        core, k = divmod(case, HALF)
        for comp in range(3):
            for p in range(2):
                t = mnat[p] * xin[case, comp, p]
                xm[core, p * 3 + comp, 8 * k:8 * k + 8] = t
                for side, y in ((0, 0), (1, 7)):
                    ysend[side, core, p, 4 * k + comp:4 * k + comp + 1] = t[y:y + 1]

    pl.semaphore_wait(barrier, expected + extra)

    def view(ref, *index):
        return ref, index

    def descriptor(src, dst, send_index, recv_index, device):
        (a, i), (b, j) = src, dst
        return pltpu.make_async_remote_copy(
            src_ref=a.at[i] if i else a, dst_ref=b.at[j] if j else b,
            send_sem=ss.at[send_index], recv_sem=rs.at[recv_index],
            device_id=device, device_id_type=MESH,
        )

    slots = [0]

    def take(count):
        base = slots[0]
        slots[0] += count
        return base

    def guarded_by(cond, go):
        if cond is None:
            go()
        else:
            pl.when(cond)(go)

    def exchange(cond, items):
        def go():
            for src, dst, index, device in items:
                pending.append((cond, src, dst, counter[0], index, device))
                descriptor(src, dst, counter[0], index, device).start()
                counter[0] += 1

        guarded_by(cond, go)

    def wait_in(cond, ref, index):
        guarded_by(cond, lambda: descriptor(ref, ref, 0, index, partner).wait_recv())

    partner = (grp, gx, gy, oz)

    arrive = []
    half_rows = pl.ds(pl.multiple_of(32 * gz, 8), 24)
    half_16 = pl.ds(pl.multiple_of(16 * gz, 8), 16)
    for dx in (1, -1):
        base = take(2)
        p, slot = (1, 0) if dx > 0 else (0, 3)
        items = [
            (view(xm, core, pl.ds(3 * p, 3)), view(nat, pl.ds(3 * slot, 3), half_rows), base + gz, (grp, gx + dx, gy, core))
            for core in (0, 1)
        ]
        exchange(exists[dx, 0], items)
        for s in (0, 1):
            arrive.append((exists[-dx, 0], view(nat, pl.ds(3 * slot, 3), pl.ds(32 * s, 24)), base + s))
    for dy in (1, -1):
        side, there = (1, 0) if dy > 0 else (0, 1)
        base = take(2)
        items = [
            (view(ysend, side, core), view(yrow, pl.ds(4 * there + 1, 2), half_16), base + gz, (grp, gx, gy + dy, core))
            for core in (0, 1)
        ]
        exchange(exists[0, dy], items)
        for s in (0, 1):
            arrive.append((exists[0, -dy], view(yrow, pl.ds(4 * there + 1, 2), pl.ds(16 * s, 16)), base + s))
        for dx in (1, -1):
            p, slot = (1, 0) if dx > 0 else (0, 3)
            base = take(2)
            items = [
                (view(ysend, side, core, p), view(yrow, 4 * there + slot, half_16), base + gz, (grp, gx + dx, gy + dy, core))
                for core in (0, 1)
            ]
            exchange(exists[dx, dy], items)
            for s in (0, 1):
                arrive.append((exists[-dx, -dy], view(yrow, 4 * there + slot, pl.ds(16 * s, 16)), base + s))
    for (dx, dy), (src, dst) in (
        ((1, 0), ((1, 1), (0, 1))),
        ((0, 1), ((0, 2), (1, 2))),
        ((1, 1), ((1, 1), (0, 1))),
    ):
        base = take(2)
        target = enat if dy == 0 else ey
        items = [
            (view(esend, pl.ds(*src)), view(target, gz, pl.ds(*dst)), base + gz, (grp, gx + dx, gy + dy, core))
            for core in (0, 1)
        ]
        exchange(exists[dx, dy], items)
        for s in (0, 1):
            arrive.append((exists[-dx, -dy], view(target, s, pl.ds(*dst)), base + s))
    other_rows = pl.ds(pl.multiple_of(32 * oz, 8), 24)
    base = take(3)
    exchange(None, [
        (view(xm, oz), view(nat, pl.ds(3, 6), half_rows), base, partner),
        (view(esend), view(enat, gz, pl.ds(1, 4)), base + 1, partner),
    ])
    arrive.append((None, view(nat, pl.ds(3, 6), other_rows), base))
    arrive.append((None, view(enat, oz, pl.ds(1, 4)), base + 1))
    q_slot = base + 2

    loads[3].wait()
    across_z = 128 * 2
    across_y = 8 * ny * across_z
    number = (gy * 8 + sub) * across_z + gz * 128 + lane + (gx * 2) * across_y
    numbers = (number, number + across_y)

    def add_points(l, acc):
        acc = list(acc)
        for case in range(CASES):
            node = nodes[case, l]
            for p in range(2):
                hit = numbers[p] == node
                for comp in range(3):
                    at = (case * 2 + p) * 3 + comp
                    acc[at] = acc[at] + jnp.where(hit, vals[case, 3 * l + comp], 0.0)
        return tuple(acc)

    zero = jnp.zeros((8, 128), f32)
    points = lax.fori_loop(0, LOADS, add_points, (zero,) * (CASES * 6))
    for case in range(CASES):
        core, k = divmod(case, HALF)
        for p in range(2):
            m = mnat[p]
            for comp in range(3):
                total = bin_[case, comp, p] + points[(case * 2 + p) * 3 + comp]
                qs[core, p * 3 + comp, 8 * k:8 * k + 8] = m * total - (1.0 - m) * xin[case, comp, p]
    exchange(None, [(view(qs, oz), view(qnat, full, half_rows), q_slot, partner)])
    for k in range(6):
        nat[3 + k, half_rows] = xm[gz, k]
        qnat[k, half_rows] = qs[gz, k]

    for cond, ref, index in arrive:
        wait_in(cond, ref, index)

    low = sub < 4

    def spread(ref, k, y):
        return jnp.where(low, ref[0, k, y:y + 1], ref[1, k, y:y + 1])

    for j in range(9):
        for e in range(3):
            t = spread(ey, e, 7) if j == 0 else spread(enat, e, j - 1)
            em[j, e] = t * (MU / 16.0)
    for y in range(8):
        rows = em[y] + em[y + 1]
        around = rows[0:2] + rows[1:3]
        esum = (around + z_dn(around, lane, sub)) * (16.0 / MU)
        m = jnp.stack([spread(enat, 3, y), spread(enat, 4, y)])
        guarded = jnp.where(m > 0, esum, 1.0)
        mob[:, 8 * y:8 * y + 8] = m
        scl[:, 8 * y:8 * y + 8] = m / (K00 * guarded) + (1.0 - m)

    for r in range(10):
        for p in range(4):
            for comp in range(3):
                if r == 0:
                    t = yrow[p, pl.ds(comp, 8, stride=4), :]
                elif r == 9:
                    t = yrow[4 + p, pl.ds(comp, 8, stride=4), :]
                else:
                    t = nat[3 * p + comp, pl.ds(r - 1, 8, stride=8), :]
                u0[comp, p, r] = jnp.where(valid, t, 0.0)

    wait_in(None, view(qnat, full, other_rows), q_slot)

    def at(y):
        return pl.ds(8 * y, 8)

    def first(y, force):
        m = mob[:, at(y)]
        s = scl[:, at(y)]
        for comp in range(3):
            q = jnp.stack([qnat[3 * p + comp, pl.ds(y, 8, stride=8), :] for p in range(2)])
            res = jnp.where(valid, q, 0.0) - m * force[comp]
            rb[gz, comp, :, at(y)] = res
            u1[comp, 1:3, 1 + y] = m * (s * res)

    apply_k(lambda c, r: u0[c, :, r], lambda j: em[j], first, lane, sub)

    def swap_halos(u):
        got = []
        for dx in (1, -1):
            src, dst = (2, 0) if dx > 0 else (1, 3)
            base = take(1)
            inner = pl.ds(1, 8)
            exchange(exists[dx, 0], [(view(u, full, src, inner), view(u, full, dst, inner), base, (grp, gx + dx, gy, gz))])
            got.append((exists[-dx, 0], view(u, full, dst, inner), base))
        for dy in (1, -1):
            ysrc, ydst = (8, 0) if dy > 0 else (1, 9)
            base = take(1)
            both = pl.ds(1, 2)
            exchange(exists[0, dy], [(view(u, full, both, ysrc), view(u, full, both, ydst), base, (grp, gx, gy + dy, gz))])
            got.append((exists[0, -dy], view(u, full, both, ydst), base))
            for dx in (1, -1):
                src, dst = (2, 0) if dx > 0 else (1, 3)
                base = take(1)
                exchange(
                    exists[dx, dy],
                    [(view(u, full, src, ysrc), view(u, full, dst, ydst), base, (grp, gx + dx, gy + dy, gz))],
                )
                got.append((exists[-dx, -dy], view(u, full, dst, ydst), base))
        return got

    def share(buf):
        base = take(1)
        exchange(None, [(view(buf, gz), view(buf, gz), base, partner)])
        return (None, view(buf, oz), base)

    got1 = swap_halos(u1)
    got_r = share(rb)
    for item in got1:
        wait_in(*item)

    def second(y, force):
        m = mob[:, at(y)]
        s = scl[:, at(y)]
        for comp in range(3):
            d = s * rb[gz, comp, :, at(y)]
            image = m * force[comp] + (1.0 - m) * d
            ib[gz, comp, :, at(y)] = image
            u2[comp, 1:3, 1 + y] = m * (s * image)

    apply_k(lambda c, r: u1[c, :, r], lambda j: em[j], second, lane, sub)

    got2 = swap_halos(u2)
    got_i = share(ib)
    wait_in(*got_r)
    wait_in(*got_i)

    def grams(make):
        acc = None
        for y in range(8):
            s = scl[:, at(y)]
            for comp in range(3):
                prods = pair_products(*make(comp, y, s), sub)
                acc = prods if acc is None else [a + b for a, b in zip(acc, prods)]
        return [a[0] + a[1] for a in acc]

    def own_other(buf, comp, y):
        return buf[gz, comp, :, at(y)], buf[oz, comp, :, at(y)]

    def make_g(comp, y, s):
        r, ro = own_other(rb, comp, y)
        return s * r, s * ro, ib[gz, comp, :, at(y)]

    def make_h(comp, y, s):
        i, io = own_other(ib, comp, y)
        return i, io, s * i

    def make_p(comp, y, s):
        r, ro = own_other(rb, comp, y)
        return r, ro, s * r

    sums = grams(make_g) + grams(make_h) + grams(make_p)

    for item in got2:
        wait_in(*item)

    jacc = []

    def third(y, force):
        m = mob[:, at(y)]
        s = scl[:, at(y)]
        for comp in range(3):
            i, io = own_other(ib, comp, y)
            w = s * i
            image = m * force[comp] + (1.0 - m) * w
            yb[gz, comp, :, at(y)] = image
            prods = pair_products(w, s * io, image, sub)
            if jacc:
                jacc[0] = [a + b for a, b in zip(jacc[0], prods)]
            else:
                jacc.append(prods)

    apply_k(lambda c, r: u2[c, :, r], lambda j: em[j], third, lane, sub)
    got_y = share(yb)
    sums = sums + [a[0] + a[1] for a in jacc[0]]

    folded = [a + pltpu.roll(a, 4, axis=0) for a in sums]
    ga[pl.ds(80, 48), :] = jnp.zeros((48, 128), f32)
    for t in range(10):
        ga[pl.ds(8 * t, 8), :] = jnp.where(low, folded[2 * t], folded[2 * t + 1])
    row = lax.dot_general(
        jnp.ones((8, 128), f32), ga[...], (((1,), (1,)), ((), ())),
        precision=lax.Precision.HIGHEST, preferred_element_type=f32,
    )
    me = gz * ny + gy
    ag[me] = row[0:1]
    base = take(2 * ny)
    got = []
    for d in range(ny):
        for flip in (0, 1):
            if d == 0 and flip == 0:
                continue
            core = oz if flip else gz
            cy = lax.rem(gy + d, ny)
            index = base + 2 * d + flip
            exchange(None, [(view(ag, me), view(ag, me), index, (grp, gx, cy, core))])
            source = core * ny + lax.rem(gy + ny - d, ny)
            got.append((None, view(ag, source), index))
    for item in got:
        wait_in(*item)
    for s in (0, 1):
        total = ag[s * ny]
        for k in range(1, ny):
            total = total + ag[s * ny + k]
        bg[gx, s:s + 1] = total
    base = take(nx)
    got = []
    for d in range(1, nx):
        exchange(None, [(view(bg, gx), view(bg, gx), base + d, (grp, lax.rem(gx + d, nx), gy, gz))])
        got.append((None, view(bg, lax.rem(gx + nx - d, nx)), base + d))
    for item in got:
        wait_in(*item)
    total = bg[0]
    for k in range(1, nx):
        total = total + bg[k]

    rows = [jnp.broadcast_to(total[s:s + 1], (8, 128)) for s in (0, 1)]

    def entry(matrix, i, j):
        ci, ki = divmod(i, HALF)
        cj, kj = divmod(j, HALF)
        if ci == cj:
            if (ki + 1) % 3 == kj:
                acc, k, s = 1, ki, ci
            elif ki == kj:
                acc, k, s = 0, ki, ci
            else:
                acc, k, s = 1, kj, ci
        else:
            if ci == 1:
                ki, kj = kj, ki
            acc, k, s = 2 + (kj - ki) % 3, ki, 0
        number = matrix * 5 + acc
        where = 8 * (number // 2) + 4 * (number % 2) + k
        return jnp.broadcast_to(rows[s][:, where:where + 1], (8, 128))

    n = CASES
    mats = []
    for matrix in range(4):
        m = {}
        for i in range(n):
            for j in range(i + 1):
                m[i, j] = entry(matrix, i, j)
                m[j, i] = m[i, j]
        mats.append(m)
    mg, mh, mp, mj = mats

    lo1, inv1 = cholesky(mg, n)
    zh = [forward(lo1, inv1, [mh[i, j] for i in range(n)], n) for j in range(n)]
    zp = [forward(lo1, inv1, [mp[i, j] for i in range(n)], n) for j in range(n)]
    th = [backward(lo1, inv1, zh[j], n) for j in range(n)]
    al = [backward(lo1, inv1, zp[j], n) for j in range(n)]
    schur, right = {}, []
    for j in range(n):
        col = []
        for i in range(n):
            t = mg[i, j]
            for k in range(n):
                t = t - zh[i][k] * zp[j][k]
            col.append(t)
            if i >= j:
                t = mj[i, j]
                for k in range(n):
                    t = t - zh[i][k] * zh[j][k]
                schur[i, j] = t
        right.append(col)
    lo2, inv2 = cholesky(schur, n)
    cb = [backward(lo2, inv2, forward(lo2, inv2, right[j], n), n) for j in range(n)]
    ca = []
    for j in range(n):
        col = []
        for i in range(n):
            t = al[j][i]
            for k in range(n):
                t = t - th[k][i] * cb[j][k]
            col.append(t)
        ca.append(col)

    wait_in(*got_y)
    stores = []
    for comp in range(3):
        for p in range(2):
            s = scl[p, pl.ds(4 * gz, 8, stride=8), :]
            fr, fi, fy = [], [], []
            for j in range(n):
                core, k = divmod(j, HALF)
                pick = pl.ds(4 * gz + k, 8, stride=8)
                fr.append(rb[core, comp, p, pick, :])
                fi.append(ib[core, comp, p, pick, :])
                fy.append(yb[core, comp, p, pick, :])
            for i in range(n):
                up = fr[0] * ca[i][0] + fi[0] * cb[i][0]
                dn = fi[0] * ca[i][0] + fy[0] * cb[i][0]
                for j in range(1, n):
                    up = up + fr[j] * ca[i][j] + fi[j] * cb[i][j]
                    dn = dn + fi[j] * ca[i][j] + fy[j] * cb[i][j]
                xout[i, comp, p] = xin[i, comp, p] + s * up
                rout[i, comp, p] = fr[i] - dn
        for k, (src, dst) in enumerate(((xout, xo_hbm), (rout, ro_hbm))):
            c = pltpu.make_async_copy(src.at[:, comp], dst.at[:, comp], out_sem.at[2 * comp + k])
            c.start()
            stores.append(c)
    for cond, *copy in pending:
        guarded_by(cond, lambda: descriptor(*copy).wait_send())
    for c in stores:
        c.wait()


def shards(design, supports, body_load, start, load_nodes, load_values):
    nx, ny = lax.axis_size("gx"), lax.axis_size("gy")
    block = body_load.shape
    vmem = lambda *shape: pltpu.VMEM(shape, f32)
    spec = pl.BlockSpec(memory_space=ANY)
    smem = pl.BlockSpec(memory_space=pltpu.SMEM)
    scratch = [
        vmem(*block), vmem(*block), pltpu.VMEM(design.shape, jnp.int32), pltpu.VMEM(design.shape, jnp.int32),
        vmem(2, 6, 24, 128), vmem(2, 2, 2, 16, 128), vmem(4, 8, 128), vmem(2, 6, 24, 128),
        vmem(12, 64, 128), vmem(8, 32, 128), vmem(2, 5, 8, 128), vmem(2, 3, 8, 128), vmem(6, 64, 128),
        vmem(3, 4, 10, 8, 128), vmem(3, 4, 10, 8, 128), vmem(3, 4, 10, 8, 128),
        vmem(9, 3, 8, 128), vmem(2, 64, 128), vmem(2, 64, 128),
        vmem(2, 3, 2, 64, 128), vmem(2, 3, 2, 64, 128), vmem(2, 3, 2, 64, 128),
        vmem(128, 128), vmem(2 * ny, 1, 128), vmem(nx, 2, 128), vmem(*block), vmem(*block),
        pltpu.SemaphoreType.DMA((4,)), pltpu.SemaphoreType.DMA((6,)),
        pltpu.SemaphoreType.DMA((2 * ny + nx + 64,)), pltpu.SemaphoreType.DMA((2 * ny + nx + 64,)),
    ]
    out = jax.ShapeDtypeStruct(block, f32)
    return pl.pallas_call(
        functools.partial(kernel, nx, ny),
        out_shape=(out, out),
        in_specs=[smem, smem, spec, spec, spec, spec],
        out_specs=(spec, spec),
        scratch_shapes=scratch,
        compiler_params=pltpu.CompilerParams(collective_id=0, has_side_effects=True),
    )(load_nodes, load_values.reshape(CASES, 3 * LOADS), start, body_load, design, supports)


def solution(mesh):
    in_specs = (
        P(("grp", "gx"), "gy", "gz"),
        P(("grp", "gx"), "gy", "gz"),
        P("grp", None, "gx", "gy", "gz"),
        P("grp", None, "gx", "gy", "gz"),
        P("grp", None),
        P("grp", None, None),
    )
    out_specs = (P("grp", None, "gx", "gy", "gz"), P("grp", None, "gx", "gy", "gz"))
    return jax.shard_map(shards, mesh=mesh, in_specs=in_specs, out_specs=out_specs, check_vma=False)
```

```python
import functools

import jax
import jax.numpy as jnp
from jax import lax
from jax.experimental import pallas as pl
from jax.experimental.pallas import tpu as pltpu
from jax.sharding import PartitionSpec as P

LEVELS = 16
CASES = 6
LOADS = 16
HALF = 3
soft_modulus = 0.05
poisson_ratio = 0.3
LAM = poisson_ratio / ((1.0 + poisson_ratio) * (1.0 - 2.0 * poisson_ratio))
MU = 1.0 / (2.0 * (1.0 + poisson_ratio))
C11 = LAM + 2.0 * MU
RHO = LAM / MU
KAP = C11 / MU + 1.0
K00 = (C11 + 2.0 * MU) / 9.0
MESH = pl.DeviceIdType.MESH
f32 = jnp.float32


def masks():
    lane = lax.broadcasted_iota(jnp.int32, (8, 128), 1)
    sub = lax.broadcasted_iota(jnp.int32, (8, 128), 0)
    return lane, sub


def z_up(v, lane, sub):
    nd = v.ndim
    sh = pltpu.roll(v, 127, axis=nd - 1)
    fx = pltpu.roll(sh, 4, axis=nd - 2)
    return jnp.where(lane == 127, jnp.where(sub < 4, fx, 0.0), sh)


def z_dn(v, lane, sub):
    nd = v.ndim
    sh = pltpu.roll(v, 1, axis=nd - 1)
    fx = pltpu.roll(sh, 4, axis=nd - 2)
    return jnp.where(lane == 0, jnp.where(sub >= 4, fx, 0.0), sh)


def modal(a, em):
    X, Y, Z = 0, 1, 2
    g = {}
    tr = RHO * (a[X, 1, 0, 0] + a[Y, 0, 1, 0] + a[Z, 0, 0, 1])
    for key in ((X, 1, 0, 0), (Y, 0, 1, 0), (Z, 0, 0, 1)):
        g[key] = em * (a[key] + a[key] + tr)
    for p, q in (
        ((X, 0, 1, 0), (Y, 1, 0, 0)),
        ((X, 0, 0, 1), (Z, 1, 0, 0)),
        ((Y, 0, 0, 1), (Z, 0, 1, 0)),
    ):
        g[p] = g[q] = em * (a[p] + a[q])
    e2 = em * (1.0 / 3.0)
    ek = em * (KAP / 3.0)
    er = em * (RHO / 3.0)
    for p, q in (
        ((X, 1, 1, 0), (Z, 0, 1, 1)),
        ((X, 1, 0, 1), (Y, 0, 1, 1)),
        ((Y, 1, 1, 0), (Z, 1, 0, 1)),
    ):
        g[p] = ek * a[p] + er * a[q]
        g[q] = ek * a[q] + er * a[p]
    three = ((X, 0, 1, 1), (Y, 1, 0, 1), (Z, 1, 1, 0))
    total = a[three[0]] + a[three[1]] + a[three[2]]
    for key in three:
        g[key] = e2 * (a[key] + total)
    e3 = em * ((C11 / MU + 2.0) / 9.0)
    for c in range(3):
        g[c, 1, 1, 1] = e3 * a[c, 1, 1, 1]
    return g


def apply_k(node_row, em_row, emit, lane, sub):
    prev_z = None
    prev_hi = None
    for r in range(10):
        zs = []
        for c in range(3):
            v = node_row(c, r)
            w = z_up(v, lane, sub)
            zs.append((v + w, w - v))
        if r > 0:
            a = {}
            for c in range(3):
                for z in (0, 1):
                    lo, hi = prev_z[c][z], zs[c][z]
                    for y, f in ((0, lo + hi), (1, hi - lo)):
                        a[c, 1, y, z] = f[1:4] - f[0:3]
                        if y or z:
                            a[c, 0, y, z] = f[0:3] + f[1:4]
            g = modal(a, em_row(r - 1))
            lows, highs = [], []
            for c in range(3):
                h = {}
                for y in (0, 1):
                    for z in (0, 1):
                        gd = g[c, 1, y, z]
                        t = gd[0:2] - gd[1:3]
                        if y or z:
                            gs = g[c, 0, y, z]
                            t = t + (gs[0:2] + gs[1:3])
                        h[y, z] = t
                lows.append([h[0, z] - h[1, z] for z in (0, 1)])
                highs.append([h[0, z] + h[1, z] for z in (0, 1)])
            if r > 1:
                out = []
                for c in range(3):
                    ks = prev_hi[c][0] + lows[c][0]
                    kd = prev_hi[c][1] + lows[c][1]
                    out.append((ks - kd) + z_dn(ks + kd, lane, sub))
                emit(r - 2, out)
            prev_hi = highs
        prev_z = zs


def cyc1(v, sub):
    return jnp.where(sub % 4 == 2, pltpu.roll(v, 2, axis=v.ndim - 2), pltpu.roll(v, 7, axis=v.ndim - 2))


def cyc2(v, sub):
    return jnp.where(sub % 4 == 0, pltpu.roll(v, 6, axis=v.ndim - 2), pltpu.roll(v, 1, axis=v.ndim - 2))


def pair_products(own_x, other_x, own_y, sub):
    return [
        own_x * own_y,
        cyc1(own_x, sub) * own_y,
        other_x * own_y,
        cyc1(other_x, sub) * own_y,
        cyc2(other_x, sub) * own_y,
    ]


def cholesky(m, n):
    low = {}
    inv = {}
    for j in range(n):
        s = m[j, j]
        for k in range(j):
            s = s - low[j, k] * low[j, k]
        inv[j] = 1.0 / jnp.sqrt(s)
        for i in range(j + 1, n):
            t = m[i, j]
            for k in range(j):
                t = t - low[i, k] * low[j, k]
            low[i, j] = t * inv[j]
    return low, inv


def forward(low, inv, rhs, n):
    out = []
    for i in range(n):
        t = rhs[i]
        for k in range(i):
            t = t - low[i, k] * out[k]
        out.append(t * inv[i])
    return out


def backward(low, inv, rhs, n):
    out = [None] * n
    for i in reversed(range(n)):
        t = rhs[i]
        for k in range(i + 1, n):
            t = t - low[k, i] * out[k]
        out[i] = t * inv[i]
    return out


def kernel(
    nx, ny,
    n_hbm, v_hbm, x_hbm, b_hbm, d_hbm, s_hbm,
    xo_hbm, ro_hbm,
    xin, bin_, din, sin, xm, ysend, esend, qs,
    nat, yrow, enat, ey, qnat,
    u0, u1, u2, em, mob, scl, rb, ib, yb, ga, ag, bg, dummy, xout, rout, nodes, vals,
    in_sem, out_sem, ss, rs, heard,
):
    grp, gx, gy, gz = (lax.axis_index(a) for a in ("grp", "gx", "gy", "gz"))
    oz = 1 - gz
    lane, sub = masks()
    valid = sub % 4 < 3
    scope = [None]

    def mark(name):
        if scope[0] is not None:
            scope[0].__exit__(None, None, None)
        scope[0] = None
        if name is not None:
            scope[0] = jax.named_scope(name)
            scope[0].__enter__()

    mark('entry')

    loads = [
        pltpu.make_async_copy(src, dst, in_sem.at[i])
        for i, (src, dst) in enumerate(((d_hbm, din), (s_hbm, sin), (x_hbm, xin), (b_hbm, bin_), (n_hbm, nodes), (v_hbm, vals)))
    ]
    for load in loads:
        load.start()

    barrier = pltpu.get_barrier_semaphore()

    def greet(cx, cy, cz):
        pl.semaphore_signal(barrier, inc=1, device_id=(grp, cx, cy, cz), device_id_type=MESH)

    exists = {}
    for dx in (-1, 0, 1):
        for dy in (-1, 0, 1):
            conds = []
            if dx:
                conds.append(gx > 0 if dx < 0 else gx < nx - 1)
            if dy:
                conds.append(gy > 0 if dy < 0 else gy < ny - 1)
            if conds:
                exists[dx, dy] = functools.reduce(jnp.logical_and, conds)

    greet(gx, gy, oz)
    expected = 1
    for (dx, dy), here in exists.items():

        @pl.when(here)
        def _(dx=dx, dy=dy):
            for core in (0, 1):
                greet(gx + dx, gy + dy, core)

        expected = expected + 2 * here.astype(jnp.int32)

    def round_of(number):
        step = 2**number
        for size, mine, place in ((nx, gx, lambda c: (c, gy)), (ny, gy, lambda c: (gx, c))):
            if step < size:
                for d in (step, -step):
                    yield (mine + d < size if d > 0 else mine + d >= 0), place(mine + d)

    def tell(number):
        for here, (cx, cy) in round_of(number):

            @pl.when(here)
            def _(cx=cx, cy=cy):
                pl.semaphore_signal(heard.at[number], inc=1, device_id=(grp, cx, cy, gz), device_id_type=MESH)

    def hear(number):
        count = sum(here.astype(jnp.int32) for here, _ in round_of(number))
        pl.semaphore_wait(heard.at[number], count)

    def clear(ref, *index):
        ref[index] = jnp.zeros(ref[index].shape, f32)

    full = slice(None)

    @pl.when(gx == 0)
    def _():
        clear(nat, pl.ds(0, 3))
        clear(enat, full, 0)
        clear(ey, full, 0)
        for side in (0, 4):
            clear(yrow, side)
        for u in (u1, u2):
            clear(u, full, 0)

    @pl.when(gx == nx - 1)
    def _():
        clear(nat, pl.ds(9, 3))
        for side in (0, 4):
            clear(yrow, side + 3)
        for u in (u1, u2):
            clear(u, full, 3)

    @pl.when(gy == 0)
    def _():
        clear(yrow, pl.ds(0, 4))
        clear(ey)
        for u in (u1, u2):
            clear(u, full, full, 0)

    @pl.when(gy == ny - 1)
    def _():
        clear(yrow, pl.ds(4, 4))
        for u in (u1, u2):
            clear(u, full, full, 9)

    mark('prep')
    loads[0].wait()
    loads[1].wait()
    mnat = []
    for p in range(2):
        density = (din[p].astype(f32) + 1.0) * (1.0 / LEVELS)
        modulus = soft_modulus + (1.0 - soft_modulus) * density * density * density
        movable = 1.0 - sin[p].astype(f32)
        esend[p] = modulus
        esend[2 + p] = movable
        enat[gz, 1 + p] = modulus
        enat[gz, 3 + p] = movable
        mnat.append(movable)
    loads[2].wait()
    for side in range(2):
        for core in range(2):
            for p in range(2):
                ysend[side, core, p, 8:16] = jnp.zeros((8, 128), f32)
    for case in range(CASES):
        core, k = divmod(case, HALF)
        for comp in range(3):
            for p in range(2):
                t = mnat[p] * xin[case, comp, p]
                xm[core, p * 3 + comp, 8 * k:8 * k + 8] = t
                for side, y in ((0, 0), (1, 7)):
                    ysend[side, core, p, 4 * k + comp:4 * k + comp + 1] = t[y:y + 1]

    mark('barrier')
    pl.semaphore_wait(barrier, expected)
    tell(0)
    mark('send1')

    def view(ref, *index):
        return ref, index

    def descriptor(src, dst, send_index, recv_index, device):
        (a, i), (b, j) = src, dst
        return pltpu.make_async_remote_copy(
            src_ref=a.at[i] if i else a, dst_ref=b.at[j] if j else b,
            send_sem=ss.at[send_index], recv_sem=rs.at[recv_index],
            device_id=device, device_id_type=MESH,
        )

    def guarded_by(cond, go):
        if cond is None:
            go()
        else:
            pl.when(cond)(go)

    def exchange(cond, send_index, recv_index, items):
        def go():
            for src, dst, device in items:
                descriptor(src, dst, send_index, recv_index, device).start()

        guarded_by(cond, go)

    def wait_in(cond, index, ref):
        guarded_by(cond, lambda: descriptor(ref, ref, 0, index, partner).wait_recv())

    def wait_out(cond, index, ref):
        guarded_by(cond, lambda: descriptor(ref, ref, index, 0, partner).wait_send())

    def rows_of(count):
        return view(dummy, pl.ds(0, count))

    slot = {key: i for i, key in enumerate(exists)}
    partner = (grp, gx, gy, oz)

    half_rows = pl.ds(pl.multiple_of(32 * gz, 8), 24)
    half_16 = pl.ds(pl.multiple_of(16 * gz, 8), 16)
    other_rows = pl.ds(pl.multiple_of(32 * oz, 8), 24)
    bytes1 = {}
    for key in sorted(exists, key=lambda k: abs(k[1])):
        dx, dy = key
        items, count = [], 0
        p, there_p = (1, 0) if dx > 0 else (0, 3)
        side, there = (1, 0) if dy > 0 else (0, 1)
        for core in (0, 1):
            device = (grp, gx + dx, gy + dy, core)
            if dy == 0:
                items.append((view(xm, core, pl.ds(3 * p, 3)), view(nat, pl.ds(3 * there_p, 3), half_rows), device))
                count += 72
                if dx > 0:
                    items.append((view(esend, pl.ds(1, 1)), view(enat, gz, pl.ds(0, 1)), device))
                    count += 8
            elif dx == 0:
                items.append((view(ysend, side, core), view(yrow, pl.ds(4 * there + 1, 2), half_16), device))
                count += 32
                if dy > 0:
                    items.append((view(esend, pl.ds(0, 2)), view(ey, gz, pl.ds(1, 2)), device))
                    count += 16
            else:
                items.append((view(ysend, side, core, p), view(yrow, 4 * there + there_p, half_16), device))
                count += 16
                if dx > 0 and dy > 0:
                    items.append((view(esend, pl.ds(1, 1)), view(ey, gz, pl.ds(0, 1)), device))
                    count += 8
        exchange(exists[key], slot[key], slot[key], items)
        bytes1[key] = count
    exchange(None, 8, 16, [
        (view(xm, oz), view(nat, pl.ds(3, 6), half_rows), partner),
        (view(esend), view(enat, gz, pl.ds(1, 4)), partner),
    ])

    mark('points')
    for load in loads[3:]:
        load.wait()
    across_z = 128 * 2
    across_y = 8 * ny * across_z
    number = (gy * 8 + sub) * across_z + gz * 128 + lane + (gx * 2) * across_y
    numbers = (number, number + across_y)

    def add_points(l, acc):
        acc = list(acc)
        for case in range(CASES):
            node = nodes[case, l]
            for p in range(2):
                hit = numbers[p] == node
                for comp in range(3):
                    at = (case * 2 + p) * 3 + comp
                    acc[at] = acc[at] + jnp.where(hit, vals[case, comp, l], 0.0)
        return tuple(acc)

    zero = jnp.zeros((8, 128), f32)
    points = lax.fori_loop(0, LOADS, add_points, (zero,) * (CASES * 6))
    for case in range(CASES):
        core, k = divmod(case, HALF)
        for p in range(2):
            m = mnat[p]
            for comp in range(3):
                total = bin_[case, comp, p] + points[(case * 2 + p) * 3 + comp]
                qs[core, p * 3 + comp, 8 * k:8 * k + 8] = m * total - (1.0 - m) * xin[case, comp, p]
    exchange(None, 9, 17, [(view(qs, oz), view(qnat, full, half_rows), partner)])
    for k in range(6):
        nat[3 + k, half_rows] = xm[gz, k]
        qnat[k, half_rows] = qs[gz, k]

    hear(0)
    tell(1)
    mark('wait1')
    for (dx, dy), index in slot.items():
        wait_in(exists[-dx, -dy], index, rows_of(bytes1[dx, dy]))
    wait_in(None, 16, rows_of(176))
    hear(1)
    tell(2)
    mark('build')

    low = sub < 4

    def spread(ref, k, y):
        return jnp.where(low, ref[0, k, y:y + 1], ref[1, k, y:y + 1])

    for j in range(9):
        for e in range(3):
            t = spread(ey, e, 7) if j == 0 else spread(enat, e, j - 1)
            em[j, e] = t * (MU / 16.0)
    for y in range(8):
        rows = em[y] + em[y + 1]
        around = rows[0:2] + rows[1:3]
        esum = (around + z_dn(around, lane, sub)) * (16.0 / MU)
        m = jnp.stack([spread(enat, 3, y), spread(enat, 4, y)])
        guarded = jnp.where(m > 0, esum, 1.0)
        mob[:, 8 * y:8 * y + 8] = m
        scl[:, 8 * y:8 * y + 8] = m / (K00 * guarded) + (1.0 - m)

    for r in range(10):
        for p in range(4):
            for comp in range(3):
                if r == 0:
                    t = yrow[p, pl.ds(comp, 8, stride=4), :]
                elif r == 9:
                    t = yrow[4 + p, pl.ds(comp, 8, stride=4), :]
                else:
                    t = nat[3 * p + comp, pl.ds(r - 1, 8, stride=8), :]
                u0[comp, p, r] = jnp.where(valid, t, 0.0)

    mark('waitq')
    wait_in(None, 17, view(qnat, full, other_rows))
    mark('k1')

    def at(y):
        return pl.ds(8 * y, 8)

    def first(y, force):
        m = mob[:, at(y)]
        s = scl[:, at(y)]
        for comp in range(3):
            q = jnp.stack([qnat[3 * p + comp, pl.ds(y, 8, stride=8), :] for p in range(2)])
            res = jnp.where(valid, q, 0.0) - m * force[comp]
            rb[gz, comp, :, at(y)] = res
            u1[comp, 1:3, 1 + y] = m * (s * res)

    apply_k(lambda c, r: u0[c, :, r], lambda j: em[j], first, lane, sub)

    def halo_views(u, key):
        dx, dy = key
        src, dst = (2, 0) if dx > 0 else (1, 3)
        ysrc, ydst = (8, 0) if dy > 0 else (1, 9)
        if dy == 0:
            return view(u, full, src, pl.ds(1, 8)), view(u, full, dst, pl.ds(1, 8))
        if dx == 0:
            return view(u, full, pl.ds(1, 2), ysrc), view(u, full, pl.ds(1, 2), ydst)
        return view(u, full, src, ysrc), view(u, full, dst, ydst)

    def swap_halos(u, first_slot):
        for key in sorted(exists, key=lambda k: abs(k[1])):
            dx, dy = key
            exchange(
                exists[key], slot[key], first_slot + slot[key],
                [(*halo_views(u, key), (grp, gx + dx, gy + dy, gz))],
            )

    def take_halos(u, first_slot):
        for dx, dy in exists:
            wait_in(exists[-dx, -dy], first_slot + slot[dx, dy], halo_views(u, (dx, dy))[1])

    def sent_halos(u):
        for key in exists:
            wait_out(exists[key], slot[key], halo_views(u, key)[0])

    def share(buf, send_index, recv_index):
        exchange(None, send_index, recv_index, [(view(buf, gz), view(buf, gz), partner)])

    for key in exists:
        wait_out(exists[key], slot[key], rows_of(bytes1[key]))
    wait_out(None, 8, rows_of(176))
    swap_halos(u1, 8)
    share(rb, 8, 18)
    mark('wait2')
    take_halos(u1, 8)
    hear(2)
    tell(3)
    mark('k2')

    def second(y, force):
        m = mob[:, at(y)]
        s = scl[:, at(y)]
        for comp in range(3):
            d = s * rb[gz, comp, :, at(y)]
            image = m * force[comp] + (1.0 - m) * d
            ib[gz, comp, :, at(y)] = image
            u2[comp, 1:3, 1 + y] = m * (s * image)

    apply_k(lambda c, r: u1[c, :, r], lambda j: em[j], second, lane, sub)

    mark('send3')
    sent_halos(u1)
    wait_out(None, 9, view(qs, oz))
    swap_halos(u2, 0)
    share(ib, 9, 19)
    wait_in(None, 18, view(rb, oz))
    wait_in(None, 19, view(ib, oz))

    mark('grams')
    def grams(make):
        acc = None
        for y in range(8):
            s = scl[:, at(y)]
            for comp in range(3):
                prods = pair_products(*make(comp, y, s), sub)
                acc = prods if acc is None else [a + b for a, b in zip(acc, prods)]
        return [a[0] + a[1] for a in acc]

    def own_other(buf, comp, y):
        return buf[gz, comp, :, at(y)], buf[oz, comp, :, at(y)]

    def make_g(comp, y, s):
        r, ro = own_other(rb, comp, y)
        return s * r, s * ro, ib[gz, comp, :, at(y)]

    def make_h(comp, y, s):
        i, io = own_other(ib, comp, y)
        return i, io, s * i

    def make_p(comp, y, s):
        r, ro = own_other(rb, comp, y)
        return r, ro, s * r

    sums = grams(make_g) + grams(make_h) + grams(make_p)

    mark('wait3')
    take_halos(u2, 0)
    mark('k3')

    jacc = []

    def third(y, force):
        m = mob[:, at(y)]
        s = scl[:, at(y)]
        for comp in range(3):
            i, io = own_other(ib, comp, y)
            w = s * i
            image = m * force[comp] + (1.0 - m) * w
            yb[gz, comp, :, at(y)] = image
            prods = pair_products(w, s * io, image, sub)
            if jacc:
                jacc[0] = [a + b for a, b in zip(jacc[0], prods)]
            else:
                jacc.append(prods)

    apply_k(lambda c, r: u2[c, :, r], lambda j: em[j], third, lane, sub)
    wait_out(None, 8, view(rb, gz))
    share(yb, 8, 20)
    sums = sums + [a[0] + a[1] for a in jacc[0]]

    mark('rowsum')
    folded = [a + pltpu.roll(a, 4, axis=0) for a in sums]
    ga[pl.ds(80, 48), :] = jnp.zeros((48, 128), f32)
    for t in range(10):
        ga[pl.ds(8 * t, 8), :] = jnp.where(low, folded[2 * t], folded[2 * t + 1])
    row = lax.dot_general(
        jnp.ones((8, 128), f32), ga[...], (((1,), (1,)), ((), ())),
        precision=lax.Precision.HIGHEST, preferred_element_type=f32,
    )
    mark('reduce_a')
    me = gz * ny + gy
    ag[me] = row[0:1]
    exchange(None, 10, 21, [
        (view(ag, me), view(ag, me), (grp, gx, lax.rem(gy + d, ny), oz if flip else gz))
        for d in range(ny) for flip in (0, 1) if d or flip
    ])
    wait_in(None, 21, view(ag, pl.ds(0, 2 * ny - 1)))
    for s in (0, 1):
        total = ag[s * ny]
        for k in range(1, ny):
            total = total + ag[s * ny + k]
        bg[gx, s:s + 1] = total
    hear(3)
    mark('reduce_b')
    exchange(None, 11, 22, [
        (view(bg, gx), view(bg, gx), (grp, lax.rem(gx + d, nx), gy, gz)) for d in range(1, nx)
    ])
    wait_in(None, 22, view(bg, pl.ds(0, nx - 1)))
    mark('solve')
    total = bg[0]
    for k in range(1, nx):
        total = total + bg[k]

    rows = [jnp.broadcast_to(total[s:s + 1], (8, 128)) for s in (0, 1)]

    def entry(matrix, i, j):
        ci, ki = divmod(i, HALF)
        cj, kj = divmod(j, HALF)
        if ci == cj:
            if (ki + 1) % 3 == kj:
                acc, k, s = 1, ki, ci
            elif ki == kj:
                acc, k, s = 0, ki, ci
            else:
                acc, k, s = 1, kj, ci
        else:
            if ci == 1:
                ki, kj = kj, ki
            acc, k, s = 2 + (kj - ki) % 3, ki, 0
        number = matrix * 5 + acc
        where = 8 * (number // 2) + 4 * (number % 2) + k
        return jnp.broadcast_to(rows[s][:, where:where + 1], (8, 128))

    n = CASES
    mats = []
    for matrix in range(4):
        m = {}
        for i in range(n):
            for j in range(i + 1):
                m[i, j] = entry(matrix, i, j)
                m[j, i] = m[i, j]
        mats.append(m)
    mg, mh, mp, mj = mats

    lo1, inv1 = cholesky(mg, n)
    zh = [forward(lo1, inv1, [mh[i, j] for i in range(n)], n) for j in range(n)]
    zp = [forward(lo1, inv1, [mp[i, j] for i in range(n)], n) for j in range(n)]
    th = [backward(lo1, inv1, zh[j], n) for j in range(n)]
    al = [backward(lo1, inv1, zp[j], n) for j in range(n)]
    schur, right = {}, []
    for j in range(n):
        col = []
        for i in range(n):
            t = mg[i, j]
            for k in range(n):
                t = t - zh[i][k] * zp[j][k]
            col.append(t)
            if i >= j:
                t = mj[i, j]
                for k in range(n):
                    t = t - zh[i][k] * zh[j][k]
                schur[i, j] = t
        right.append(col)
    lo2, inv2 = cholesky(schur, n)
    cb = [backward(lo2, inv2, forward(lo2, inv2, right[j], n), n) for j in range(n)]
    ca = []
    for j in range(n):
        col = []
        for i in range(n):
            t = al[j][i]
            for k in range(n):
                t = t - th[k][i] * cb[j][k]
            col.append(t)
        ca.append(col)

    mark('combine')
    wait_in(None, 20, view(yb, oz))
    for comp in range(3):
        for p in range(2):
            s = scl[p, pl.ds(4 * gz, 8, stride=8), :]
            fr, fi, fy = [], [], []
            for j in range(n):
                core, k = divmod(j, HALF)
                pick = pl.ds(4 * gz + k, 8, stride=8)
                fr.append(rb[core, comp, p, pick, :])
                fi.append(ib[core, comp, p, pick, :])
                fy.append(yb[core, comp, p, pick, :])
            for i in range(n):
                up = fr[0] * ca[i][0] + fi[0] * cb[i][0]
                dn = fi[0] * ca[i][0] + fy[0] * cb[i][0]
                for j in range(1, n):
                    up = up + fr[j] * ca[i][j] + fi[j] * cb[i][j]
                    dn = dn + fi[j] * ca[i][j] + fy[j] * cb[i][j]
                xout[i, comp, p] = xin[i, comp, p] + s * up
                rout[i, comp, p] = fr[i] - dn
        for i, (src, dst) in enumerate(((xout, xo_hbm), (rout, ro_hbm))):
            pltpu.make_async_copy(src.at[:, comp], dst.at[:, comp], out_sem.at[i]).start()
    mark('drain')
    sent_halos(u2)
    wait_out(None, 8, view(yb, gz))
    wait_out(None, 9, view(ib, gz))
    wait_out(None, 10, view(ag, pl.ds(0, 2 * ny - 1)))
    wait_out(None, 11, view(bg, pl.ds(0, nx - 1)))
    for i, (src, dst) in enumerate(((xout, xo_hbm), (rout, ro_hbm))):
        pltpu.make_async_copy(src, dst, out_sem.at[i]).wait()
    mark(None)


def shards(design, supports, body_load, start, load_nodes, load_values):
    nx, ny = lax.axis_size("gx"), lax.axis_size("gy")
    block = body_load.shape
    vmem = lambda *shape: pltpu.VMEM(shape, f32)
    spec = pl.BlockSpec(memory_space=pl.ANY)
    scratch = [
        vmem(*block), vmem(*block), pltpu.VMEM(design.shape, jnp.int32), pltpu.VMEM(design.shape, jnp.int32),
        vmem(2, 6, 24, 128), vmem(2, 2, 2, 16, 128), vmem(4, 8, 128), vmem(2, 6, 24, 128),
        vmem(12, 64, 128), vmem(8, 32, 128), vmem(2, 5, 8, 128), vmem(2, 3, 8, 128), vmem(6, 64, 128),
        vmem(3, 4, 10, 8, 128), vmem(3, 4, 10, 8, 128), vmem(3, 4, 10, 8, 128),
        vmem(9, 3, 8, 128), vmem(2, 64, 128), vmem(2, 64, 128),
        vmem(2, 3, 2, 64, 128), vmem(2, 3, 2, 64, 128), vmem(2, 3, 2, 64, 128),
        vmem(128, 128), vmem(2 * ny, 1, 128), vmem(nx, 2, 128), vmem(176, 128), vmem(*block), vmem(*block),
        pltpu.SMEM(load_nodes.shape, jnp.int32), pltpu.SMEM((CASES, 3, LOADS), f32),
        pltpu.SemaphoreType.DMA((6,)), pltpu.SemaphoreType.DMA((2,)), pltpu.SemaphoreType.DMA((12,)), pltpu.SemaphoreType.DMA((23,)),
        pltpu.SemaphoreType.REGULAR((4,)),
    ]
    out = jax.ShapeDtypeStruct(block, f32)
    return pl.pallas_call(
        functools.partial(kernel, nx, ny),
        out_shape=(out, out),
        in_specs=[spec] * 6,
        out_specs=(spec, spec),
        scratch_shapes=scratch,
        compiler_params=pltpu.CompilerParams(collective_id=0, has_side_effects=True),
    )(load_nodes, jnp.transpose(load_values, (0, 2, 1)), start, body_load, design, supports)


def solution(mesh):
    in_specs = (
        P(("grp", "gx"), "gy", "gz"),
        P(("grp", "gx"), "gy", "gz"),
        P("grp", None, "gx", "gy", "gz"),
        P("grp", None, "gx", "gy", "gz"),
        P("grp", None),
        P("grp", None, None),
    )
    out_specs = (P("grp", None, "gx", "gy", "gz"), P("grp", None, "gx", "gy", "gz"))
    return jax.shard_map(shards, mesh=mesh, in_specs=in_specs, out_specs=out_specs, check_vma=False)
```

```python
import functools

import jax
import jax.numpy as jnp
from jax import lax
from jax.experimental import pallas as pl
from jax.experimental.pallas import tpu as pltpu
from jax.sharding import PartitionSpec as P

LEVELS = 16
CASES = 6
LOADS = 16
HALF = 3
soft_modulus = 0.05
poisson_ratio = 0.3
LAM = poisson_ratio / ((1.0 + poisson_ratio) * (1.0 - 2.0 * poisson_ratio))
MU = 1.0 / (2.0 * (1.0 + poisson_ratio))
C11 = LAM + 2.0 * MU
RHO = LAM / MU
KAP = C11 / MU + 1.0
K00 = (C11 + 2.0 * MU) / 9.0
MESH = pl.DeviceIdType.MESH
f32 = jnp.float32


def masks():
    lane = lax.broadcasted_iota(jnp.int32, (8, 128), 1)
    sub = lax.broadcasted_iota(jnp.int32, (8, 128), 0)
    return lane, sub


def z_up(v, lane, sub):
    nd = v.ndim
    sh = pltpu.roll(v, 127, axis=nd - 1)
    fx = pltpu.roll(sh, 4, axis=nd - 2)
    return jnp.where(lane == 127, jnp.where(sub < 4, fx, 0.0), sh)


def z_dn(v, lane, sub):
    nd = v.ndim
    sh = pltpu.roll(v, 1, axis=nd - 1)
    fx = pltpu.roll(sh, 4, axis=nd - 2)
    return jnp.where(lane == 0, jnp.where(sub >= 4, fx, 0.0), sh)


def modal(a, em):
    X, Y, Z = 0, 1, 2
    g = {}
    tr = RHO * (a[X, 1, 0, 0] + a[Y, 0, 1, 0] + a[Z, 0, 0, 1])
    for key in ((X, 1, 0, 0), (Y, 0, 1, 0), (Z, 0, 0, 1)):
        g[key] = em * (a[key] + a[key] + tr)
    for p, q in (
        ((X, 0, 1, 0), (Y, 1, 0, 0)),
        ((X, 0, 0, 1), (Z, 1, 0, 0)),
        ((Y, 0, 0, 1), (Z, 0, 1, 0)),
    ):
        g[p] = g[q] = em * (a[p] + a[q])
    e2 = em * (1.0 / 3.0)
    ek = em * (KAP / 3.0)
    er = em * (RHO / 3.0)
    for p, q in (
        ((X, 1, 1, 0), (Z, 0, 1, 1)),
        ((X, 1, 0, 1), (Y, 0, 1, 1)),
        ((Y, 1, 1, 0), (Z, 1, 0, 1)),
    ):
        g[p] = ek * a[p] + er * a[q]
        g[q] = ek * a[q] + er * a[p]
    three = ((X, 0, 1, 1), (Y, 1, 0, 1), (Z, 1, 1, 0))
    total = a[three[0]] + a[three[1]] + a[three[2]]
    for key in three:
        g[key] = e2 * (a[key] + total)
    e3 = em * ((C11 / MU + 2.0) / 9.0)
    for c in range(3):
        g[c, 1, 1, 1] = e3 * a[c, 1, 1, 1]
    return g


def apply_k(node_row, em_row, emit, lane, sub):
    prev_z = None
    prev_hi = None
    for r in range(10):
        zs = []
        for c in range(3):
            v = node_row(c, r)
            w = z_up(v, lane, sub)
            zs.append((v + w, w - v))
        if r > 0:
            a = {}
            for c in range(3):
                for z in (0, 1):
                    lo, hi = prev_z[c][z], zs[c][z]
                    for y, f in ((0, lo + hi), (1, hi - lo)):
                        a[c, 1, y, z] = f[1:4] - f[0:3]
                        if y or z:
                            a[c, 0, y, z] = f[0:3] + f[1:4]
            g = modal(a, em_row(r - 1))
            lows, highs = [], []
            for c in range(3):
                h = {}
                for y in (0, 1):
                    for z in (0, 1):
                        gd = g[c, 1, y, z]
                        t = gd[0:2] - gd[1:3]
                        if y or z:
                            gs = g[c, 0, y, z]
                            t = t + (gs[0:2] + gs[1:3])
                        h[y, z] = t
                lows.append([h[0, z] - h[1, z] for z in (0, 1)])
                highs.append([h[0, z] + h[1, z] for z in (0, 1)])
            if r > 1:
                out = []
                for c in range(3):
                    ks = prev_hi[c][0] + lows[c][0]
                    kd = prev_hi[c][1] + lows[c][1]
                    out.append((ks - kd) + z_dn(ks + kd, lane, sub))
                emit(r - 2, out)
            prev_hi = highs
        prev_z = zs


def cyc1(v, sub):
    return jnp.where(sub % 4 == 2, pltpu.roll(v, 2, axis=v.ndim - 2), pltpu.roll(v, 7, axis=v.ndim - 2))


def cyc2(v, sub):
    return jnp.where(sub % 4 == 0, pltpu.roll(v, 6, axis=v.ndim - 2), pltpu.roll(v, 1, axis=v.ndim - 2))


def pair_products(own_x, other_x, own_y, sub):
    return [
        own_x * own_y,
        cyc1(own_x, sub) * own_y,
        other_x * own_y,
        cyc1(other_x, sub) * own_y,
        cyc2(other_x, sub) * own_y,
    ]


def cholesky(m, n):
    low = {}
    inv = {}
    for j in range(n):
        s = m[j, j]
        for k in range(j):
            s = s - low[j, k] * low[j, k]
        inv[j] = 1.0 / jnp.sqrt(s)
        for i in range(j + 1, n):
            t = m[i, j]
            for k in range(j):
                t = t - low[i, k] * low[j, k]
            low[i, j] = t * inv[j]
    return low, inv


def forward(low, inv, rhs, n):
    out = []
    for i in range(n):
        t = rhs[i]
        for k in range(i):
            t = t - low[i, k] * out[k]
        out.append(t * inv[i])
    return out


def backward(low, inv, rhs, n):
    out = [None] * n
    for i in reversed(range(n)):
        t = rhs[i]
        for k in range(i + 1, n):
            t = t - low[k, i] * out[k]
        out[i] = t * inv[i]
    return out


def kernel(
    nx, ny,
    n_hbm, v_hbm, x_hbm, b_hbm, d_hbm, s_hbm,
    xo_hbm, ro_hbm,
    xin, bin_, din, sin, xm, ysend, esend, qs,
    nat, yrow, enat, ey, qnat,
    u0, u1, u2, em, mob, scl, rb, ib, yb, ga, ag, bg, dummy, xout, rout, nodes, vals,
    in_sem, out_sem, ss, rs, heard,
):
    grp, gx, gy, gz = (lax.axis_index(a) for a in ("grp", "gx", "gy", "gz"))
    oz = 1 - gz
    lane, sub = masks()
    valid = sub % 4 < 3
    scope = [None]

    def mark(name):
        if scope[0] is not None:
            scope[0].__exit__(None, None, None)
        scope[0] = None
        if name is not None:
            scope[0] = jax.named_scope(name)
            scope[0].__enter__()

    mark('entry')

    loads = [
        pltpu.make_async_copy(src, dst, in_sem.at[i])
        for i, (src, dst) in enumerate(((d_hbm, din), (s_hbm, sin), (x_hbm, xin), (b_hbm, bin_), (n_hbm, nodes), (v_hbm, vals)))
    ]
    for load in loads:
        load.start()

    barrier = pltpu.get_barrier_semaphore()

    def greet(cx, cy, cz):
        pl.semaphore_signal(barrier, inc=1, device_id=(grp, cx, cy, cz), device_id_type=MESH)

    exists = {}
    for dx in (-1, 0, 1):
        for dy in (-1, 0, 1):
            conds = []
            if dx:
                conds.append(gx > 0 if dx < 0 else gx < nx - 1)
            if dy:
                conds.append(gy > 0 if dy < 0 else gy < ny - 1)
            if conds:
                exists[dx, dy] = functools.reduce(jnp.logical_and, conds)

    greet(gx, gy, oz)
    expected = 1
    for (dx, dy), here in exists.items():

        @pl.when(here)
        def _(dx=dx, dy=dy):
            for core in (0, 1):
                greet(gx + dx, gy + dy, core)

        expected = expected + 2 * here.astype(jnp.int32)

    def round_of(number):
        step = 2**number
        for size, mine, place in ((nx, gx, lambda c: (c, gy)), (ny, gy, lambda c: (gx, c))):
            if step < size:
                for d in (step, -step):
                    yield (mine + d < size if d > 0 else mine + d >= 0), place(mine + d)

    def tell(number):
        for here, (cx, cy) in round_of(number):

            @pl.when(here)
            def _(cx=cx, cy=cy):
                pl.semaphore_signal(heard.at[number], inc=1, device_id=(grp, cx, cy, gz), device_id_type=MESH)

    def hear(number):
        count = sum(here.astype(jnp.int32) for here, _ in round_of(number))
        pl.semaphore_wait(heard.at[number], count)

    def clear(ref, *index):
        ref[index] = jnp.zeros(ref[index].shape, f32)

    full = slice(None)

    @pl.when(gx == 0)
    def _():
        clear(nat, pl.ds(0, 3))
        clear(enat, full, 0)
        clear(ey, full, 0)
        for side in (0, 4):
            clear(yrow, side)
        for u in (u1, u2):
            clear(u, full, 0)

    @pl.when(gx == nx - 1)
    def _():
        clear(nat, pl.ds(9, 3))
        for side in (0, 4):
            clear(yrow, side + 3)
        for u in (u1, u2):
            clear(u, full, 3)

    @pl.when(gy == 0)
    def _():
        clear(yrow, pl.ds(0, 4))
        clear(ey)
        for u in (u1, u2):
            clear(u, full, full, 0)

    @pl.when(gy == ny - 1)
    def _():
        clear(yrow, pl.ds(4, 4))
        for u in (u1, u2):
            clear(u, full, full, 9)

    mark('prep')
    loads[0].wait()
    loads[1].wait()
    mnat = []
    for p in range(2):
        density = (din[p].astype(f32) + 1.0) * (1.0 / LEVELS)
        modulus = soft_modulus + (1.0 - soft_modulus) * density * density * density
        movable = 1.0 - sin[p].astype(f32)
        esend[p] = modulus
        esend[2 + p] = movable
        enat[gz, 1 + p] = modulus
        enat[gz, 3 + p] = movable
        mnat.append(movable)
    loads[2].wait()
    for side in range(2):
        for core in range(2):
            for p in range(2):
                ysend[side, core, p, 8:16] = jnp.zeros((8, 128), f32)
    for case in range(CASES):
        core, k = divmod(case, HALF)
        for comp in range(3):
            for p in range(2):
                t = mnat[p] * xin[case, comp, p]
                xm[core, p * 3 + comp, 8 * k:8 * k + 8] = t
                for side, y in ((0, 0), (1, 7)):
                    ysend[side, core, p, 4 * k + comp:4 * k + comp + 1] = t[y:y + 1]

    mark('barrier')
    pl.semaphore_wait(barrier, expected)
    tell(0)
    mark('send1')

    def view(ref, *index):
        return ref, index

    def descriptor(src, dst, send_index, recv_index, device):
        (a, i), (b, j) = src, dst
        return pltpu.make_async_remote_copy(
            src_ref=a.at[i] if i else a, dst_ref=b.at[j] if j else b,
            send_sem=ss.at[send_index], recv_sem=rs.at[recv_index],
            device_id=device, device_id_type=MESH,
        )

    def guarded_by(cond, go):
        if cond is None:
            go()
        else:
            pl.when(cond)(go)

    def exchange(cond, send_index, recv_index, items):
        def go():
            for src, dst, device in items:
                descriptor(src, dst, send_index, recv_index, device).start()

        guarded_by(cond, go)

    def wait_in(cond, index, ref):
        guarded_by(cond, lambda: descriptor(ref, ref, 0, index, partner).wait_recv())

    def wait_out(cond, index, ref):
        guarded_by(cond, lambda: descriptor(ref, ref, index, 0, partner).wait_send())

    def rows_of(count):
        return view(dummy, pl.ds(0, count))

    slot = {key: i for i, key in enumerate(exists)}
    partner = (grp, gx, gy, oz)

    half_rows = pl.ds(pl.multiple_of(32 * gz, 8), 24)
    half_16 = pl.ds(pl.multiple_of(16 * gz, 8), 16)
    other_rows = pl.ds(pl.multiple_of(32 * oz, 8), 24)
    bytes1 = {}
    for key in sorted(exists, key=lambda k: (k[1] == 0, -abs(k[0]))):
        dx, dy = key
        items, count = [], 0
        p, there_p = (1, 0) if dx > 0 else (0, 3)
        side, there = (1, 0) if dy > 0 else (0, 1)
        for core in (0, 1):
            device = (grp, gx + dx, gy + dy, core)
            if dy == 0:
                items.append((view(xm, core, pl.ds(3 * p, 3)), view(nat, pl.ds(3 * there_p, 3), half_rows), device))
                count += 72
                if dx > 0:
                    items.append((view(esend, pl.ds(1, 1)), view(enat, gz, pl.ds(0, 1)), device))
                    count += 8
            elif dx == 0:
                items.append((view(ysend, side, core), view(yrow, pl.ds(4 * there + 1, 2), half_16), device))
                count += 32
                if dy > 0:
                    items.append((view(esend, pl.ds(0, 2)), view(ey, gz, pl.ds(1, 2)), device))
                    count += 16
            else:
                items.append((view(ysend, side, core, p), view(yrow, 4 * there + there_p, half_16), device))
                count += 16
                if dx > 0 and dy > 0:
                    items.append((view(esend, pl.ds(1, 1)), view(ey, gz, pl.ds(0, 1)), device))
                    count += 8
        exchange(exists[key], slot[key], slot[key], items)
        bytes1[key] = count
    exchange(None, 8, 16, [
        (view(xm, oz), view(nat, pl.ds(3, 6), half_rows), partner),
        (view(esend), view(enat, gz, pl.ds(1, 4)), partner),
    ])

    mark('points')
    for load in loads[3:]:
        load.wait()
    across_z = 128 * 2
    across_y = 8 * ny * across_z
    number = (gy * 8 + sub) * across_z + gz * 128 + lane + (gx * 2) * across_y
    numbers = (number, number + across_y)

    def add_points(l, acc):
        acc = list(acc)
        for case in range(CASES):
            node = nodes[case, l]
            for p in range(2):
                hit = numbers[p] == node
                for comp in range(3):
                    at = (case * 2 + p) * 3 + comp
                    acc[at] = acc[at] + jnp.where(hit, vals[case, comp, l], 0.0)
        return tuple(acc)

    zero = jnp.zeros((8, 128), f32)
    points = lax.fori_loop(0, LOADS, add_points, (zero,) * (CASES * 6))
    for case in range(CASES):
        core, k = divmod(case, HALF)
        for p in range(2):
            m = mnat[p]
            for comp in range(3):
                total = bin_[case, comp, p] + points[(case * 2 + p) * 3 + comp]
                qs[core, p * 3 + comp, 8 * k:8 * k + 8] = m * total - (1.0 - m) * xin[case, comp, p]
    exchange(None, 9, 17, [(view(qs, oz), view(qnat, full, half_rows), partner)])
    for k in range(6):
        nat[3 + k, half_rows] = xm[gz, k]
        qnat[k, half_rows] = qs[gz, k]

    hear(0)
    tell(1)
    mark('wait1')
    for (dx, dy), index in slot.items():
        wait_in(exists[-dx, -dy], index, rows_of(bytes1[dx, dy]))
    wait_in(None, 16, rows_of(176))
    hear(1)
    tell(2)
    mark('build')

    low = sub < 4

    def spread(ref, k, y):
        return jnp.where(low, ref[0, k, y:y + 1], ref[1, k, y:y + 1])

    for j in range(9):
        for e in range(3):
            t = spread(ey, e, 7) if j == 0 else spread(enat, e, j - 1)
            em[j, e] = t * (MU / 16.0)
    for y in range(8):
        rows = em[y] + em[y + 1]
        around = rows[0:2] + rows[1:3]
        esum = (around + z_dn(around, lane, sub)) * (16.0 / MU)
        m = jnp.stack([spread(enat, 3, y), spread(enat, 4, y)])
        guarded = jnp.where(m > 0, esum, 1.0)
        mob[:, 8 * y:8 * y + 8] = m
        scl[:, 8 * y:8 * y + 8] = m / (K00 * guarded) + (1.0 - m)

    for r in range(10):
        for p in range(4):
            for comp in range(3):
                if r == 0:
                    t = yrow[p, pl.ds(comp, 8, stride=4), :]
                elif r == 9:
                    t = yrow[4 + p, pl.ds(comp, 8, stride=4), :]
                else:
                    t = nat[3 * p + comp, pl.ds(r - 1, 8, stride=8), :]
                u0[comp, p, r] = jnp.where(valid, t, 0.0)

    mark('waitq')
    wait_in(None, 17, view(qnat, full, other_rows))
    mark('k1')

    def at(y):
        return pl.ds(8 * y, 8)

    def first(y, force):
        m = mob[:, at(y)]
        s = scl[:, at(y)]
        for comp in range(3):
            q = jnp.stack([qnat[3 * p + comp, pl.ds(y, 8, stride=8), :] for p in range(2)])
            res = jnp.where(valid, q, 0.0) - m * force[comp]
            rb[gz, comp, :, at(y)] = res
            u1[comp, 1:3, 1 + y] = m * (s * res)

    apply_k(lambda c, r: u0[c, :, r], lambda j: em[j], first, lane, sub)

    def halo_views(u, key):
        dx, dy = key
        src, dst = (2, 0) if dx > 0 else (1, 3)
        ysrc, ydst = (8, 0) if dy > 0 else (1, 9)
        if dy == 0:
            return [(view(u, full, src, pl.ds(k, 3)), view(u, full, dst, pl.ds(k, 3))) for k in (1, 5)]
        if dx == 0:
            return [(view(u, full, pl.ds(1, 2), ysrc), view(u, full, pl.ds(1, 2), ydst))]
        return [(view(u, full, src, ysrc), view(u, full, dst, ydst))]

    halo_rows = {(dx, dy): 8 * 3 * (6 if dy == 0 else 2 if dx == 0 else 1) for dx, dy in exists}

    free = sub % 4 == 3

    def pack(u):
        for k in (0, 4):
            t = u[:, 1:3, k + 4]
            for i in (1, 2, 3):
                u[:, 1:3, k + i] = jnp.where(free, pltpu.roll(t, 4 - i, axis=2), u[:, 1:3, k + i])

    def unpack(u):
        for p in (0, 3):
            for k in (0, 4):
                a, b, c = (pltpu.roll(u[:, p, k + i], 4 + i, axis=1) for i in (1, 2, 3))
                u[:, p, k + 4] = jnp.where(sub % 4 == 0, a, jnp.where(sub % 4 == 1, b, c))

    def swap_halos(u, first_slot):
        pack(u)
        for key in sorted(exists, key=lambda k: (k[1] == 0, -abs(k[0]))):
            dx, dy = key
            exchange(
                exists[key], slot[key], first_slot + slot[key],
                [(a, b, (grp, gx + dx, gy + dy, gz)) for a, b in halo_views(u, key)],
            )

    def take_halos(u, first_slot):
        for dx, dy in exists:
            wait_in(exists[-dx, -dy], first_slot + slot[dx, dy], rows_of(halo_rows[dx, dy]))
        unpack(u)

    def sent_halos(u):
        for key in exists:
            wait_out(exists[key], slot[key], rows_of(halo_rows[key]))

    def share(buf, send_index, recv_index):
        exchange(None, send_index, recv_index, [(view(buf, gz), view(buf, gz), partner)])

    for key in exists:
        wait_out(exists[key], slot[key], rows_of(bytes1[key]))
    wait_out(None, 8, rows_of(176))
    swap_halos(u1, 8)
    share(rb, 8, 18)
    mark('wait2')
    take_halos(u1, 8)
    hear(2)
    tell(3)
    mark('k2')

    def second(y, force):
        m = mob[:, at(y)]
        s = scl[:, at(y)]
        for comp in range(3):
            d = s * rb[gz, comp, :, at(y)]
            image = m * force[comp] + (1.0 - m) * d
            ib[gz, comp, :, at(y)] = image
            u2[comp, 1:3, 1 + y] = m * (s * image)

    apply_k(lambda c, r: u1[c, :, r], lambda j: em[j], second, lane, sub)

    mark('send3')
    sent_halos(u1)
    wait_out(None, 9, view(qs, oz))
    swap_halos(u2, 0)
    share(ib, 9, 19)
    wait_in(None, 18, view(rb, oz))
    wait_in(None, 19, view(ib, oz))

    mark('grams')
    def grams(make):
        acc = None
        for y in range(8):
            s = scl[:, at(y)]
            for comp in range(3):
                prods = pair_products(*make(comp, y, s), sub)
                acc = prods if acc is None else [a + b for a, b in zip(acc, prods)]
        return [a[0] + a[1] for a in acc]

    def own_other(buf, comp, y):
        return buf[gz, comp, :, at(y)], buf[oz, comp, :, at(y)]

    def make_g(comp, y, s):
        r, ro = own_other(rb, comp, y)
        return s * r, s * ro, ib[gz, comp, :, at(y)]

    def make_h(comp, y, s):
        i, io = own_other(ib, comp, y)
        return i, io, s * i

    def make_p(comp, y, s):
        r, ro = own_other(rb, comp, y)
        return r, ro, s * r

    sums = grams(make_g) + grams(make_h) + grams(make_p)

    mark('wait3')
    take_halos(u2, 0)
    mark('k3')

    jacc = []

    def third(y, force):
        m = mob[:, at(y)]
        s = scl[:, at(y)]
        for comp in range(3):
            i, io = own_other(ib, comp, y)
            w = s * i
            image = m * force[comp] + (1.0 - m) * w
            yb[gz, comp, :, at(y)] = image
            prods = pair_products(w, s * io, image, sub)
            if jacc:
                jacc[0] = [a + b for a, b in zip(jacc[0], prods)]
            else:
                jacc.append(prods)

    apply_k(lambda c, r: u2[c, :, r], lambda j: em[j], third, lane, sub)
    wait_out(None, 8, view(rb, gz))
    share(yb, 8, 20)
    sums = sums + [a[0] + a[1] for a in jacc[0]]

    mark('rowsum')
    folded = [a + pltpu.roll(a, 4, axis=0) for a in sums]
    ga[pl.ds(80, 48), :] = jnp.zeros((48, 128), f32)
    for t in range(10):
        ga[pl.ds(8 * t, 8), :] = jnp.where(low, folded[2 * t], folded[2 * t + 1])
    row = lax.dot_general(
        jnp.ones((8, 128), f32), ga[...], (((1,), (1,)), ((), ())),
        precision=lax.Precision.HIGHEST, preferred_element_type=f32,
    )
    mark('reduce_a')
    me = gz * ny + gy
    ag[me] = row[0:1]
    exchange(None, 10, 21, [
        (view(ag, me), view(ag, me), (grp, gx, lax.rem(gy + d, ny), oz if flip else gz))
        for d in range(ny) for flip in (0, 1) if d or flip
    ])
    wait_in(None, 21, view(ag, pl.ds(0, 2 * ny - 1)))
    for s in (0, 1):
        total = ag[s * ny]
        for k in range(1, ny):
            total = total + ag[s * ny + k]
        bg[gx, s:s + 1] = total
    hear(3)
    mark('reduce_b')
    exchange(None, 11, 22, [
        (view(bg, gx), view(bg, gx), (grp, lax.rem(gx + d, nx), gy, gz)) for d in range(1, nx)
    ])
    wait_in(None, 22, view(bg, pl.ds(0, nx - 1)))
    mark('solve')
    total = bg[0]
    for k in range(1, nx):
        total = total + bg[k]

    rows = [jnp.broadcast_to(total[s:s + 1], (8, 128)) for s in (0, 1)]

    def entry(matrix, i, j):
        ci, ki = divmod(i, HALF)
        cj, kj = divmod(j, HALF)
        if ci == cj:
            if (ki + 1) % 3 == kj:
                acc, k, s = 1, ki, ci
            elif ki == kj:
                acc, k, s = 0, ki, ci
            else:
                acc, k, s = 1, kj, ci
        else:
            if ci == 1:
                ki, kj = kj, ki
            acc, k, s = 2 + (kj - ki) % 3, ki, 0
        number = matrix * 5 + acc
        where = 8 * (number // 2) + 4 * (number % 2) + k
        return jnp.broadcast_to(rows[s][:, where:where + 1], (8, 128))

    n = CASES
    mats = []
    for matrix in range(4):
        m = {}
        for i in range(n):
            for j in range(i + 1):
                m[i, j] = entry(matrix, i, j)
                m[j, i] = m[i, j]
        mats.append(m)
    mg, mh, mp, mj = mats

    lo1, inv1 = cholesky(mg, n)
    zh = [forward(lo1, inv1, [mh[i, j] for i in range(n)], n) for j in range(n)]
    zp = [forward(lo1, inv1, [mp[i, j] for i in range(n)], n) for j in range(n)]
    th = [backward(lo1, inv1, zh[j], n) for j in range(n)]
    al = [backward(lo1, inv1, zp[j], n) for j in range(n)]
    schur, right = {}, []
    for j in range(n):
        col = []
        for i in range(n):
            t = mg[i, j]
            for k in range(n):
                t = t - zh[i][k] * zp[j][k]
            col.append(t)
            if i >= j:
                t = mj[i, j]
                for k in range(n):
                    t = t - zh[i][k] * zh[j][k]
                schur[i, j] = t
        right.append(col)
    lo2, inv2 = cholesky(schur, n)
    cb = [backward(lo2, inv2, forward(lo2, inv2, right[j], n), n) for j in range(n)]
    ca = []
    for j in range(n):
        col = []
        for i in range(n):
            t = al[j][i]
            for k in range(n):
                t = t - th[k][i] * cb[j][k]
            col.append(t)
        ca.append(col)

    mark('combine')
    wait_in(None, 20, view(yb, oz))
    for comp in range(3):
        for p in range(2):
            s = scl[p, pl.ds(4 * gz, 8, stride=8), :]
            fr, fi, fy = [], [], []
            for j in range(n):
                core, k = divmod(j, HALF)
                pick = pl.ds(4 * gz + k, 8, stride=8)
                fr.append(rb[core, comp, p, pick, :])
                fi.append(ib[core, comp, p, pick, :])
                fy.append(yb[core, comp, p, pick, :])
            for i in range(n):
                up = fr[0] * ca[i][0] + fi[0] * cb[i][0]
                dn = fi[0] * ca[i][0] + fy[0] * cb[i][0]
                for j in range(1, n):
                    up = up + fr[j] * ca[i][j] + fi[j] * cb[i][j]
                    dn = dn + fi[j] * ca[i][j] + fy[j] * cb[i][j]
                xout[i, comp, p] = s * up
                rout[i, comp, p] = (fr[i] - dn) + xin[i, comp, p]
        for i, (src, dst) in enumerate(((xout, xo_hbm), (rout, ro_hbm))):
            pltpu.make_async_copy(src.at[:, comp], dst.at[:, comp], out_sem.at[i]).start()
    mark('drain')
    sent_halos(u2)
    wait_out(None, 8, view(yb, gz))
    wait_out(None, 9, view(ib, gz))
    wait_out(None, 10, view(ag, pl.ds(0, 2 * ny - 1)))
    wait_out(None, 11, view(bg, pl.ds(0, nx - 1)))
    for i, (src, dst) in enumerate(((xout, xo_hbm), (rout, ro_hbm))):
        pltpu.make_async_copy(src, dst, out_sem.at[i]).wait()
    mark(None)


def shards(design, supports, body_load, start, load_nodes, load_values):
    nx, ny = lax.axis_size("gx"), lax.axis_size("gy")
    block = body_load.shape
    vmem = lambda *shape: pltpu.VMEM(shape, f32)
    spec = pl.BlockSpec(memory_space=pl.ANY)
    scratch = [
        vmem(*block), vmem(*block), pltpu.VMEM(design.shape, jnp.int32), pltpu.VMEM(design.shape, jnp.int32),
        vmem(2, 6, 24, 128), vmem(2, 2, 2, 16, 128), vmem(4, 8, 128), vmem(2, 6, 24, 128),
        vmem(12, 64, 128), vmem(8, 32, 128), vmem(2, 5, 8, 128), vmem(2, 3, 8, 128), vmem(6, 64, 128),
        vmem(3, 4, 10, 8, 128), vmem(3, 4, 10, 8, 128), vmem(3, 4, 10, 8, 128),
        vmem(9, 3, 8, 128), vmem(2, 64, 128), vmem(2, 64, 128),
        vmem(2, 3, 2, 64, 128), vmem(2, 3, 2, 64, 128), vmem(2, 3, 2, 64, 128),
        vmem(128, 128), vmem(2 * ny, 1, 128), vmem(nx, 2, 128), vmem(176, 128), vmem(*block), vmem(*block),
        pltpu.SMEM(load_nodes.shape, jnp.int32), pltpu.SMEM((CASES, 3, LOADS), f32),
        pltpu.SemaphoreType.DMA((6,)), pltpu.SemaphoreType.DMA((2,)), pltpu.SemaphoreType.DMA((12,)), pltpu.SemaphoreType.DMA((23,)),
        pltpu.SemaphoreType.REGULAR((4,)),
    ]
    out = jax.ShapeDtypeStruct(block, f32)
    change, shifted = pl.pallas_call(
        functools.partial(kernel, nx, ny),
        out_shape=(out, out),
        in_specs=[spec] * 6,
        out_specs=(spec, spec),
        scratch_shapes=scratch,
        compiler_params=pltpu.CompilerParams(collective_id=0, has_side_effects=True),
    )(load_nodes, jnp.transpose(load_values, (0, 2, 1)), start, body_load, design, supports)

    return start + change, shifted - start


def solution(mesh):
    in_specs = (
        P(("grp", "gx"), "gy", "gz"),
        P(("grp", "gx"), "gy", "gz"),
        P("grp", None, "gx", "gy", "gz"),
        P("grp", None, "gx", "gy", "gz"),
        P("grp", None),
        P("grp", None, None),
    )
    out_specs = (P("grp", None, "gx", "gy", "gz"), P("grp", None, "gx", "gy", "gz"))
    return jax.shard_map(shards, mesh=mesh, in_specs=in_specs, out_specs=out_specs, check_vma=False)
```

```python
import functools

import jax
import jax.numpy as jnp
from jax import lax
from jax.experimental import pallas as pl
from jax.experimental.pallas import tpu as pltpu
from jax.sharding import PartitionSpec as P

LEVELS = 16
CASES = 6
LOADS = 16
HALF = 3
soft_modulus = 0.05
poisson_ratio = 0.3
LAM = poisson_ratio / ((1.0 + poisson_ratio) * (1.0 - 2.0 * poisson_ratio))
MU = 1.0 / (2.0 * (1.0 + poisson_ratio))
C11 = LAM + 2.0 * MU
RHO = LAM / MU
KAP = C11 / MU + 1.0
K00 = (C11 + 2.0 * MU) / 9.0
MESH = pl.DeviceIdType.MESH
f32 = jnp.float32


def masks():
    lane = lax.broadcasted_iota(jnp.int32, (8, 128), 1)
    sub = lax.broadcasted_iota(jnp.int32, (8, 128), 0)
    return lane, sub


def z_up(v, lane, sub):
    nd = v.ndim
    sh = pltpu.roll(v, 127, axis=nd - 1)
    fx = pltpu.roll(sh, 4, axis=nd - 2)
    return jnp.where(lane == 127, jnp.where(sub < 4, fx, 0.0), sh)


def z_dn(v, lane, sub):
    nd = v.ndim
    sh = pltpu.roll(v, 1, axis=nd - 1)
    fx = pltpu.roll(sh, 4, axis=nd - 2)
    return jnp.where(lane == 0, jnp.where(sub >= 4, fx, 0.0), sh)


def modal(a, em):
    X, Y, Z = 0, 1, 2
    g = {}
    tr = RHO * (a[X, 1, 0, 0] + a[Y, 0, 1, 0] + a[Z, 0, 0, 1])
    for key in ((X, 1, 0, 0), (Y, 0, 1, 0), (Z, 0, 0, 1)):
        g[key] = em * (a[key] + a[key] + tr)
    for p, q in (
        ((X, 0, 1, 0), (Y, 1, 0, 0)),
        ((X, 0, 0, 1), (Z, 1, 0, 0)),
        ((Y, 0, 0, 1), (Z, 0, 1, 0)),
    ):
        g[p] = g[q] = em * (a[p] + a[q])
    e2 = em * (1.0 / 3.0)
    ek = em * (KAP / 3.0)
    er = em * (RHO / 3.0)
    for p, q in (
        ((X, 1, 1, 0), (Z, 0, 1, 1)),
        ((X, 1, 0, 1), (Y, 0, 1, 1)),
        ((Y, 1, 1, 0), (Z, 1, 0, 1)),
    ):
        g[p] = ek * a[p] + er * a[q]
        g[q] = ek * a[q] + er * a[p]
    three = ((X, 0, 1, 1), (Y, 1, 0, 1), (Z, 1, 1, 0))
    total = a[three[0]] + a[three[1]] + a[three[2]]
    for key in three:
        g[key] = e2 * (a[key] + total)
    e3 = em * ((C11 / MU + 2.0) / 9.0)
    for c in range(3):
        g[c, 1, 1, 1] = e3 * a[c, 1, 1, 1]
    return g


def apply_k(node_row, em_row, emit, lane, sub):
    prev_z = None
    prev_hi = None
    for r in range(10):
        zs = []
        for c in range(3):
            v = node_row(c, r)
            w = z_up(v, lane, sub)
            zs.append((v + w, w - v))
        if r > 0:
            a = {}
            for c in range(3):
                for z in (0, 1):
                    lo, hi = prev_z[c][z], zs[c][z]
                    for y, f in ((0, lo + hi), (1, hi - lo)):
                        a[c, 1, y, z] = f[1:4] - f[0:3]
                        if y or z:
                            a[c, 0, y, z] = f[0:3] + f[1:4]
            g = modal(a, em_row(r - 1))
            lows, highs = [], []
            for c in range(3):
                h = {}
                for y in (0, 1):
                    for z in (0, 1):
                        gd = g[c, 1, y, z]
                        t = gd[0:2] - gd[1:3]
                        if y or z:
                            gs = g[c, 0, y, z]
                            t = t + (gs[0:2] + gs[1:3])
                        h[y, z] = t
                lows.append([h[0, z] - h[1, z] for z in (0, 1)])
                highs.append([h[0, z] + h[1, z] for z in (0, 1)])
            if r > 1:
                out = []
                for c in range(3):
                    ks = prev_hi[c][0] + lows[c][0]
                    kd = prev_hi[c][1] + lows[c][1]
                    out.append((ks - kd) + z_dn(ks + kd, lane, sub))
                emit(r - 2, out)
            prev_hi = highs
        prev_z = zs


def cyc1(v, sub):
    return jnp.where(sub % 4 == 2, pltpu.roll(v, 2, axis=v.ndim - 2), pltpu.roll(v, 7, axis=v.ndim - 2))


def cyc2(v, sub):
    return jnp.where(sub % 4 == 0, pltpu.roll(v, 6, axis=v.ndim - 2), pltpu.roll(v, 1, axis=v.ndim - 2))


def pair_products(own_x, other_x, own_y, sub):
    return [
        own_x * own_y,
        cyc1(own_x, sub) * own_y,
        other_x * own_y,
        cyc1(other_x, sub) * own_y,
        cyc2(other_x, sub) * own_y,
    ]


def cholesky(m, n):
    low = {}
    inv = {}
    for j in range(n):
        s = m[j, j]
        for k in range(j):
            s = s - low[j, k] * low[j, k]
        inv[j] = 1.0 / jnp.sqrt(s)
        for i in range(j + 1, n):
            t = m[i, j]
            for k in range(j):
                t = t - low[i, k] * low[j, k]
            low[i, j] = t * inv[j]
    return low, inv


def forward(low, inv, rhs, n):
    out = []
    for i in range(n):
        t = rhs[i]
        for k in range(i):
            t = t - low[i, k] * out[k]
        out.append(t * inv[i])
    return out


def backward(low, inv, rhs, n):
    out = [None] * n
    for i in reversed(range(n)):
        t = rhs[i]
        for k in range(i + 1, n):
            t = t - low[k, i] * out[k]
        out[i] = t * inv[i]
    return out


def kernel(
    nx, ny,
    n_hbm, v_hbm, x_hbm, b_hbm, d_hbm, s_hbm,
    xo_hbm, ro_hbm,
    xin, bin_, din, sin, xm, ysend, esend, qs,
    nat, yrow, enat, ey, qnat,
    u0, u1, u2, em, mob, scl, rb, ib, yb, ga, ag, bg, dummy, xout, rout, nodes, vals,
    in_sem, out_sem, ss, rs, heard,
):
    grp, gx, gy, gz = (lax.axis_index(a) for a in ("grp", "gx", "gy", "gz"))
    oz = 1 - gz
    lane, sub = masks()
    valid = sub % 4 < 3
    scope = [None]

    def mark(name):
        if scope[0] is not None:
            scope[0].__exit__(None, None, None)
        scope[0] = None
        if name is not None:
            scope[0] = jax.named_scope(name)
            scope[0].__enter__()

    mark('entry')

    loads = [
        pltpu.make_async_copy(src, dst, in_sem.at[i])
        for i, (src, dst) in enumerate(((d_hbm, din), (s_hbm, sin), (x_hbm, xin), (b_hbm, bin_), (n_hbm, nodes), (v_hbm, vals)))
    ]
    for load in loads:
        load.start()

    barrier = pltpu.get_barrier_semaphore()

    def greet(cx, cy, cz):
        pl.semaphore_signal(barrier, inc=1, device_id=(grp, cx, cy, cz), device_id_type=MESH)

    exists = {}
    for dx in (-1, 0, 1):
        for dy in (-1, 0, 1):
            conds = []
            if dx:
                conds.append(gx > 0 if dx < 0 else gx < nx - 1)
            if dy:
                conds.append(gy > 0 if dy < 0 else gy < ny - 1)
            if conds:
                exists[dx, dy] = functools.reduce(jnp.logical_and, conds)

    def greet_if(here, targets):
        @pl.when(here)
        def _():
            for target in targets:
                greet(*target)

    bottom = gx == 0
    expected = bottom.astype(jnp.int32)
    for dy in (-1, 0, 1):
        greet_if(exists[1, dy], [(gx + 1, gy + dy, core) for core in (0, 1)])
        expected = expected + 2 * exists[-1, dy].astype(jnp.int32)
        if dy:
            here = jnp.logical_and(bottom, exists[0, dy])
            greet_if(here, [(gx, gy + dy, core) for core in (0, 1)])
            expected = expected + 2 * here.astype(jnp.int32)
        else:
            greet_if(bottom, [(gx, gy, oz)])

    def signal(index, cx, cy, cz):
        pl.semaphore_signal(heard.at[index], inc=1, device_id=(grp, cx, cy, cz), device_id_type=MESH)

    def signal_if(here, index, cx, cy, cz):
        pl.when(here)(lambda: signal(index, cx, cy, cz))

    def count_of(*conds):
        return sum(c.astype(jnp.int32) for c in conds)

    def wait_heard(index, each, *conds):
        @pl.when(functools.reduce(jnp.logical_or, conds))
        def _():
            pl.semaphore_wait(heard.at[index], each * count_of(*conds))

    def tell_y(k):
        step = 2**k
        if step < ny:
            signal_if(gy + step < ny, 1 + k, gx, gy + step, gz)
            signal_if(gy >= step, 1 + k, gx, gy - step, gz)

    def hear_y(k):
        step = 2**k
        if step < ny:
            wait_heard(1 + k, 1, gy + step < ny, gy >= step)

    def tell_x(k):
        step = 2**k
        if step < nx:
            signal_if(gx + step < nx, 4 + k, gx + step, gy, gz)
            signal_if(gx >= step, 8 + k, gx - step, gy, gz)

    def hear_x(k, below=True, above=True):
        step = 2**k
        if step < nx:
            if below:
                wait_heard(4 + k, 1, gx >= step)
            if above:
                wait_heard(8 + k, 1, gx + step < nx)

    def clear(ref, *index):
        ref[index] = jnp.zeros(ref[index].shape, f32)

    full = slice(None)

    @pl.when(gx == 0)
    def _():
        clear(nat, pl.ds(0, 3))
        clear(enat, full, 0)
        clear(ey, full, 0)
        for side in (0, 4):
            clear(yrow, side)
        for u in (u1, u2):
            clear(u, full, 0)

    @pl.when(gx == nx - 1)
    def _():
        clear(nat, pl.ds(9, 3))
        for side in (0, 4):
            clear(yrow, side + 3)
        for u in (u1, u2):
            clear(u, full, 3)

    @pl.when(gy == 0)
    def _():
        clear(yrow, pl.ds(0, 4))
        clear(ey)
        for u in (u1, u2):
            clear(u, full, full, 0)

    @pl.when(gy == ny - 1)
    def _():
        clear(yrow, pl.ds(4, 4))
        for u in (u1, u2):
            clear(u, full, full, 9)

    mark('barrier')
    pl.semaphore_wait(barrier, expected)
    for dy in (0, -1, 1):

        @pl.when(exists[-1, dy])
        def _(dy=dy):
            for core in (0, 1):
                signal(0, gx - 1, gy + dy, core)

    mark('prep')
    loads[0].wait()
    loads[1].wait()
    mnat = []
    for p in range(2):
        density = (din[p].astype(f32) + 1.0) * (1.0 / LEVELS)
        modulus = soft_modulus + (1.0 - soft_modulus) * density * density * density
        movable = 1.0 - sin[p].astype(f32)
        esend[p] = modulus
        esend[2 + p] = movable
        enat[gz, 1 + p] = modulus
        enat[gz, 3 + p] = movable
        mnat.append(movable)
    loads[2].wait()
    for side in range(2):
        for core in range(2):
            for p in range(2):
                ysend[side, core, p, 8:16] = jnp.zeros((8, 128), f32)
    for case in range(CASES):
        core, k = divmod(case, HALF)
        for comp in range(3):
            for p in range(2):
                t = mnat[p] * xin[case, comp, p]
                xm[core, p * 3 + comp, 8 * k:8 * k + 8] = t
                for side, y in ((0, 0), (1, 7)):
                    ysend[side, core, p, 4 * k + comp:4 * k + comp + 1] = t[y:y + 1]

    mark('send1')

    def view(ref, *index):
        return ref, index

    def descriptor(src, dst, send_index, recv_index, device):
        (a, i), (b, j) = src, dst
        return pltpu.make_async_remote_copy(
            src_ref=a.at[i] if i else a, dst_ref=b.at[j] if j else b,
            send_sem=ss.at[send_index], recv_sem=rs.at[recv_index],
            device_id=device, device_id_type=MESH,
        )

    def guarded_by(cond, go):
        if cond is None:
            go()
        else:
            pl.when(cond)(go)

    def exchange(cond, send_index, recv_index, items):
        def go():
            for src, dst, device in items:
                descriptor(src, dst, send_index, recv_index, device).start()

        guarded_by(cond, go)

    def wait_in(cond, index, ref):
        guarded_by(cond, lambda: descriptor(ref, ref, 0, index, partner).wait_recv())

    def wait_out(cond, index, ref):
        guarded_by(cond, lambda: descriptor(ref, ref, index, 0, partner).wait_send())

    def rows_of(count):
        return view(dummy, pl.ds(0, count))

    slot = {key: i for i, key in enumerate(exists)}
    partner = (grp, gx, gy, oz)

    half_rows = pl.ds(pl.multiple_of(32 * gz, 8), 24)
    half_16 = pl.ds(pl.multiple_of(16 * gz, 8), 16)
    other_rows = pl.ds(pl.multiple_of(32 * oz, 8), 24)
    bytes1 = {}

    def send_start(key):
        dx, dy = key
        items, count = [], 0
        p, there_p = (1, 0) if dx > 0 else (0, 3)
        side, there = (1, 0) if dy > 0 else (0, 1)
        for core in (0, 1):
            device = (grp, gx + dx, gy + dy, core)
            if dy == 0:
                items.append((view(xm, core, pl.ds(3 * p, 3)), view(nat, pl.ds(3 * there_p, 3), half_rows), device))
                count += 72
                if dx > 0:
                    items.append((view(esend, pl.ds(1, 1)), view(enat, gz, pl.ds(0, 1)), device))
                    count += 8
            elif dx == 0:
                items.append((view(ysend, side, core), view(yrow, pl.ds(4 * there + 1, 2), half_16), device))
                count += 32
                if dy > 0:
                    items.append((view(esend, pl.ds(0, 2)), view(ey, gz, pl.ds(1, 2)), device))
                    count += 16
            else:
                items.append((view(ysend, side, core, p), view(yrow, 4 * there + there_p, half_16), device))
                count += 16
                if dx > 0 and dy > 0:
                    items.append((view(esend, pl.ds(1, 1)), view(ey, gz, pl.ds(0, 1)), device))
                    count += 8
        exchange(exists[key], slot[key], slot[key], items)
        bytes1[key] = count

    order = sorted(exists, key=lambda k: (k[1] == 0, -abs(k[0])))
    for key in order:
        if key[0] < 0:
            send_start(key)
    mark('points')
    for load in loads[3:]:
        load.wait()
    across_z = 128 * 2
    across_y = 8 * ny * across_z
    number = (gy * 8 + sub) * across_z + gz * 128 + lane + (gx * 2) * across_y
    numbers = (number, number + across_y)

    def add_points(l, acc):
        acc = list(acc)
        for case in range(CASES):
            node = nodes[case, l]
            for p in range(2):
                hit = numbers[p] == node
                for comp in range(3):
                    at = (case * 2 + p) * 3 + comp
                    acc[at] = acc[at] + jnp.where(hit, vals[case, comp, l], 0.0)
        return tuple(acc)

    zero = jnp.zeros((8, 128), f32)
    points = lax.fori_loop(0, LOADS, add_points, (zero,) * (CASES * 6))
    for case in range(CASES):
        core, k = divmod(case, HALF)
        for p in range(2):
            m = mnat[p]
            for comp in range(3):
                total = bin_[case, comp, p] + points[(case * 2 + p) * 3 + comp]
                qs[core, p * 3 + comp, 8 * k:8 * k + 8] = m * total - (1.0 - m) * xin[case, comp, p]
    for k in range(6):
        nat[3 + k, half_rows] = xm[gz, k]
        qnat[k, half_rows] = qs[gz, k]

    mark('above')
    wait_heard(0, 2, *(exists[1, dy] for dy in (-1, 0, 1)))
    signal_if(gx < nx - 1, 12, gx + 1, gy, gz)
    for key in order:
        if key[0] > 0:
            send_start(key)
    wait_heard(12, 1, gx > 0)
    for key in order:
        if key[0] == 0:
            send_start(key)
    exchange(None, 8, 16, [
        (view(xm, oz), view(nat, pl.ds(3, 6), half_rows), partner),
        (view(esend), view(enat, gz, pl.ds(1, 4)), partner),
    ])
    exchange(None, 9, 17, [(view(qs, oz), view(qnat, full, half_rows), partner)])
    tell_x(0)
    tell_y(0)
    mark('wait1')
    for (dx, dy), index in slot.items():
        wait_in(exists[-dx, -dy], index, rows_of(bytes1[dx, dy]))
    wait_in(None, 16, rows_of(176))
    hear_x(0)
    tell_x(1)
    hear_y(0)
    tell_y(1)
    mark('build')

    low = sub < 4

    def spread(ref, k, y):
        return jnp.where(low, ref[0, k, y:y + 1], ref[1, k, y:y + 1])

    for j in range(9):
        for e in range(3):
            t = spread(ey, e, 7) if j == 0 else spread(enat, e, j - 1)
            em[j, e] = t * (MU / 16.0)
    for y in range(8):
        rows = em[y] + em[y + 1]
        around = rows[0:2] + rows[1:3]
        esum = (around + z_dn(around, lane, sub)) * (16.0 / MU)
        m = jnp.stack([spread(enat, 3, y), spread(enat, 4, y)])
        guarded = jnp.where(m > 0, esum, 1.0)
        mob[:, 8 * y:8 * y + 8] = m
        scl[:, 8 * y:8 * y + 8] = m / (K00 * guarded) + (1.0 - m)

    for r in range(10):
        for p in range(4):
            for comp in range(3):
                if r == 0:
                    t = yrow[p, pl.ds(comp, 8, stride=4), :]
                elif r == 9:
                    t = yrow[4 + p, pl.ds(comp, 8, stride=4), :]
                else:
                    t = nat[3 * p + comp, pl.ds(r - 1, 8, stride=8), :]
                u0[comp, p, r] = jnp.where(valid, t, 0.0)

    mark('waitq')
    wait_in(None, 17, view(qnat, full, other_rows))
    mark('k1')

    def at(y):
        return pl.ds(8 * y, 8)

    def first(y, force):
        m = mob[:, at(y)]
        s = scl[:, at(y)]
        for comp in range(3):
            q = jnp.stack([qnat[3 * p + comp, pl.ds(y, 8, stride=8), :] for p in range(2)])
            res = jnp.where(valid, q, 0.0) - m * force[comp]
            rb[gz, comp, :, at(y)] = res
            u1[comp, 1:3, 1 + y] = m * (s * res)

    apply_k(lambda c, r: u0[c, :, r], lambda j: em[j], first, lane, sub)

    def halo_views(u, key):
        dx, dy = key
        src, dst = (2, 0) if dx > 0 else (1, 3)
        ysrc, ydst = (8, 0) if dy > 0 else (1, 9)
        if dy == 0:
            return [(view(u, full, src, pl.ds(k, 3)), view(u, full, dst, pl.ds(k, 3))) for k in (1, 5)]
        if dx == 0:
            return [(view(u, full, pl.ds(1, 2), ysrc), view(u, full, pl.ds(1, 2), ydst))]
        return [(view(u, full, src, ysrc), view(u, full, dst, ydst))]

    halo_rows = {(dx, dy): 8 * 3 * (6 if dy == 0 else 2 if dx == 0 else 1) for dx, dy in exists}

    free = sub % 4 == 3

    def pack(u):
        for k in (0, 4):
            t = u[:, 1:3, k + 4]
            for i in (1, 2, 3):
                u[:, 1:3, k + i] = jnp.where(free, pltpu.roll(t, 4 - i, axis=2), u[:, 1:3, k + i])

    def unpack(u):
        for p in (0, 3):
            for k in (0, 4):
                a, b, c = (pltpu.roll(u[:, p, k + i], 4 + i, axis=1) for i in (1, 2, 3))
                u[:, p, k + 4] = jnp.where(sub % 4 == 0, a, jnp.where(sub % 4 == 1, b, c))

    def swap_halos(u, first_slot):
        pack(u)
        for key in sorted(exists, key=lambda k: (k[1] == 0, -abs(k[0]))):
            dx, dy = key
            exchange(
                exists[key], slot[key], first_slot + slot[key],
                [(a, b, (grp, gx + dx, gy + dy, gz)) for a, b in halo_views(u, key)],
            )

    def take_halos(u, first_slot):
        for dx, dy in exists:
            wait_in(exists[-dx, -dy], first_slot + slot[dx, dy], rows_of(halo_rows[dx, dy]))
        unpack(u)

    def sent_halos(u):
        for key in exists:
            wait_out(exists[key], slot[key], rows_of(halo_rows[key]))

    def share(buf, send_index, recv_index):
        exchange(None, send_index, recv_index, [(view(buf, gz), view(buf, gz), partner)])

    for key in exists:
        wait_out(exists[key], slot[key], rows_of(bytes1[key]))
    wait_out(None, 8, rows_of(176))
    swap_halos(u1, 8)
    share(rb, 8, 18)
    mark('wait2')
    take_halos(u1, 8)
    mark('k2')

    def second(y, force):
        m = mob[:, at(y)]
        s = scl[:, at(y)]
        for comp in range(3):
            d = s * rb[gz, comp, :, at(y)]
            image = m * force[comp] + (1.0 - m) * d
            ib[gz, comp, :, at(y)] = image
            u2[comp, 1:3, 1 + y] = m * (s * image)

    apply_k(lambda c, r: u1[c, :, r], lambda j: em[j], second, lane, sub)

    mark('send3')
    sent_halos(u1)
    wait_out(None, 9, view(qs, oz))
    swap_halos(u2, 0)
    share(ib, 9, 19)
    hear_x(1)
    tell_x(2)
    hear_y(1)
    tell_y(2)
    wait_in(None, 18, view(rb, oz))
    wait_in(None, 19, view(ib, oz))

    mark('grams')
    def grams(make):
        acc = None
        for y in range(8):
            s = scl[:, at(y)]
            for comp in range(3):
                prods = pair_products(*make(comp, y, s), sub)
                acc = prods if acc is None else [a + b for a, b in zip(acc, prods)]
        return [a[0] + a[1] for a in acc]

    def own_other(buf, comp, y):
        return buf[gz, comp, :, at(y)], buf[oz, comp, :, at(y)]

    def make_g(comp, y, s):
        r, ro = own_other(rb, comp, y)
        return s * r, s * ro, ib[gz, comp, :, at(y)]

    def make_h(comp, y, s):
        i, io = own_other(ib, comp, y)
        return i, io, s * i

    def make_p(comp, y, s):
        r, ro = own_other(rb, comp, y)
        return r, ro, s * r

    sums = grams(make_g) + grams(make_h) + grams(make_p)

    mark('wait3')
    take_halos(u2, 0)
    mark('k3')

    jacc = []

    def third(y, force):
        m = mob[:, at(y)]
        s = scl[:, at(y)]
        for comp in range(3):
            i, io = own_other(ib, comp, y)
            w = s * i
            image = m * force[comp] + (1.0 - m) * w
            yb[gz, comp, :, at(y)] = image
            prods = pair_products(w, s * io, image, sub)
            if jacc:
                jacc[0] = [a + b for a, b in zip(jacc[0], prods)]
            else:
                jacc.append(prods)

    apply_k(lambda c, r: u2[c, :, r], lambda j: em[j], third, lane, sub)
    wait_out(None, 8, view(rb, gz))
    share(yb, 8, 20)
    sums = sums + [a[0] + a[1] for a in jacc[0]]

    mark('rowsum')
    folded = [a + pltpu.roll(a, 4, axis=0) for a in sums]
    ga[pl.ds(80, 48), :] = jnp.zeros((48, 128), f32)
    for t in range(10):
        ga[pl.ds(8 * t, 8), :] = jnp.where(low, folded[2 * t], folded[2 * t + 1])
    row = lax.dot_general(
        jnp.ones((8, 128), f32), ga[...], (((1,), (1,)), ((), ())),
        precision=lax.Precision.HIGHEST, preferred_element_type=f32,
    )
    hear_y(2)
    mark('reduce_a')
    me = gz * ny + gy
    ag[me] = row[0:1]
    exchange(None, 10, 21, [
        (view(ag, me), view(ag, me), (grp, gx, lax.rem(gy + d, ny), oz if flip else gz))
        for d in range(ny) for flip in (0, 1) if d or flip
    ])
    hear_x(2)
    tell_x(3)
    wait_in(None, 21, view(ag, pl.ds(0, 2 * ny - 1)))
    for s in (0, 1):
        total = ag[s * ny]
        for k in range(1, ny):
            total = total + ag[s * ny + k]
        bg[gx, s:s + 1] = total
    hear_x(3, above=False)
    mark('reduce_b')
    def send_sum(target, carry):
        descriptor(view(bg, gx), view(bg, gx), 11, 22, (grp, target, gy, gz)).start()
        return carry

    lax.fori_loop(0, gx, send_sum, 0)
    hear_x(3, below=False)
    lax.fori_loop(gx + 1, nx, send_sum, 0)
    wait_in(None, 22, view(bg, pl.ds(0, nx - 1)))
    mark('solve')
    total = bg[0]
    for k in range(1, nx):
        total = total + bg[k]

    rows = [jnp.broadcast_to(total[s:s + 1], (8, 128)) for s in (0, 1)]

    def entry(matrix, i, j):
        ci, ki = divmod(i, HALF)
        cj, kj = divmod(j, HALF)
        if ci == cj:
            if (ki + 1) % 3 == kj:
                acc, k, s = 1, ki, ci
            elif ki == kj:
                acc, k, s = 0, ki, ci
            else:
                acc, k, s = 1, kj, ci
        else:
            if ci == 1:
                ki, kj = kj, ki
            acc, k, s = 2 + (kj - ki) % 3, ki, 0
        number = matrix * 5 + acc
        where = 8 * (number // 2) + 4 * (number % 2) + k
        return jnp.broadcast_to(rows[s][:, where:where + 1], (8, 128))

    n = CASES
    mats = []
    for matrix in range(4):
        m = {}
        for i in range(n):
            for j in range(i + 1):
                m[i, j] = entry(matrix, i, j)
                m[j, i] = m[i, j]
        mats.append(m)
    mg, mh, mp, mj = mats

    lo1, inv1 = cholesky(mg, n)
    zh = [forward(lo1, inv1, [mh[i, j] for i in range(n)], n) for j in range(n)]
    zp = [forward(lo1, inv1, [mp[i, j] for i in range(n)], n) for j in range(n)]
    th = [backward(lo1, inv1, zh[j], n) for j in range(n)]
    al = [backward(lo1, inv1, zp[j], n) for j in range(n)]
    schur, right = {}, []
    for j in range(n):
        col = []
        for i in range(n):
            t = mg[i, j]
            for k in range(n):
                t = t - zh[i][k] * zp[j][k]
            col.append(t)
            if i >= j:
                t = mj[i, j]
                for k in range(n):
                    t = t - zh[i][k] * zh[j][k]
                schur[i, j] = t
        right.append(col)
    lo2, inv2 = cholesky(schur, n)
    cb = [backward(lo2, inv2, forward(lo2, inv2, right[j], n), n) for j in range(n)]
    ca = []
    for j in range(n):
        col = []
        for i in range(n):
            t = al[j][i]
            for k in range(n):
                t = t - th[k][i] * cb[j][k]
            col.append(t)
        ca.append(col)

    mark('combine')
    wait_in(None, 20, view(yb, oz))
    for comp in range(3):
        for p in range(2):
            s = scl[p, pl.ds(4 * gz, 8, stride=8), :]
            fr, fi, fy = [], [], []
            for j in range(n):
                core, k = divmod(j, HALF)
                pick = pl.ds(4 * gz + k, 8, stride=8)
                fr.append(rb[core, comp, p, pick, :])
                fi.append(ib[core, comp, p, pick, :])
                fy.append(yb[core, comp, p, pick, :])
            for i in range(n):
                up = fr[0] * ca[i][0] + fi[0] * cb[i][0]
                dn = fi[0] * ca[i][0] + fy[0] * cb[i][0]
                for j in range(1, n):
                    up = up + fr[j] * ca[i][j] + fi[j] * cb[i][j]
                    dn = dn + fi[j] * ca[i][j] + fy[j] * cb[i][j]
                xout[i, comp, p] = s * up
                rout[i, comp, p] = (fr[i] - dn) + xin[i, comp, p]
        for i, (src, dst) in enumerate(((xout, xo_hbm), (rout, ro_hbm))):
            pltpu.make_async_copy(src.at[:, comp], dst.at[:, comp], out_sem.at[i]).start()
    mark('drain')
    sent_halos(u2)
    wait_out(None, 8, view(yb, gz))
    wait_out(None, 9, view(ib, gz))
    wait_out(None, 10, view(ag, pl.ds(0, 2 * ny - 1)))
    wait_out(None, 11, view(bg, pl.ds(0, nx - 1)))
    for i, (src, dst) in enumerate(((xout, xo_hbm), (rout, ro_hbm))):
        pltpu.make_async_copy(src, dst, out_sem.at[i]).wait()
    mark(None)


def shards(design, supports, body_load, start, load_nodes, load_values):
    nx, ny = lax.axis_size("gx"), lax.axis_size("gy")
    block = body_load.shape
    vmem = lambda *shape: pltpu.VMEM(shape, f32)
    spec = pl.BlockSpec(memory_space=pl.ANY)
    scratch = [
        vmem(*block), vmem(*block), pltpu.VMEM(design.shape, jnp.int32), pltpu.VMEM(design.shape, jnp.int32),
        vmem(2, 6, 24, 128), vmem(2, 2, 2, 16, 128), vmem(4, 8, 128), vmem(2, 6, 24, 128),
        vmem(12, 64, 128), vmem(8, 32, 128), vmem(2, 5, 8, 128), vmem(2, 3, 8, 128), vmem(6, 64, 128),
        vmem(3, 4, 10, 8, 128), vmem(3, 4, 10, 8, 128), vmem(3, 4, 10, 8, 128),
        vmem(9, 3, 8, 128), vmem(2, 64, 128), vmem(2, 64, 128),
        vmem(2, 3, 2, 64, 128), vmem(2, 3, 2, 64, 128), vmem(2, 3, 2, 64, 128),
        vmem(128, 128), vmem(2 * ny, 1, 128), vmem(nx, 2, 128), vmem(176, 128), vmem(*block), vmem(*block),
        pltpu.SMEM(load_nodes.shape, jnp.int32), pltpu.SMEM((CASES, 3, LOADS), f32),
        pltpu.SemaphoreType.DMA((6,)), pltpu.SemaphoreType.DMA((2,)), pltpu.SemaphoreType.DMA((12,)), pltpu.SemaphoreType.DMA((23,)),
        pltpu.SemaphoreType.REGULAR((13,)),
    ]
    out = jax.ShapeDtypeStruct(block, f32)
    change, shifted = pl.pallas_call(
        functools.partial(kernel, nx, ny),
        out_shape=(out, out),
        in_specs=[spec] * 6,
        out_specs=(spec, spec),
        scratch_shapes=scratch,
        compiler_params=pltpu.CompilerParams(collective_id=0, has_side_effects=True),
    )(load_nodes, jnp.transpose(load_values, (0, 2, 1)), start, body_load, design, supports)

    return start + change, shifted - start


def solution(mesh):
    in_specs = (
        P(("grp", "gx"), "gy", "gz"),
        P(("grp", "gx"), "gy", "gz"),
        P("grp", None, "gx", "gy", "gz"),
        P("grp", None, "gx", "gy", "gz"),
        P("grp", None),
        P("grp", None, None),
    )
    out_specs = (P("grp", None, "gx", "gy", "gz"), P("grp", None, "gx", "gy", "gz"))
    return jax.shard_map(shards, mesh=mesh, in_specs=in_specs, out_specs=out_specs, check_vma=False)
```

```python
import functools

import jax
import jax.numpy as jnp
from jax import lax
from jax.experimental import pallas as pl
from jax.experimental.pallas import tpu as pltpu
from jax.sharding import PartitionSpec as P

LEVELS = 16
CASES = 6
LOADS = 16
HALF = 3
soft_modulus = 0.05
poisson_ratio = 0.3
LAM = poisson_ratio / ((1.0 + poisson_ratio) * (1.0 - 2.0 * poisson_ratio))
MU = 1.0 / (2.0 * (1.0 + poisson_ratio))
C11 = LAM + 2.0 * MU
RHO = LAM / MU
KAP = C11 / MU + 1.0
K00 = (C11 + 2.0 * MU) / 9.0
MESH = pl.DeviceIdType.MESH
f32 = jnp.float32


def masks():
    lane = lax.broadcasted_iota(jnp.int32, (8, 128), 1)
    sub = lax.broadcasted_iota(jnp.int32, (8, 128), 0)
    return lane, sub


def z_up(v, lane, sub):
    nd = v.ndim
    sh = pltpu.roll(v, 127, axis=nd - 1)
    fx = pltpu.roll(sh, 4, axis=nd - 2)
    return jnp.where(lane == 127, jnp.where(sub < 4, fx, 0.0), sh)


def z_dn(v, lane, sub):
    nd = v.ndim
    sh = pltpu.roll(v, 1, axis=nd - 1)
    fx = pltpu.roll(sh, 4, axis=nd - 2)
    return jnp.where(lane == 0, jnp.where(sub >= 4, fx, 0.0), sh)


def modal(a, em):
    X, Y, Z = 0, 1, 2
    g = {}
    tr = RHO * (a[X, 1, 0, 0] + a[Y, 0, 1, 0] + a[Z, 0, 0, 1])
    for key in ((X, 1, 0, 0), (Y, 0, 1, 0), (Z, 0, 0, 1)):
        g[key] = em * (a[key] + a[key] + tr)
    for p, q in (
        ((X, 0, 1, 0), (Y, 1, 0, 0)),
        ((X, 0, 0, 1), (Z, 1, 0, 0)),
        ((Y, 0, 0, 1), (Z, 0, 1, 0)),
    ):
        g[p] = g[q] = em * (a[p] + a[q])
    e2 = em * (1.0 / 3.0)
    ek = em * (KAP / 3.0)
    er = em * (RHO / 3.0)
    for p, q in (
        ((X, 1, 1, 0), (Z, 0, 1, 1)),
        ((X, 1, 0, 1), (Y, 0, 1, 1)),
        ((Y, 1, 1, 0), (Z, 1, 0, 1)),
    ):
        g[p] = ek * a[p] + er * a[q]
        g[q] = ek * a[q] + er * a[p]
    three = ((X, 0, 1, 1), (Y, 1, 0, 1), (Z, 1, 1, 0))
    total = a[three[0]] + a[three[1]] + a[three[2]]
    for key in three:
        g[key] = e2 * (a[key] + total)
    e3 = em * ((C11 / MU + 2.0) / 9.0)
    for c in range(3):
        g[c, 1, 1, 1] = e3 * a[c, 1, 1, 1]
    return g


class Stiffness:
    def __init__(self, node_row, em_row, emit, lane, sub):
        self.node_row, self.em_row, self.emit, self.lane, self.sub = node_row, em_row, emit, lane, sub
        self.nodes, self.elements = {}, {}

    def node(self, r):
        if r not in self.nodes:
            zs = []
            for c in range(3):
                v = self.node_row(c, r)
                w = z_up(v, self.lane, self.sub)
                zs.append((v + w, w - v))
            self.nodes[r] = zs
        return self.nodes[r]

    def element(self, j):
        if j not in self.elements:
            low_row, high_row = self.node(j), self.node(j + 1)
            a = {}
            for c in range(3):
                for z in (0, 1):
                    lo, hi = low_row[c][z], high_row[c][z]
                    for y, f in ((0, lo + hi), (1, hi - lo)):
                        a[c, 1, y, z] = f[1:4] - f[0:3]
                        if y or z:
                            a[c, 0, y, z] = f[0:3] + f[1:4]
            g = modal(a, self.em_row(j))
            lows, highs = [], []
            for c in range(3):
                h = {}
                for y in (0, 1):
                    for z in (0, 1):
                        gd = g[c, 1, y, z]
                        t = gd[0:2] - gd[1:3]
                        if y or z:
                            gs = g[c, 0, y, z]
                            t = t + (gs[0:2] + gs[1:3])
                        h[y, z] = t
                lows.append([h[0, z] - h[1, z] for z in (0, 1)])
                highs.append([h[0, z] + h[1, z] for z in (0, 1)])
            self.elements[j] = lows, highs
        return self.elements[j]

    def rows(self, *ys):
        for y in ys:
            highs, lows = self.element(y)[1], self.element(y + 1)[0]
            out = []
            for c in range(3):
                ks = highs[c][0] + lows[c][0]
                kd = highs[c][1] + lows[c][1]
                out.append((ks - kd) + z_dn(ks + kd, self.lane, self.sub))
            self.emit(y, out)


def cyc1(v, sub):
    return jnp.where(sub % 4 == 2, pltpu.roll(v, 2, axis=v.ndim - 2), pltpu.roll(v, 7, axis=v.ndim - 2))


def cyc2(v, sub):
    return jnp.where(sub % 4 == 0, pltpu.roll(v, 6, axis=v.ndim - 2), pltpu.roll(v, 1, axis=v.ndim - 2))


def pair_products(own_x, other_x, own_y, sub):
    return [
        own_x * own_y,
        cyc1(own_x, sub) * own_y,
        other_x * own_y,
        cyc1(other_x, sub) * own_y,
        cyc2(other_x, sub) * own_y,
    ]


def cholesky(m, n):
    low = {}
    inv = {}
    for j in range(n):
        s = m[j, j]
        for k in range(j):
            s = s - low[j, k] * low[j, k]
        inv[j] = 1.0 / jnp.sqrt(s)
        for i in range(j + 1, n):
            t = m[i, j]
            for k in range(j):
                t = t - low[i, k] * low[j, k]
            low[i, j] = t * inv[j]
    return low, inv


def forward(low, inv, rhs, n):
    out = []
    for i in range(n):
        t = rhs[i]
        for k in range(i):
            t = t - low[i, k] * out[k]
        out.append(t * inv[i])
    return out


def backward(low, inv, rhs, n):
    out = [None] * n
    for i in reversed(range(n)):
        t = rhs[i]
        for k in range(i + 1, n):
            t = t - low[k, i] * out[k]
        out[i] = t * inv[i]
    return out


def kernel(
    nx, ny,
    n_hbm, v_hbm, x_hbm, b_hbm, d_hbm, s_hbm,
    xo_hbm, ro_hbm,
    xin, bin_, din, sin, xm, ysend, esend, qs,
    nat, yrow, enat, ey, qnat,
    u0, u1, u2, em, mob, scl, rb, ib, yb, ga, ag, bg, dummy, xout, rout, nodes, vals,
    in_sem, out_sem, ss, rs, heard,
):
    grp, gx, gy, gz = (lax.axis_index(a) for a in ("grp", "gx", "gy", "gz"))
    oz = 1 - gz
    lane, sub = masks()
    valid = sub % 4 < 3
    scope = [None]

    def mark(name):
        if scope[0] is not None:
            scope[0].__exit__(None, None, None)
        scope[0] = None
        if name is not None:
            scope[0] = jax.named_scope(name)
            scope[0].__enter__()

    mark('entry')

    loads = [
        pltpu.make_async_copy(src, dst, in_sem.at[i])
        for i, (src, dst) in enumerate(((d_hbm, din), (s_hbm, sin), (x_hbm, xin), (b_hbm, bin_), (n_hbm, nodes), (v_hbm, vals)))
    ]
    for load in loads:
        load.start()

    barrier = pltpu.get_barrier_semaphore()

    def greet(cx, cy, cz):
        pl.semaphore_signal(barrier, inc=1, device_id=(grp, cx, cy, cz), device_id_type=MESH)

    exists = {}
    for dx in (-1, 0, 1):
        for dy in (-1, 0, 1):
            conds = []
            if dx:
                conds.append(gx > 0 if dx < 0 else gx < nx - 1)
            if dy:
                conds.append(gy > 0 if dy < 0 else gy < ny - 1)
            if conds:
                exists[dx, dy] = functools.reduce(jnp.logical_and, conds)

    def greet_if(here, targets):
        @pl.when(here)
        def _():
            for target in targets:
                greet(*target)

    bottom = gx == 0
    expected = bottom.astype(jnp.int32)
    for dy in (-1, 0, 1):
        greet_if(exists[1, dy], [(gx + 1, gy + dy, core) for core in (0, 1)])
        expected = expected + 2 * exists[-1, dy].astype(jnp.int32)
        if dy:
            here = jnp.logical_and(bottom, exists[0, dy])
            greet_if(here, [(gx, gy + dy, core) for core in (0, 1)])
            expected = expected + 2 * here.astype(jnp.int32)
        else:
            greet_if(bottom, [(gx, gy, oz)])

    def signal(index, cx, cy, cz):
        pl.semaphore_signal(heard.at[index], inc=1, device_id=(grp, cx, cy, cz), device_id_type=MESH)

    def signal_if(here, index, cx, cy, cz):
        pl.when(here)(lambda: signal(index, cx, cy, cz))

    def count_of(*conds):
        return sum(c.astype(jnp.int32) for c in conds)

    def wait_heard(index, each, *conds):
        @pl.when(functools.reduce(jnp.logical_or, conds))
        def _():
            pl.semaphore_wait(heard.at[index], each * count_of(*conds))

    def tell_y(k):
        step = 2**k
        if step < ny:
            signal_if(gy + step < ny, 1 + k, gx, gy + step, gz)
            signal_if(gy >= step, 1 + k, gx, gy - step, gz)

    def hear_y(k):
        step = 2**k
        if step < ny:
            wait_heard(1 + k, 1, gy + step < ny, gy >= step)

    def tell_x(k):
        step = 2**k
        if step < nx:
            signal_if(gx + step < nx, 4 + k, gx + step, gy, gz)
            signal_if(gx >= step, 8 + k, gx - step, gy, gz)

    def hear_x(k, below=True, above=True):
        step = 2**k
        if step < nx:
            if below:
                wait_heard(4 + k, 1, gx >= step)
            if above:
                wait_heard(8 + k, 1, gx + step < nx)

    def clear(ref, *index):
        ref[index] = jnp.zeros(ref[index].shape, f32)

    full = slice(None)

    @pl.when(gx == 0)
    def _():
        clear(nat, pl.ds(0, 3))
        clear(enat, full, 0)
        clear(ey, full, 0)
        for side in (0, 4):
            clear(yrow, side)
        for u in (u1, u2):
            clear(u, full, 0)

    @pl.when(gx == nx - 1)
    def _():
        clear(nat, pl.ds(9, 3))
        for side in (0, 4):
            clear(yrow, side + 3)
        for u in (u1, u2):
            clear(u, full, 3)

    @pl.when(gy == 0)
    def _():
        clear(yrow, pl.ds(0, 4))
        clear(ey)
        for u in (u1, u2):
            clear(u, full, full, 0)

    @pl.when(gy == ny - 1)
    def _():
        clear(yrow, pl.ds(4, 4))
        for u in (u1, u2):
            clear(u, full, full, 9)

    mark('barrier')
    pl.semaphore_wait(barrier, expected)
    for dy in (0, -1, 1):

        @pl.when(exists[-1, dy])
        def _(dy=dy):
            for core in (0, 1):
                signal(13 if dy else 0, gx - 1, gy + dy, core)

    mark('prep')
    loads[0].wait()
    loads[1].wait()
    mnat = []
    for p in range(2):
        density = (din[p].astype(f32) + 1.0) * (1.0 / LEVELS)
        modulus = soft_modulus + (1.0 - soft_modulus) * density * density * density
        movable = 1.0 - sin[p].astype(f32)
        esend[p] = modulus
        esend[2 + p] = movable
        enat[gz, 1 + p] = modulus
        enat[gz, 3 + p] = movable
        mnat.append(movable)
    loads[2].wait()
    for side in range(2):
        for core in range(2):
            for p in range(2):
                ysend[side, core, p, 8:16] = jnp.zeros((8, 128), f32)
    for case in range(CASES):
        core, k = divmod(case, HALF)
        for comp in range(3):
            for p in range(2):
                t = mnat[p] * xin[case, comp, p]
                xm[core, p * 3 + comp, 8 * k:8 * k + 8] = t
                for side, y in ((0, 0), (1, 7)):
                    ysend[side, core, p, 4 * k + comp:4 * k + comp + 1] = t[y:y + 1]

    mark('send1')

    def view(ref, *index):
        return ref, index

    def descriptor(src, dst, send_index, recv_index, device):
        (a, i), (b, j) = src, dst
        return pltpu.make_async_remote_copy(
            src_ref=a.at[i] if i else a, dst_ref=b.at[j] if j else b,
            send_sem=ss.at[send_index], recv_sem=rs.at[recv_index],
            device_id=device, device_id_type=MESH,
        )

    def guarded_by(cond, go):
        if cond is None:
            go()
        else:
            pl.when(cond)(go)

    def exchange(cond, send_index, recv_index, items):
        def go():
            for src, dst, device in items:
                descriptor(src, dst, send_index, recv_index, device).start()

        guarded_by(cond, go)

    def wait_in(cond, index, ref):
        guarded_by(cond, lambda: descriptor(ref, ref, 0, index, partner).wait_recv())

    def wait_out(cond, index, ref):
        guarded_by(cond, lambda: descriptor(ref, ref, index, 0, partner).wait_send())

    def rows_of(count):
        return view(dummy, pl.ds(0, count))

    slot = {key: i for i, key in enumerate(exists)}
    partner = (grp, gx, gy, oz)

    half_rows = pl.ds(pl.multiple_of(32 * gz, 8), 24)
    half_16 = pl.ds(pl.multiple_of(16 * gz, 8), 16)
    other_rows = pl.ds(pl.multiple_of(32 * oz, 8), 24)
    bytes1 = {}

    def send_start(key):
        dx, dy = key
        items, count = [], 0
        p, there_p = (1, 0) if dx > 0 else (0, 3)
        side, there = (1, 0) if dy > 0 else (0, 1)
        for core in (0, 1):
            device = (grp, gx + dx, gy + dy, core)
            if dy == 0:
                items.append((view(xm, core, pl.ds(3 * p, 3)), view(nat, pl.ds(3 * there_p, 3), half_rows), device))
                count += 72
                if dx > 0:
                    items.append((view(esend, pl.ds(1, 1)), view(enat, gz, pl.ds(0, 1)), device))
                    count += 8
            elif dx == 0:
                items.append((view(ysend, side, core), view(yrow, pl.ds(4 * there + 1, 2), half_16), device))
                count += 32
                if dy > 0:
                    items.append((view(esend, pl.ds(0, 2)), view(ey, gz, pl.ds(1, 2)), device))
                    count += 16
            else:
                items.append((view(ysend, side, core, p), view(yrow, 4 * there + there_p, half_16), device))
                count += 16
                if dx > 0 and dy > 0:
                    items.append((view(esend, pl.ds(1, 1)), view(ey, gz, pl.ds(0, 1)), device))
                    count += 8
        exchange(exists[key], slot[key], slot[key], items)
        bytes1[key] = count

    order = sorted(exists, key=lambda k: (k[1] == 0, -abs(k[0])))
    for key in order:
        if key[0] < 0:
            send_start(key)
    mark('points')
    for load in loads[3:]:
        load.wait()
    across_z = 128 * 2
    across_y = 8 * ny * across_z
    number = (gy * 8 + sub) * across_z + gz * 128 + lane + (gx * 2) * across_y
    numbers = (number, number + across_y)

    def add_points(l, acc):
        acc = list(acc)
        for case in range(CASES):
            node = nodes[case, l]
            for p in range(2):
                hit = numbers[p] == node
                for comp in range(3):
                    at = (case * 2 + p) * 3 + comp
                    acc[at] = acc[at] + jnp.where(hit, vals[case, comp, l], 0.0)
        return tuple(acc)

    zero = jnp.zeros((8, 128), f32)
    points = lax.fori_loop(0, LOADS, add_points, (zero,) * (CASES * 6))
    for case in range(CASES):
        core, k = divmod(case, HALF)
        for p in range(2):
            m = mnat[p]
            for comp in range(3):
                total = bin_[case, comp, p] + points[(case * 2 + p) * 3 + comp]
                qs[core, p * 3 + comp, 8 * k:8 * k + 8] = m * total - (1.0 - m) * xin[case, comp, p]
    for k in range(6):
        nat[3 + k, half_rows] = xm[gz, k]
        qnat[k, half_rows] = qs[gz, k]

    mark('above')
    wait_heard(0, 2, exists[1, 0])
    send_start((1, 0))
    wait_heard(13, 2, exists[1, -1], exists[1, 1])
    signal_if(gx < nx - 1, 12, gx + 1, gy, gz)
    send_start((1, -1))
    send_start((1, 1))
    wait_heard(12, 1, gx > 0)
    for key in order:
        if key[0] == 0:
            send_start(key)
    exchange(None, 8, 16, [
        (view(xm, oz), view(nat, pl.ds(3, 6), half_rows), partner),
        (view(esend), view(enat, gz, pl.ds(1, 4)), partner),
    ])
    exchange(None, 9, 17, [(view(qs, oz), view(qnat, full, half_rows), partner)])
    tell_x(0)
    tell_y(0)
    mark('wait1')
    for (dx, dy), index in slot.items():
        wait_in(exists[-dx, -dy], index, rows_of(bytes1[dx, dy]))
    wait_in(None, 16, rows_of(176))
    hear_x(0)
    tell_x(1)
    hear_y(0)
    tell_y(1)
    mark('build')

    low = sub < 4

    def spread(ref, k, y):
        return jnp.where(low, ref[0, k, y:y + 1], ref[1, k, y:y + 1])

    for j in range(9):
        for e in range(3):
            t = spread(ey, e, 7) if j == 0 else spread(enat, e, j - 1)
            em[j, e] = t * (MU / 16.0)
    for y in range(8):
        rows = em[y] + em[y + 1]
        around = rows[0:2] + rows[1:3]
        esum = (around + z_dn(around, lane, sub)) * (16.0 / MU)
        m = jnp.stack([spread(enat, 3, y), spread(enat, 4, y)])
        guarded = jnp.where(m > 0, esum, 1.0)
        mob[:, 8 * y:8 * y + 8] = m
        scl[:, 8 * y:8 * y + 8] = m / (K00 * guarded) + (1.0 - m)

    for r in range(10):
        for p in range(4):
            for comp in range(3):
                if r == 0:
                    t = yrow[p, pl.ds(comp, 8, stride=4), :]
                elif r == 9:
                    t = yrow[4 + p, pl.ds(comp, 8, stride=4), :]
                else:
                    t = nat[3 * p + comp, pl.ds(r - 1, 8, stride=8), :]
                u0[comp, p, r] = jnp.where(valid, t, 0.0)

    mark('waitq')
    wait_in(None, 17, view(qnat, full, other_rows))
    mark('k1')

    def at(y):
        return pl.ds(8 * y, 8)

    def halo_views(u, key, chunk):
        dx, dy = key
        src, dst = (2, 0) if dx > 0 else (1, 3)
        ysrc, ydst = (8, 0) if dy > 0 else (1, 9)
        if dy == 0:
            return [
                (view(u, full, src, pl.ds(k, m)), view(u, full, dst, pl.ds(k, m)))
                for k, m in (((1, 2), (7, 1)) if chunk == 0 else ((3, 3),))
            ]
        if dx == 0:
            return [(view(u, full, pl.ds(1, 2), ysrc), view(u, full, pl.ds(1, 2), ydst))]
        return [(view(u, full, src, ysrc), view(u, full, dst, ydst))]

    halo_rows = {(dx, dy): 8 * 3 * (6 if dy == 0 else 2 if dx == 0 else 1) for dx, dy in exists}

    free = sub % 4 == 3
    chunks = ((1, 2, 7, 8), (3, 4, 5, 6))

    def pack(u, chunk):
        *carriers, last = chunks[chunk]
        t = u[:, 1:3, last]
        for i, k in enumerate(carriers, 1):
            u[:, 1:3, k] = jnp.where(free, pltpu.roll(t, 4 - i, axis=2), u[:, 1:3, k])

    def unpack(u, chunk):
        *carriers, last = chunks[chunk]
        for p in (0, 3):
            a, b, c = (pltpu.roll(u[:, p, k], 4 + i, axis=1) for i, k in enumerate(carriers, 1))
            u[:, p, last] = jnp.where(sub % 4 == 0, a, jnp.where(sub % 4 == 1, b, c))

    def halo_slot(first_slot, key, chunk):
        if chunk == 0:
            return first_slot + slot[key]
        return 23 + 2 * (first_slot == 0) + (key[0] > 0)

    def send_halos(u, first_slot, chunk):
        pack(u, chunk)
        for key in order:
            dx, dy = key
            if chunk == 0 or dy == 0:
                exchange(
                    exists[key], slot[key], halo_slot(first_slot, key, chunk),
                    [(a, b, (grp, gx + dx, gy + dy, gz)) for a, b in halo_views(u, key, chunk)],
                )

    def take_halos(u, first_slot, chunk):
        for key in exists:
            dx, dy = key
            if chunk == 0 or dy == 0:
                rows = halo_rows[key] // 2 if dy == 0 else halo_rows[key]
                wait_in(exists[-dx, -dy], halo_slot(first_slot, key, chunk), rows_of(rows))
        unpack(u, chunk)

    def sent_halos(u):
        for key in exists:
            wait_out(exists[key], slot[key], rows_of(halo_rows[key]))

    def share(buf, send_index, recv_index):
        exchange(None, send_index, recv_index, [(view(buf, gz), view(buf, gz), partner)])

    def first(y, force):
        m = mob[:, at(y)]
        s = scl[:, at(y)]
        for comp in range(3):
            q = jnp.stack([qnat[3 * p + comp, pl.ds(y, 8, stride=8), :] for p in range(2)])
            res = jnp.where(valid, q, 0.0) - m * force[comp]
            rb[gz, comp, :, at(y)] = res
            u1[comp, 1:3, 1 + y] = m * (s * res)

    def em_row(j):
        return em[j]

    stiff = Stiffness(lambda c, r: u0[c, :, r], em_row, first, lane, sub)
    stiff.rows(0, 7, 1, 6)
    for key in exists:
        wait_out(exists[key], slot[key], rows_of(bytes1[key]))
    wait_out(None, 8, rows_of(176))
    send_halos(u1, 8, 0)
    stiff.rows(2, 3, 4, 5)
    send_halos(u1, 8, 1)
    share(rb, 8, 18)
    mark('wait2')
    take_halos(u1, 8, 0)
    mark('k2')

    def second(y, force):
        m = mob[:, at(y)]
        s = scl[:, at(y)]
        for comp in range(3):
            d = s * rb[gz, comp, :, at(y)]
            image = m * force[comp] + (1.0 - m) * d
            ib[gz, comp, :, at(y)] = image
            u2[comp, 1:3, 1 + y] = m * (s * image)

    stiff = Stiffness(lambda c, r: u1[c, :, r], em_row, second, lane, sub)
    stiff.rows(0, 7)
    take_halos(u1, 8, 1)
    stiff.rows(1, 6)
    sent_halos(u1)
    send_halos(u2, 0, 0)
    stiff.rows(2, 3, 4, 5)
    send_halos(u2, 0, 1)
    mark('send3')
    wait_out(None, 9, view(qs, oz))
    share(ib, 9, 19)
    hear_x(1)
    tell_x(2)
    hear_y(1)
    tell_y(2)
    wait_in(None, 18, view(rb, oz))
    wait_in(None, 19, view(ib, oz))

    mark('grams')
    def grams(make):
        acc = None
        for y in range(8):
            s = scl[:, at(y)]
            for comp in range(3):
                prods = pair_products(*make(comp, y, s), sub)
                acc = prods if acc is None else [a + b for a, b in zip(acc, prods)]
        return [a[0] + a[1] for a in acc]

    def own_other(buf, comp, y):
        return buf[gz, comp, :, at(y)], buf[oz, comp, :, at(y)]

    def make_g(comp, y, s):
        r, ro = own_other(rb, comp, y)
        return s * r, s * ro, ib[gz, comp, :, at(y)]

    def make_h(comp, y, s):
        i, io = own_other(ib, comp, y)
        return i, io, s * i

    def make_p(comp, y, s):
        r, ro = own_other(rb, comp, y)
        return r, ro, s * r

    sums = grams(make_g) + grams(make_h) + grams(make_p)

    mark('wait3')
    take_halos(u2, 0, 0)
    mark('k3')

    jacc = []

    def third(y, force):
        m = mob[:, at(y)]
        s = scl[:, at(y)]
        for comp in range(3):
            i, io = own_other(ib, comp, y)
            w = s * i
            image = m * force[comp] + (1.0 - m) * w
            yb[gz, comp, :, at(y)] = image
            prods = pair_products(w, s * io, image, sub)
            if jacc:
                jacc[0] = [a + b for a, b in zip(jacc[0], prods)]
            else:
                jacc.append(prods)

    stiff = Stiffness(lambda c, r: u2[c, :, r], em_row, third, lane, sub)
    stiff.rows(0, 7)
    take_halos(u2, 0, 1)
    stiff.rows(1, 6, 2, 3, 4, 5)
    wait_out(None, 8, view(rb, gz))
    share(yb, 8, 20)
    sums = sums + [a[0] + a[1] for a in jacc[0]]

    mark('rowsum')
    folded = [a + pltpu.roll(a, 4, axis=0) for a in sums]
    ga[pl.ds(80, 48), :] = jnp.zeros((48, 128), f32)
    for t in range(10):
        ga[pl.ds(8 * t, 8), :] = jnp.where(low, folded[2 * t], folded[2 * t + 1])
    row = lax.dot_general(
        jnp.ones((8, 128), f32), ga[...], (((1,), (1,)), ((), ())),
        precision=lax.Precision.HIGHEST, preferred_element_type=f32,
    )
    hear_y(2)
    mark('reduce_a')
    me = gz * ny + gy
    ag[me] = row[0:1]
    exchange(None, 10, 21, [
        (view(ag, me), view(ag, me), (grp, gx, lax.rem(gy + d, ny), oz if flip else gz))
        for d in sorted(range(ny), key=lambda d: -min(d, ny - d)) for flip in (0, 1) if d or flip
    ])
    hear_x(2)
    tell_x(3)
    wait_in(None, 21, view(ag, pl.ds(0, 2 * ny - 1)))
    for s in (0, 1):
        total = ag[s * ny]
        for k in range(1, ny):
            total = total + ag[s * ny + k]
        bg[gx, s:s + 1] = total
    hear_x(3, above=False)
    mark('reduce_b')
    def send_sum(target, carry):
        descriptor(view(bg, gx), view(bg, gx), 11, 22, (grp, target, gy, gz)).start()
        return carry

    lax.fori_loop(0, gx, send_sum, 0)
    hear_x(3, below=False)
    lax.fori_loop(gx + 1, nx, send_sum, 0)
    wait_in(None, 22, view(bg, pl.ds(0, nx - 1)))
    mark('solve')
    total = bg[0]
    for k in range(1, nx):
        total = total + bg[k]

    rows = [jnp.broadcast_to(total[s:s + 1], (8, 128)) for s in (0, 1)]

    def entry(matrix, i, j):
        ci, ki = divmod(i, HALF)
        cj, kj = divmod(j, HALF)
        if ci == cj:
            if (ki + 1) % 3 == kj:
                acc, k, s = 1, ki, ci
            elif ki == kj:
                acc, k, s = 0, ki, ci
            else:
                acc, k, s = 1, kj, ci
        else:
            if ci == 1:
                ki, kj = kj, ki
            acc, k, s = 2 + (kj - ki) % 3, ki, 0
        number = matrix * 5 + acc
        where = 8 * (number // 2) + 4 * (number % 2) + k
        return jnp.broadcast_to(rows[s][:, where:where + 1], (8, 128))

    n = CASES
    mats = []
    for matrix in range(4):
        m = {}
        for i in range(n):
            for j in range(i + 1):
                m[i, j] = entry(matrix, i, j)
                m[j, i] = m[i, j]
        mats.append(m)
    mg, mh, mp, mj = mats

    lo1, inv1 = cholesky(mg, n)
    zh = [forward(lo1, inv1, [mh[i, j] for i in range(n)], n) for j in range(n)]
    zp = [forward(lo1, inv1, [mp[i, j] for i in range(n)], n) for j in range(n)]
    th = [backward(lo1, inv1, zh[j], n) for j in range(n)]
    al = [backward(lo1, inv1, zp[j], n) for j in range(n)]
    schur, right = {}, []
    for j in range(n):
        col = []
        for i in range(n):
            t = mg[i, j]
            for k in range(n):
                t = t - zh[i][k] * zp[j][k]
            col.append(t)
            if i >= j:
                t = mj[i, j]
                for k in range(n):
                    t = t - zh[i][k] * zh[j][k]
                schur[i, j] = t
        right.append(col)
    lo2, inv2 = cholesky(schur, n)
    cb = [backward(lo2, inv2, forward(lo2, inv2, right[j], n), n) for j in range(n)]
    ca = []
    for j in range(n):
        col = []
        for i in range(n):
            t = al[j][i]
            for k in range(n):
                t = t - th[k][i] * cb[j][k]
            col.append(t)
        ca.append(col)

    mark('combine')
    wait_in(None, 20, view(yb, oz))
    for comp in range(3):
        for p in range(2):
            s = scl[p, pl.ds(4 * gz, 8, stride=8), :]
            fr, fi, fy = [], [], []
            for j in range(n):
                core, k = divmod(j, HALF)
                pick = pl.ds(4 * gz + k, 8, stride=8)
                fr.append(rb[core, comp, p, pick, :])
                fi.append(ib[core, comp, p, pick, :])
                fy.append(yb[core, comp, p, pick, :])
            for i in range(n):
                up = fr[0] * ca[i][0] + fi[0] * cb[i][0]
                dn = fi[0] * ca[i][0] + fy[0] * cb[i][0]
                for j in range(1, n):
                    up = up + fr[j] * ca[i][j] + fi[j] * cb[i][j]
                    dn = dn + fi[j] * ca[i][j] + fy[j] * cb[i][j]
                xout[i, comp, p] = s * up
                rout[i, comp, p] = (fr[i] - dn) + xin[i, comp, p]
        for i, (src, dst) in enumerate(((xout, xo_hbm), (rout, ro_hbm))):
            pltpu.make_async_copy(src.at[:, comp], dst.at[:, comp], out_sem.at[i]).start()
    mark('drain')
    sent_halos(u2)
    wait_out(None, 8, view(yb, gz))
    wait_out(None, 9, view(ib, gz))
    wait_out(None, 10, view(ag, pl.ds(0, 2 * ny - 1)))
    wait_out(None, 11, view(bg, pl.ds(0, nx - 1)))
    for i, (src, dst) in enumerate(((xout, xo_hbm), (rout, ro_hbm))):
        pltpu.make_async_copy(src, dst, out_sem.at[i]).wait()
    mark(None)


def shards(design, supports, body_load, start, load_nodes, load_values):
    nx, ny = lax.axis_size("gx"), lax.axis_size("gy")
    block = body_load.shape
    vmem = lambda *shape: pltpu.VMEM(shape, f32)
    spec = pl.BlockSpec(memory_space=pl.ANY)
    scratch = [
        vmem(*block), vmem(*block), pltpu.VMEM(design.shape, jnp.int32), pltpu.VMEM(design.shape, jnp.int32),
        vmem(2, 6, 24, 128), vmem(2, 2, 2, 16, 128), vmem(4, 8, 128), vmem(2, 6, 24, 128),
        vmem(12, 64, 128), vmem(8, 32, 128), vmem(2, 5, 8, 128), vmem(2, 3, 8, 128), vmem(6, 64, 128),
        vmem(3, 4, 10, 8, 128), vmem(3, 4, 10, 8, 128), vmem(3, 4, 10, 8, 128),
        vmem(9, 3, 8, 128), vmem(2, 64, 128), vmem(2, 64, 128),
        vmem(2, 3, 2, 64, 128), vmem(2, 3, 2, 64, 128), vmem(2, 3, 2, 64, 128),
        vmem(128, 128), vmem(2 * ny, 1, 128), vmem(nx, 2, 128), vmem(176, 128), vmem(*block), vmem(*block),
        pltpu.SMEM(load_nodes.shape, jnp.int32), pltpu.SMEM((CASES, 3, LOADS), f32),
        pltpu.SemaphoreType.DMA((6,)), pltpu.SemaphoreType.DMA((2,)), pltpu.SemaphoreType.DMA((12,)), pltpu.SemaphoreType.DMA((27,)),
        pltpu.SemaphoreType.REGULAR((14,)),
    ]
    out = jax.ShapeDtypeStruct(block, f32)
    change, shifted = pl.pallas_call(
        functools.partial(kernel, nx, ny),
        out_shape=(out, out),
        in_specs=[spec] * 6,
        out_specs=(spec, spec),
        scratch_shapes=scratch,
        compiler_params=pltpu.CompilerParams(collective_id=0, has_side_effects=True),
    )(load_nodes, jnp.transpose(load_values, (0, 2, 1)), start, body_load, design, supports)

    return start + change, shifted - start


def solution(mesh):
    in_specs = (
        P(("grp", "gx"), "gy", "gz"),
        P(("grp", "gx"), "gy", "gz"),
        P("grp", None, "gx", "gy", "gz"),
        P("grp", None, "gx", "gy", "gz"),
        P("grp", None),
        P("grp", None, None),
    )
    out_specs = (P("grp", None, "gx", "gy", "gz"), P("grp", None, "gx", "gy", "gz"))
    return jax.shard_map(shards, mesh=mesh, in_specs=in_specs, out_specs=out_specs, check_vma=False)
```

```python
import functools

import jax
import jax.numpy as jnp
from jax import lax
from jax.experimental import pallas as pl
from jax.experimental.pallas import tpu as pltpu
from jax.sharding import PartitionSpec as P

LEVELS = 16
CASES = 6
LOADS = 16
HALF = 3
soft_modulus = 0.05
poisson_ratio = 0.3
LAM = poisson_ratio / ((1.0 + poisson_ratio) * (1.0 - 2.0 * poisson_ratio))
MU = 1.0 / (2.0 * (1.0 + poisson_ratio))
C11 = LAM + 2.0 * MU
RHO = LAM / MU
KAP = C11 / MU + 1.0
K00 = (C11 + 2.0 * MU) / 9.0
MESH = pl.DeviceIdType.MESH
f32 = jnp.float32


def masks():
    lane = lax.broadcasted_iota(jnp.int32, (8, 128), 1)
    sub = lax.broadcasted_iota(jnp.int32, (8, 128), 0)
    return lane, sub


def z_up(v, lane, sub):
    nd = v.ndim
    sh = pltpu.roll(v, 127, axis=nd - 1)
    fx = pltpu.roll(sh, 4, axis=nd - 2)
    return jnp.where(lane == 127, jnp.where(sub < 4, fx, 0.0), sh)


def z_dn(v, lane, sub):
    nd = v.ndim
    sh = pltpu.roll(v, 1, axis=nd - 1)
    fx = pltpu.roll(sh, 4, axis=nd - 2)
    return jnp.where(lane == 0, jnp.where(sub >= 4, fx, 0.0), sh)


def modal(a, em):
    X, Y, Z = 0, 1, 2
    g = {}
    tr = RHO * (a[X, 1, 0, 0] + a[Y, 0, 1, 0] + a[Z, 0, 0, 1])
    for key in ((X, 1, 0, 0), (Y, 0, 1, 0), (Z, 0, 0, 1)):
        g[key] = em * (a[key] + a[key] + tr)
    for p, q in (
        ((X, 0, 1, 0), (Y, 1, 0, 0)),
        ((X, 0, 0, 1), (Z, 1, 0, 0)),
        ((Y, 0, 0, 1), (Z, 0, 1, 0)),
    ):
        g[p] = g[q] = em * (a[p] + a[q])
    e2 = em * (1.0 / 3.0)
    ek = em * (KAP / 3.0)
    er = em * (RHO / 3.0)
    for p, q in (
        ((X, 1, 1, 0), (Z, 0, 1, 1)),
        ((X, 1, 0, 1), (Y, 0, 1, 1)),
        ((Y, 1, 1, 0), (Z, 1, 0, 1)),
    ):
        g[p] = ek * a[p] + er * a[q]
        g[q] = ek * a[q] + er * a[p]
    three = ((X, 0, 1, 1), (Y, 1, 0, 1), (Z, 1, 1, 0))
    total = a[three[0]] + a[three[1]] + a[three[2]]
    for key in three:
        g[key] = e2 * (a[key] + total)
    e3 = em * ((C11 / MU + 2.0) / 9.0)
    for c in range(3):
        g[c, 1, 1, 1] = e3 * a[c, 1, 1, 1]
    return g


class Stiffness:
    def __init__(self, node_row, em_row, emit, lane, sub):
        self.node_row, self.em_row, self.emit, self.lane, self.sub = node_row, em_row, emit, lane, sub
        self.nodes, self.elements = {}, {}

    def node(self, r):
        if r not in self.nodes:
            zs = []
            for c in range(3):
                v = self.node_row(c, r)
                w = z_up(v, self.lane, self.sub)
                zs.append((v + w, w - v))
            self.nodes[r] = zs
        return self.nodes[r]

    def element(self, j):
        if j not in self.elements:
            low_row, high_row = self.node(j), self.node(j + 1)
            a = {}
            for c in range(3):
                for z in (0, 1):
                    lo, hi = low_row[c][z], high_row[c][z]
                    for y, f in ((0, lo + hi), (1, hi - lo)):
                        a[c, 1, y, z] = f[1:4] - f[0:3]
                        if y or z:
                            a[c, 0, y, z] = f[0:3] + f[1:4]
            g = modal(a, self.em_row(j))
            lows, highs = [], []
            for c in range(3):
                h = {}
                for y in (0, 1):
                    for z in (0, 1):
                        gd = g[c, 1, y, z]
                        t = gd[0:2] - gd[1:3]
                        if y or z:
                            gs = g[c, 0, y, z]
                            t = t + (gs[0:2] + gs[1:3])
                        h[y, z] = t
                lows.append([h[0, z] - h[1, z] for z in (0, 1)])
                highs.append([h[0, z] + h[1, z] for z in (0, 1)])
            self.elements[j] = lows, highs
        return self.elements[j]

    def rows(self, *ys):
        for y in ys:
            highs, lows = self.element(y)[1], self.element(y + 1)[0]
            out = []
            for c in range(3):
                ks = highs[c][0] + lows[c][0]
                kd = highs[c][1] + lows[c][1]
                out.append((ks - kd) + z_dn(ks + kd, self.lane, self.sub))
            self.emit(y, out)


def cyc1(v, sub):
    return jnp.where(sub % 4 == 2, pltpu.roll(v, 2, axis=v.ndim - 2), pltpu.roll(v, 7, axis=v.ndim - 2))


def cyc2(v, sub):
    return jnp.where(sub % 4 == 0, pltpu.roll(v, 6, axis=v.ndim - 2), pltpu.roll(v, 1, axis=v.ndim - 2))


def pair_products(own_x, other_x, own_y, sub):
    return [
        own_x * own_y,
        cyc1(own_x, sub) * own_y,
        other_x * own_y,
        cyc1(other_x, sub) * own_y,
        cyc2(other_x, sub) * own_y,
    ]


def cholesky(m, n):
    low = {}
    inv = {}
    for j in range(n):
        s = m[j, j]
        for k in range(j):
            s = s - low[j, k] * low[j, k]
        inv[j] = lax.rsqrt(s)
        for i in range(j + 1, n):
            t = m[i, j]
            for k in range(j):
                t = t - low[i, k] * low[j, k]
            low[i, j] = t * inv[j]
    return low, inv


def forward(low, inv, rhs, n):
    out = []
    for i in range(n):
        t = rhs[i]
        for k in range(i):
            t = t - low[i, k] * out[k]
        out.append(t * inv[i])
    return out


def backward(low, inv, rhs, n):
    out = [None] * n
    for i in reversed(range(n)):
        t = rhs[i]
        for k in range(i + 1, n):
            t = t - low[k, i] * out[k]
        out[i] = t * inv[i]
    return out


def kernel(
    nx, ny,
    n_hbm, v_hbm, x_hbm, b_hbm, d_hbm, s_hbm,
    xo_hbm, ro_hbm,
    xin, bin_, din, sin, xm, ysend, esend, qs,
    nat, yrow, enat, qnat,
    u0, u1, u2, em, mob, scl, rb, ib, yb, ga, ag, bg, dummy, xout, rout, nodes, vals,
    in_sem, out_sem, ss, rs, heard,
):
    grp, gx, gy, gz = (lax.axis_index(a) for a in ("grp", "gx", "gy", "gz"))
    oz = 1 - gz
    lane, sub = masks()
    valid = sub % 4 < 3
    scope = [None]

    def mark(name):
        if scope[0] is not None:
            scope[0].__exit__(None, None, None)
        scope[0] = None
        if name is not None:
            scope[0] = jax.named_scope(name)
            scope[0].__enter__()

    mark('entry')

    loads = [
        pltpu.make_async_copy(src, dst, in_sem.at[i])
        for i, (src, dst) in enumerate(((d_hbm, din), (s_hbm, sin), (x_hbm, xin), (b_hbm, bin_), (n_hbm, nodes), (v_hbm, vals)))
    ]
    for load in loads:
        load.start()

    barrier = pltpu.get_barrier_semaphore()

    def greet(cx, cy, cz):
        pl.semaphore_signal(barrier, inc=1, device_id=(grp, cx, cy, cz), device_id_type=MESH)

    exists = {}
    for dx in (-1, 0, 1):
        for dy in (-1, 0, 1):
            conds = []
            if dx:
                conds.append(gx > 0 if dx < 0 else gx < nx - 1)
            if dy:
                conds.append(gy > 0 if dy < 0 else gy < ny - 1)
            if conds:
                exists[dx, dy] = functools.reduce(jnp.logical_and, conds)

    def greet_if(here, targets):
        @pl.when(here)
        def _():
            for target in targets:
                greet(*target)

    bottom = gx == 0
    expected = bottom.astype(jnp.int32)
    for dy in (-1, 0, 1):
        greet_if(exists[1, dy], [(gx + 1, gy + dy, core) for core in (0, 1)])
        expected = expected + 2 * exists[-1, dy].astype(jnp.int32)
        if dy:
            here = jnp.logical_and(bottom, exists[0, dy])
            greet_if(here, [(gx, gy + dy, core) for core in (0, 1)])
            expected = expected + 2 * here.astype(jnp.int32)
        else:
            greet_if(bottom, [(gx, gy, oz)])

    def signal(index, cx, cy, cz):
        pl.semaphore_signal(heard.at[index], inc=1, device_id=(grp, cx, cy, cz), device_id_type=MESH)

    def signal_if(here, index, cx, cy, cz):
        pl.when(here)(lambda: signal(index, cx, cy, cz))

    def count_of(*conds):
        return sum(c.astype(jnp.int32) for c in conds)

    def wait_heard(index, each, *conds):
        @pl.when(functools.reduce(jnp.logical_or, conds))
        def _():
            pl.semaphore_wait(heard.at[index], each * count_of(*conds))

    def tell_y(k):
        step = 2**k
        if step < ny:
            signal_if(gy + step < ny, 1 + k, gx, gy + step, gz)
            signal_if(gy >= step, 1 + k, gx, gy - step, gz)

    def hear_y(k):
        step = 2**k
        if step < ny:
            wait_heard(1 + k, 1, gy + step < ny, gy >= step)

    def tell_x(k):
        step = 2**k
        if step < nx:
            signal_if(gx + step < nx, 4 + k, gx + step, gy, gz)
            signal_if(gx >= step, 8 + k, gx - step, gy, gz)

    def hear_x(k, below=True, above=True):
        step = 2**k
        if step < nx:
            if below:
                wait_heard(4 + k, 1, gx >= step)
            if above:
                wait_heard(8 + k, 1, gx + step < nx)

    def clear(ref, *index):
        ref[index] = jnp.zeros(ref[index].shape, f32)

    full = slice(None)

    @pl.when(gx == 0)
    def _():
        clear(nat, pl.ds(0, 3))
        clear(enat, full, 0)
        for side in (0, 4):
            clear(yrow, side)
        for u in (u1, u2):
            clear(u, full, 0)

    @pl.when(gx == nx - 1)
    def _():
        clear(nat, pl.ds(9, 3))
        for side in (0, 4):
            clear(yrow, side + 3)
        for u in (u1, u2):
            clear(u, full, 3)

    @pl.when(gy == 0)
    def _():
        clear(yrow, pl.ds(0, 4))
        for u in (u1, u2):
            clear(u, full, full, 0)

    @pl.when(gy == ny - 1)
    def _():
        clear(yrow, pl.ds(4, 4))
        for u in (u1, u2):
            clear(u, full, full, 9)

    mark('barrier')
    pl.semaphore_wait(barrier, expected)
    for dy in (0, -1, 1):

        @pl.when(exists[-1, dy])
        def _(dy=dy):
            for core in (0, 1):
                signal(13 if dy else 0, gx - 1, gy + dy, core)

    mark('prep')
    loads[0].wait()
    loads[1].wait()
    mnat = []
    for p in range(2):
        density = (din[p].astype(f32) + 1.0) * (1.0 / LEVELS)
        modulus = soft_modulus + (1.0 - soft_modulus) * density * density * density
        movable = 1.0 - sin[p].astype(f32)
        esend[p] = modulus
        esend[2 + p] = movable
        enat[gz, 1 + p] = modulus
        enat[gz, 3 + p] = movable
        mnat.append(movable)
    loads[2].wait()
    for side in range(2):
        for core in range(2):
            for p in range(2):
                ysend[side, core, p, 8:16] = jnp.zeros((8, 128), f32)
                if side == 1:
                    ysend[side, core, p, 12:13] = esend[p, 7:8]
    for case in range(CASES):
        core, k = divmod(case, HALF)
        for comp in range(3):
            for p in range(2):
                t = mnat[p] * xin[case, comp, p]
                xm[core, p * 3 + comp, 8 * k:8 * k + 8] = t
                for side, y in ((0, 0), (1, 7)):
                    ysend[side, core, p, 4 * k + comp:4 * k + comp + 1] = t[y:y + 1]

    mark('send1')

    def view(ref, *index):
        return ref, index

    def descriptor(src, dst, send_index, recv_index, device):
        (a, i), (b, j) = src, dst
        return pltpu.make_async_remote_copy(
            src_ref=a.at[i] if i else a, dst_ref=b.at[j] if j else b,
            send_sem=ss.at[send_index], recv_sem=rs.at[recv_index],
            device_id=device, device_id_type=MESH,
        )

    def guarded_by(cond, go):
        if cond is None:
            go()
        else:
            pl.when(cond)(go)

    def exchange(cond, send_index, recv_index, items):
        def go():
            for src, dst, device in items:
                descriptor(src, dst, send_index, recv_index, device).start()

        guarded_by(cond, go)

    def wait_in(cond, index, ref):
        guarded_by(cond, lambda: descriptor(ref, ref, 0, index, partner).wait_recv())

    def wait_out(cond, index, ref):
        guarded_by(cond, lambda: descriptor(ref, ref, index, 0, partner).wait_send())

    def rows_of(count):
        return view(dummy, pl.ds(0, count))

    slot = {key: i for i, key in enumerate(exists)}
    partner = (grp, gx, gy, oz)

    half_rows = pl.ds(pl.multiple_of(32 * gz, 8), 24)
    half_16 = pl.ds(pl.multiple_of(16 * gz, 8), 16)
    other_rows = pl.ds(pl.multiple_of(32 * oz, 8), 24)
    bytes1 = {}

    def send_start(key):
        dx, dy = key
        items, count = [], 0
        p, there_p = (1, 0) if dx > 0 else (0, 3)
        side, there = (1, 0) if dy > 0 else (0, 1)
        for core in (0, 1):
            device = (grp, gx + dx, gy + dy, core)
            if dy == 0:
                items.append((view(xm, core, pl.ds(3 * p, 3)), view(nat, pl.ds(3 * there_p, 3), half_rows), device))
                count += 72
                if dx > 0:
                    items.append((view(esend, pl.ds(1, 1)), view(enat, gz, pl.ds(0, 1)), device))
                    count += 8
            elif dx == 0:
                items.append((view(ysend, side, core), view(yrow, pl.ds(4 * there + 1, 2), half_16), device))
                count += 32
            else:
                items.append((view(ysend, side, core, p), view(yrow, 4 * there + there_p, half_16), device))
                count += 16
        exchange(exists[key], slot[key], slot[key], items)
        bytes1[key] = count

    order = sorted(exists, key=lambda k: (k[1] == 0, -abs(k[0])))
    for key in order:
        if key[0] < 0:
            send_start(key)
    mark('points')
    for load in loads[3:]:
        load.wait()
    across_z = 128 * 2
    across_y = 8 * ny * across_z
    number = (gy * 8 + sub) * across_z + gz * 128 + lane + (gx * 2) * across_y
    numbers = (number, number + across_y)

    def add_points(l, acc):
        acc = list(acc)
        for case in range(CASES):
            node = nodes[case, l]
            for p in range(2):
                hit = numbers[p] == node
                for comp in range(3):
                    at = (case * 2 + p) * 3 + comp
                    acc[at] = acc[at] + jnp.where(hit, vals[case, comp, l], 0.0)
        return tuple(acc)

    zero = jnp.zeros((8, 128), f32)
    points = lax.fori_loop(0, LOADS, add_points, (zero,) * (CASES * 6))
    for case in range(CASES):
        core, k = divmod(case, HALF)
        for p in range(2):
            m = mnat[p]
            for comp in range(3):
                total = bin_[case, comp, p] + points[(case * 2 + p) * 3 + comp]
                qs[core, p * 3 + comp, 8 * k:8 * k + 8] = m * total - (1.0 - m) * xin[case, comp, p]
    for k in range(6):
        nat[3 + k, half_rows] = xm[gz, k]
        qnat[k, half_rows] = qs[gz, k]

    mark('above')
    wait_heard(0, 2, exists[1, 0])
    send_start((1, 0))
    wait_heard(13, 2, exists[1, -1], exists[1, 1])
    signal_if(gx < nx - 1, 12, gx + 1, gy, gz)
    send_start((1, -1))
    send_start((1, 1))
    wait_heard(12, 1, gx > 0)
    for key in order:
        if key[0] == 0:
            send_start(key)
    exchange(None, 8, 16, [
        (view(xm, oz), view(nat, pl.ds(3, 6), half_rows), partner),
        (view(esend), view(enat, gz, pl.ds(1, 4)), partner),
    ])
    exchange(None, 9, 17, [(view(qs, oz), view(qnat, full, half_rows), partner)])
    tell_x(0)
    tell_y(0)
    mark('wait1')
    for (dx, dy), index in slot.items():
        wait_in(exists[-dx, -dy], index, rows_of(bytes1[dx, dy]))
    wait_in(None, 16, rows_of(176))
    hear_x(0)
    tell_x(1)
    hear_y(0)
    tell_y(1)
    mark('build')

    low = sub < 4

    def spread(ref, k, y):
        return jnp.where(low, ref[0, k, y:y + 1], ref[1, k, y:y + 1])

    for j in range(9):
        for e in range(3):
            if j == 0:
                t = jnp.where(low, yrow[e, 12:13], yrow[e, 28:29])
            else:
                t = spread(enat, e, j - 1)
            em[j, e] = t * (MU / 16.0)
    for y in range(8):
        rows = em[y] + em[y + 1]
        around = rows[0:2] + rows[1:3]
        esum = (around + z_dn(around, lane, sub)) * (16.0 / MU)
        m = jnp.stack([spread(enat, 3, y), spread(enat, 4, y)])
        guarded = jnp.where(m > 0, esum, 1.0)
        mob[:, 8 * y:8 * y + 8] = m
        scl[:, 8 * y:8 * y + 8] = m / (K00 * guarded) + (1.0 - m)

    for r in range(10):
        for p in range(4):
            for comp in range(3):
                if r == 0:
                    t = yrow[p, pl.ds(comp, 8, stride=4), :]
                elif r == 9:
                    t = yrow[4 + p, pl.ds(comp, 8, stride=4), :]
                else:
                    t = nat[3 * p + comp, pl.ds(r - 1, 8, stride=8), :]
                u0[comp, p, r] = jnp.where(valid, t, 0.0)

    mark('waitq')
    wait_in(None, 17, view(qnat, full, other_rows))
    mark('k1')

    def at(y):
        return pl.ds(8 * y, 8)

    def halo_views(u, key, chunk):
        dx, dy = key
        src, dst = (2, 0) if dx > 0 else (1, 3)
        ysrc, ydst = (8, 0) if dy > 0 else (1, 9)
        if dy == 0:
            return [
                (view(u, full, src, pl.ds(k, m)), view(u, full, dst, pl.ds(k, m)))
                for k, m in (((1, 2), (7, 1)) if chunk == 0 else ((3, 3),))
            ]
        if dx == 0:
            return [(view(u, full, pl.ds(1, 2), ysrc), view(u, full, pl.ds(1, 2), ydst))]
        return [(view(u, full, src, ysrc), view(u, full, dst, ydst))]

    halo_rows = {(dx, dy): 8 * 3 * (6 if dy == 0 else 2 if dx == 0 else 1) for dx, dy in exists}

    free = sub % 4 == 3
    chunks = ((1, 2, 7, 8), (3, 4, 5, 6))

    def pack(u, chunk):
        *carriers, last = chunks[chunk]
        t = u[:, 1:3, last]
        for i, k in enumerate(carriers, 1):
            u[:, 1:3, k] = jnp.where(free, pltpu.roll(t, 4 - i, axis=2), u[:, 1:3, k])

    def unpack(u, chunk):
        *carriers, last = chunks[chunk]
        for p in (0, 3):
            a, b, c = (pltpu.roll(u[:, p, k], 4 + i, axis=1) for i, k in enumerate(carriers, 1))
            u[:, p, last] = jnp.where(sub % 4 == 0, a, jnp.where(sub % 4 == 1, b, c))

    def halo_slot(first_slot, key, chunk):
        if chunk == 0:
            return first_slot + slot[key]
        return 23 + 2 * (first_slot == 0) + (key[0] > 0)

    def send_halos(u, first_slot, chunk):
        pack(u, chunk)
        for key in order:
            dx, dy = key
            if chunk == 0 or dy == 0:
                exchange(
                    exists[key], slot[key], halo_slot(first_slot, key, chunk),
                    [(a, b, (grp, gx + dx, gy + dy, gz)) for a, b in halo_views(u, key, chunk)],
                )

    def take_halos(u, first_slot, chunk):
        for key in exists:
            dx, dy = key
            if chunk == 0 or dy == 0:
                rows = halo_rows[key] // 2 if dy == 0 else halo_rows[key]
                wait_in(exists[-dx, -dy], halo_slot(first_slot, key, chunk), rows_of(rows))
        unpack(u, chunk)

    def sent_halos(u):
        for key in exists:
            wait_out(exists[key], slot[key], rows_of(halo_rows[key]))

    def share(buf, send_index, recv_index):
        exchange(None, send_index, recv_index, [(view(buf, gz), view(buf, gz), partner)])

    def first(y, force):
        m = mob[:, at(y)]
        s = scl[:, at(y)]
        for comp in range(3):
            q = jnp.stack([qnat[3 * p + comp, pl.ds(y, 8, stride=8), :] for p in range(2)])
            res = jnp.where(valid, q, 0.0) - m * force[comp]
            rb[gz, comp, :, at(y)] = res
            u1[comp, 1:3, 1 + y] = m * (s * res)

    def em_row(j):
        return em[j]

    stiff = Stiffness(lambda c, r: u0[c, :, r], em_row, first, lane, sub)
    stiff.rows(0, 7, 1, 6)
    for key in exists:
        wait_out(exists[key], slot[key], rows_of(bytes1[key]))
    wait_out(None, 8, rows_of(176))
    send_halos(u1, 8, 0)
    stiff.rows(2, 3, 4, 5)
    send_halos(u1, 8, 1)
    share(rb, 8, 18)
    mark('wait2')
    take_halos(u1, 8, 0)
    take_halos(u1, 8, 1)
    mark('k2')

    def second(y, force):
        m = mob[:, at(y)]
        s = scl[:, at(y)]
        for comp in range(3):
            d = s * rb[gz, comp, :, at(y)]
            image = m * force[comp] + (1.0 - m) * d
            ib[gz, comp, :, at(y)] = image
            u2[comp, 1:3, 1 + y] = m * (s * image)

    stiff = Stiffness(lambda c, r: u1[c, :, r], em_row, second, lane, sub)
    stiff.rows(0, 7)
    stiff.rows(1, 6)
    sent_halos(u1)
    send_halos(u2, 0, 0)
    stiff.rows(2, 3, 4, 5)
    send_halos(u2, 0, 1)
    mark('send3')
    wait_out(None, 9, view(qs, oz))
    share(ib, 9, 19)
    hear_x(1)
    tell_x(2)
    hear_y(1)
    tell_y(2)
    wait_in(None, 18, view(rb, oz))
    wait_in(None, 19, view(ib, oz))

    mark('grams')
    def grams(make):
        acc = None
        for y in range(8):
            s = scl[:, at(y)]
            for comp in range(3):
                prods = pair_products(*make(comp, y, s), sub)
                acc = prods if acc is None else [a + b for a, b in zip(acc, prods)]
        return [a[0] + a[1] for a in acc]

    def own_other(buf, comp, y):
        return buf[gz, comp, :, at(y)], buf[oz, comp, :, at(y)]

    def make_g(comp, y, s):
        r, ro = own_other(rb, comp, y)
        return s * r, s * ro, ib[gz, comp, :, at(y)]

    def make_h(comp, y, s):
        i, io = own_other(ib, comp, y)
        return i, io, s * i

    def make_p(comp, y, s):
        r, ro = own_other(rb, comp, y)
        return r, ro, s * r

    sums = grams(make_g) + grams(make_h) + grams(make_p)

    mark('wait3')
    take_halos(u2, 0, 0)
    mark('k3')

    jacc = []

    def third(y, force):
        m = mob[:, at(y)]
        s = scl[:, at(y)]
        for comp in range(3):
            i, io = own_other(ib, comp, y)
            w = s * i
            image = m * force[comp] + (1.0 - m) * w
            yb[gz, comp, :, at(y)] = image
            prods = pair_products(w, s * io, image, sub)
            if jacc:
                jacc[0] = [a + b for a, b in zip(jacc[0], prods)]
            else:
                jacc.append(prods)

    stiff = Stiffness(lambda c, r: u2[c, :, r], em_row, third, lane, sub)
    stiff.rows(0, 7)
    take_halos(u2, 0, 1)
    stiff.rows(1, 6, 2, 3, 4, 5)
    wait_out(None, 8, view(rb, gz))
    share(yb, 8, 20)
    sums = sums + [a[0] + a[1] for a in jacc[0]]

    mark('rowsum')
    folded = [a + pltpu.roll(a, 4, axis=0) for a in sums]
    ga[pl.ds(80, 48), :] = jnp.zeros((48, 128), f32)
    for t in range(10):
        ga[pl.ds(8 * t, 8), :] = jnp.where(low, folded[2 * t], folded[2 * t + 1])
    row = lax.dot_general(
        jnp.ones((8, 128), f32), ga[...], (((1,), (1,)), ((), ())),
        precision=lax.Precision.HIGHEST, preferred_element_type=f32,
    )
    hear_y(2)
    mark('reduce_a')
    me = gz * ny + gy
    ag[me] = row[0:1]
    exchange(None, 10, 21, [
        (view(ag, me), view(ag, me), (grp, gx, lax.rem(gy + d, ny), oz if flip else gz))
        for d in sorted(range(ny), key=lambda d: -min(d, ny - d)) for flip in (0, 1) if d or flip
    ])
    hear_x(2)
    tell_x(3)
    wait_in(None, 21, view(ag, pl.ds(0, 2 * ny - 1)))
    for s in (0, 1):
        total = ag[s * ny]
        for k in range(1, ny):
            total = total + ag[s * ny + k]
        bg[gx, s:s + 1] = total
    hear_x(3, above=False)
    mark('reduce_b')
    def send_sum(target, carry):
        descriptor(view(bg, gx), view(bg, gx), 11, 22, (grp, target, gy, gz)).start()
        return carry

    lax.fori_loop(0, gx, send_sum, 0)
    hear_x(3, below=False)
    lax.fori_loop(gx + 1, nx, send_sum, 0)
    wait_in(None, 22, view(bg, pl.ds(0, nx - 1)))
    mark('solve')
    total = bg[0]
    for k in range(1, nx):
        total = total + bg[k]

    rows = [jnp.broadcast_to(total[s:s + 1], (8, 128)) for s in (0, 1)]

    def entry(matrix, i, j):
        ci, ki = divmod(i, HALF)
        cj, kj = divmod(j, HALF)
        if ci == cj:
            if (ki + 1) % 3 == kj:
                acc, k, s = 1, ki, ci
            elif ki == kj:
                acc, k, s = 0, ki, ci
            else:
                acc, k, s = 1, kj, ci
        else:
            if ci == 1:
                ki, kj = kj, ki
            acc, k, s = 2 + (kj - ki) % 3, ki, 0
        number = matrix * 5 + acc
        where = 8 * (number // 2) + 4 * (number % 2) + k
        return jnp.broadcast_to(rows[s][:, where:where + 1], (8, 128))

    n = CASES
    mats = []
    for matrix in range(4):
        m = {}
        for i in range(n):
            for j in range(i + 1):
                m[i, j] = entry(matrix, i, j)
                m[j, i] = m[i, j]
        mats.append(m)
    mg, mh, mp, mj = mats

    lo1, inv1 = cholesky(mg, n)
    zh = [forward(lo1, inv1, [mh[i, j] for i in range(n)], n) for j in range(n)]
    zp = [forward(lo1, inv1, [mp[i, j] for i in range(n)], n) for j in range(n)]
    th = [backward(lo1, inv1, zh[j], n) for j in range(n)]
    al = [backward(lo1, inv1, zp[j], n) for j in range(n)]
    schur, right = {}, []
    for j in range(n):
        col = []
        for i in range(n):
            t = mg[i, j]
            for k in range(n):
                t = t - zh[i][k] * zp[j][k]
            col.append(t)
            if i >= j:
                t = mj[i, j]
                for k in range(n):
                    t = t - zh[i][k] * zh[j][k]
                schur[i, j] = t
        right.append(col)
    lo2, inv2 = cholesky(schur, n)
    cb = [backward(lo2, inv2, forward(lo2, inv2, right[j], n), n) for j in range(n)]
    ca = []
    for j in range(n):
        col = []
        for i in range(n):
            t = al[j][i]
            for k in range(n):
                t = t - th[k][i] * cb[j][k]
            col.append(t)
        ca.append(col)

    mark('combine')
    wait_in(None, 20, view(yb, oz))
    for comp in range(3):
        for p in range(2):
            s = scl[p, pl.ds(4 * gz, 8, stride=8), :]
            fr, fi, fy = [], [], []
            for j in range(n):
                core, k = divmod(j, HALF)
                pick = pl.ds(4 * gz + k, 8, stride=8)
                fr.append(rb[core, comp, p, pick, :])
                fi.append(ib[core, comp, p, pick, :])
                fy.append(yb[core, comp, p, pick, :])
            for i in range(n):
                up = fr[0] * ca[i][0] + fi[0] * cb[i][0]
                dn = fi[0] * ca[i][0] + fy[0] * cb[i][0]
                for j in range(1, n):
                    up = up + fr[j] * ca[i][j] + fi[j] * cb[i][j]
                    dn = dn + fi[j] * ca[i][j] + fy[j] * cb[i][j]
                xout[i, comp, p] = s * up
                rout[i, comp, p] = (fr[i] - dn) + xin[i, comp, p]
        for i, (src, dst) in enumerate(((xout, xo_hbm), (rout, ro_hbm))):
            pltpu.make_async_copy(src.at[:, comp], dst.at[:, comp], out_sem.at[i]).start()
    mark('drain')
    sent_halos(u2)
    wait_out(None, 8, view(yb, gz))
    wait_out(None, 9, view(ib, gz))
    wait_out(None, 10, view(ag, pl.ds(0, 2 * ny - 1)))
    wait_out(None, 11, view(bg, pl.ds(0, nx - 1)))
    for i, (src, dst) in enumerate(((xout, xo_hbm), (rout, ro_hbm))):
        pltpu.make_async_copy(src, dst, out_sem.at[i]).wait()
    mark(None)


def shards(design, supports, body_load, start, load_nodes, load_values):
    nx, ny = lax.axis_size("gx"), lax.axis_size("gy")
    block = body_load.shape
    vmem = lambda *shape: pltpu.VMEM(shape, f32)
    spec = pl.BlockSpec(memory_space=pl.ANY)
    scratch = [
        vmem(*block), vmem(*block), pltpu.VMEM(design.shape, jnp.int32), pltpu.VMEM(design.shape, jnp.int32),
        vmem(2, 6, 24, 128), vmem(2, 2, 2, 16, 128), vmem(4, 8, 128), vmem(2, 6, 24, 128),
        vmem(12, 64, 128), vmem(8, 32, 128), vmem(2, 5, 8, 128), vmem(6, 64, 128),
        vmem(3, 4, 10, 8, 128), vmem(3, 4, 10, 8, 128), vmem(3, 4, 10, 8, 128),
        vmem(9, 3, 8, 128), vmem(2, 64, 128), vmem(2, 64, 128),
        vmem(2, 3, 2, 64, 128), vmem(2, 3, 2, 64, 128), vmem(2, 3, 2, 64, 128),
        vmem(128, 128), vmem(2 * ny, 1, 128), vmem(nx, 2, 128), vmem(176, 128), vmem(*block), vmem(*block),
        pltpu.SMEM(load_nodes.shape, jnp.int32), pltpu.SMEM((CASES, 3, LOADS), f32),
        pltpu.SemaphoreType.DMA((6,)), pltpu.SemaphoreType.DMA((2,)), pltpu.SemaphoreType.DMA((12,)), pltpu.SemaphoreType.DMA((27,)),
        pltpu.SemaphoreType.REGULAR((14,)),
    ]
    out = jax.ShapeDtypeStruct(block, f32)
    change, shifted = pl.pallas_call(
        functools.partial(kernel, nx, ny),
        out_shape=(out, out),
        in_specs=[spec] * 6,
        out_specs=(spec, spec),
        scratch_shapes=scratch,
        compiler_params=pltpu.CompilerParams(collective_id=0, has_side_effects=True),
    )(load_nodes, jnp.transpose(load_values, (0, 2, 1)), start, body_load, design, supports)

    return start + change, shifted - start


def solution(mesh):
    in_specs = (
        P(("grp", "gx"), "gy", "gz"),
        P(("grp", "gx"), "gy", "gz"),
        P("grp", None, "gx", "gy", "gz"),
        P("grp", None, "gx", "gy", "gz"),
        P("grp", None),
        P("grp", None, None),
    )
    out_specs = (P("grp", None, "gx", "gy", "gz"), P("grp", None, "gx", "gy", "gz"))
    return jax.shard_map(shards, mesh=mesh, in_specs=in_specs, out_specs=out_specs, check_vma=False)
```

```python
import functools

import jax
import jax.numpy as jnp
from jax import lax
from jax.experimental import pallas as pl
from jax.experimental.pallas import tpu as pltpu
from jax.sharding import PartitionSpec as P

LEVELS = 16
CASES = 6
LOADS = 16
HALF = 3
soft_modulus = 0.05
poisson_ratio = 0.3
LAM = poisson_ratio / ((1.0 + poisson_ratio) * (1.0 - 2.0 * poisson_ratio))
MU = 1.0 / (2.0 * (1.0 + poisson_ratio))
C11 = LAM + 2.0 * MU
RHO = LAM / MU
KAP = C11 / MU + 1.0
K00 = (C11 + 2.0 * MU) / 9.0
MESH = pl.DeviceIdType.MESH
f32 = jnp.float32


def masks():
    lane = lax.broadcasted_iota(jnp.int32, (8, 128), 1)
    sub = lax.broadcasted_iota(jnp.int32, (8, 128), 0)
    return lane, sub


def z_up(v, lane, sub):
    nd = v.ndim
    sh = pltpu.roll(v, 127, axis=nd - 1)
    fx = pltpu.roll(sh, 4, axis=nd - 2)
    return jnp.where(lane == 127, jnp.where(sub < 4, fx, 0.0), sh)


def z_dn(v, lane, sub):
    nd = v.ndim
    sh = pltpu.roll(v, 1, axis=nd - 1)
    fx = pltpu.roll(sh, 4, axis=nd - 2)
    return jnp.where(lane == 0, jnp.where(sub >= 4, fx, 0.0), sh)


def modal(a, em):
    X, Y, Z = 0, 1, 2
    g = {}
    tr = RHO * (a[X, 1, 0, 0] + a[Y, 0, 1, 0] + a[Z, 0, 0, 1])
    for key in ((X, 1, 0, 0), (Y, 0, 1, 0), (Z, 0, 0, 1)):
        g[key] = em * (a[key] + a[key] + tr)
    for p, q in (
        ((X, 0, 1, 0), (Y, 1, 0, 0)),
        ((X, 0, 0, 1), (Z, 1, 0, 0)),
        ((Y, 0, 0, 1), (Z, 0, 1, 0)),
    ):
        g[p] = g[q] = em * (a[p] + a[q])
    e2 = em * (1.0 / 3.0)
    ek = em * (KAP / 3.0)
    er = em * (RHO / 3.0)
    for p, q in (
        ((X, 1, 1, 0), (Z, 0, 1, 1)),
        ((X, 1, 0, 1), (Y, 0, 1, 1)),
        ((Y, 1, 1, 0), (Z, 1, 0, 1)),
    ):
        g[p] = ek * a[p] + er * a[q]
        g[q] = ek * a[q] + er * a[p]
    three = ((X, 0, 1, 1), (Y, 1, 0, 1), (Z, 1, 1, 0))
    total = a[three[0]] + a[three[1]] + a[three[2]]
    for key in three:
        g[key] = e2 * (a[key] + total)
    e3 = em * ((C11 / MU + 2.0) / 9.0)
    for c in range(3):
        g[c, 1, 1, 1] = e3 * a[c, 1, 1, 1]
    return g


class Stiffness:
    def __init__(self, planes, em_at, emit, lane, sub):
        self.planes, self.em_at, self.emit, self.lane, self.sub = planes, em_at, emit, lane, sub
        self.nodes, self.fields_, self.middles, self.elements = {}, {}, {}, {}

    def node(self, r, which):
        if (r, which) not in self.nodes:
            zs = []
            for c in range(3):
                v = self.planes(c, r, which)
                w = z_up(v, self.lane, self.sub)
                zs.append((v + w, w - v))
            self.nodes[r, which] = zs
        return self.nodes[r, which]

    def fields(self, j, which):
        if (j, which) not in self.fields_:
            low_row, high_row = self.node(j, which), self.node(j + 1, which)
            f = {}
            for c in range(3):
                for z in (0, 1):
                    lo, hi = low_row[c][z], high_row[c][z]
                    f[c, 0, z], f[c, 1, z] = lo + hi, hi - lo
            self.fields_[j, which] = f
        return self.fields_[j, which]

    def middle(self, j):
        if j not in self.middles:
            a = {}
            for (c, y, z), f in self.fields(j, "own").items():
                a[c, 1, y, z] = f[1] - f[0]
                if y or z:
                    a[c, 0, y, z] = f[0] + f[1]
            g = modal(a, self.em_at(j, 1))
            parts = {}
            for c, y, z in self.fields(j, "own"):
                gd = g[c, 1, y, z]
                if y or z:
                    gs = g[c, 0, y, z]
                    parts[c, y, z] = gs - gd, gs + gd
                else:
                    parts[c, y, z] = -gd, gd
            self.middles[j] = parts
        return self.middles[j]

    def begin(self):
        for j in range(1, 8):
            self.middle(j)

    def element(self, j):
        if j not in self.elements:
            own, outer, parts = self.fields(j, "own"), self.fields(j, "outer"), self.middle(j)
            a = {}
            for c, y, z in own:
                fo, fh = own[c, y, z], outer[c, y, z]
                a[c, 1, y, z] = jnp.stack([fo[0] - fh[0], fh[1] - fo[1]])
                if y or z:
                    a[c, 0, y, z] = fo + fh
            g = modal(a, self.em_at(j, 0, 2))
            h = {}
            for c, y, z in own:
                p1, p2 = parts[c, y, z]
                gd = g[c, 1, y, z]
                if y or z:
                    gs = g[c, 0, y, z]
                    p1, p2 = p1 + gs[0], p2 + gs[1]
                h[c, y, z] = jnp.stack([p1 + gd[0], p2 - gd[1]])
            lows = [[h[c, 0, z] - h[c, 1, z] for z in (0, 1)] for c in range(3)]
            highs = [[h[c, 0, z] + h[c, 1, z] for z in (0, 1)] for c in range(3)]
            self.elements[j] = lows, highs
        return self.elements[j]

    def rows(self, *ys):
        for y in ys:
            highs, lows = self.element(y)[1], self.element(y + 1)[0]
            out = []
            for c in range(3):
                ks = highs[c][0] + lows[c][0]
                kd = highs[c][1] + lows[c][1]
                out.append((ks - kd) + z_dn(ks + kd, self.lane, self.sub))
            self.emit(y, out)


def cyc1(v, sub):
    return jnp.where(sub % 4 == 2, pltpu.roll(v, 2, axis=v.ndim - 2), pltpu.roll(v, 7, axis=v.ndim - 2))


def cyc2(v, sub):
    return jnp.where(sub % 4 == 0, pltpu.roll(v, 6, axis=v.ndim - 2), pltpu.roll(v, 1, axis=v.ndim - 2))


def pair_products(own_x, other_x, own_y, sub):
    return [
        own_x * own_y,
        cyc1(own_x, sub) * own_y,
        other_x * own_y,
        cyc1(other_x, sub) * own_y,
        cyc2(other_x, sub) * own_y,
    ]


def cholesky(m, n):
    low = {}
    inv = {}
    for j in range(n):
        s = m[j, j]
        for k in range(j):
            s = s - low[j, k] * low[j, k]
        inv[j] = lax.rsqrt(s)
        for i in range(j + 1, n):
            t = m[i, j]
            for k in range(j):
                t = t - low[i, k] * low[j, k]
            low[i, j] = t * inv[j]
    return low, inv


def forward(low, inv, rhs, n):
    out = []
    for i in range(n):
        t = rhs[i]
        for k in range(i):
            t = t - low[i, k] * out[k]
        out.append(t * inv[i])
    return out


def backward(low, inv, rhs, n):
    out = [None] * n
    for i in reversed(range(n)):
        t = rhs[i]
        for k in range(i + 1, n):
            t = t - low[k, i] * out[k]
        out[i] = t * inv[i]
    return out


def kernel(
    nx, ny,
    n_hbm, v_hbm, x_hbm, b_hbm, d_hbm, s_hbm,
    xo_hbm, ro_hbm,
    xin, bin_, din, sin, xm, ysend, esend, qs,
    nat, yrow, enat, qnat,
    u0, u1, u2, em, mob, scl, rb, ib, yb, ga, ag, bg, dummy, xout, rout, nodes, vals,
    in_sem, out_sem, ss, rs, heard,
):
    grp, gx, gy, gz = (lax.axis_index(a) for a in ("grp", "gx", "gy", "gz"))
    oz = 1 - gz
    lane, sub = masks()
    valid = sub % 4 < 3
    scope = [None]

    def mark(name):
        if scope[0] is not None:
            scope[0].__exit__(None, None, None)
        scope[0] = None
        if name is not None:
            scope[0] = jax.named_scope(name)
            scope[0].__enter__()

    mark('entry')

    loads = [
        pltpu.make_async_copy(src, dst, in_sem.at[i])
        for i, (src, dst) in enumerate(((d_hbm, din), (s_hbm, sin), (x_hbm, xin), (b_hbm, bin_), (n_hbm, nodes), (v_hbm, vals)))
    ]
    for load in loads:
        load.start()

    barrier = pltpu.get_barrier_semaphore()

    def greet(cx, cy, cz):
        pl.semaphore_signal(barrier, inc=1, device_id=(grp, cx, cy, cz), device_id_type=MESH)

    exists = {}
    for dx in (-1, 0, 1):
        for dy in (-1, 0, 1):
            conds = []
            if dx:
                conds.append(gx > 0 if dx < 0 else gx < nx - 1)
            if dy:
                conds.append(gy > 0 if dy < 0 else gy < ny - 1)
            if conds:
                exists[dx, dy] = functools.reduce(jnp.logical_and, conds)

    def greet_if(here, targets):
        @pl.when(here)
        def _():
            for target in targets:
                greet(*target)

    bottom = gx == 0
    expected = bottom.astype(jnp.int32)
    for dy in (-1, 0, 1):
        greet_if(exists[1, dy], [(gx + 1, gy + dy, core) for core in (0, 1)])
        expected = expected + 2 * exists[-1, dy].astype(jnp.int32)
        if dy:
            here = jnp.logical_and(bottom, exists[0, dy])
            greet_if(here, [(gx, gy + dy, core) for core in (0, 1)])
            expected = expected + 2 * here.astype(jnp.int32)
        else:
            greet_if(bottom, [(gx, gy, oz)])

    def signal(index, cx, cy, cz):
        pl.semaphore_signal(heard.at[index], inc=1, device_id=(grp, cx, cy, cz), device_id_type=MESH)

    def signal_if(here, index, cx, cy, cz):
        pl.when(here)(lambda: signal(index, cx, cy, cz))

    def count_of(*conds):
        return sum(c.astype(jnp.int32) for c in conds)

    def wait_heard(index, each, *conds):
        @pl.when(functools.reduce(jnp.logical_or, conds))
        def _():
            pl.semaphore_wait(heard.at[index], each * count_of(*conds))

    def tell_y(k):
        step = 2**k
        if step < ny:
            signal_if(gy + step < ny, 1 + k, gx, gy + step, gz)
            signal_if(gy >= step, 1 + k, gx, gy - step, gz)

    def hear_y(k):
        step = 2**k
        if step < ny:
            wait_heard(1 + k, 1, gy + step < ny, gy >= step)

    def tell_x(k):
        step = 2**k
        if step < nx:
            signal_if(gx + step < nx, 4 + k, gx + step, gy, gz)
            signal_if(gx >= step, 8 + k, gx - step, gy, gz)

    def hear_x(k, below=True, above=True):
        step = 2**k
        if step < nx:
            if below:
                wait_heard(4 + k, 1, gx >= step)
            if above:
                wait_heard(8 + k, 1, gx + step < nx)

    def clear(ref, *index):
        ref[index] = jnp.zeros(ref[index].shape, f32)

    full = slice(None)

    @pl.when(gx == 0)
    def _():
        clear(nat, pl.ds(0, 3))
        clear(enat, full, 0)
        for side in (0, 4):
            clear(yrow, side)
        for u in (u1, u2):
            clear(u, full, 0)

    @pl.when(gx == nx - 1)
    def _():
        clear(nat, pl.ds(9, 3))
        for side in (0, 4):
            clear(yrow, side + 3)
        for u in (u1, u2):
            clear(u, full, 3)

    @pl.when(gy == 0)
    def _():
        clear(yrow, pl.ds(0, 4))
        for u in (u1, u2):
            clear(u, full, full, 0)

    @pl.when(gy == ny - 1)
    def _():
        clear(yrow, pl.ds(4, 4))
        for u in (u1, u2):
            clear(u, full, full, 9)

    mark('barrier')
    pl.semaphore_wait(barrier, expected)
    for dy in (0, -1, 1):

        @pl.when(exists[-1, dy])
        def _(dy=dy):
            for core in (0, 1):
                signal(13 if dy else 0, gx - 1, gy + dy, core)

    mark('prep')
    loads[0].wait()
    loads[1].wait()
    mnat = []
    for p in range(2):
        density = (din[p].astype(f32) + 1.0) * (1.0 / LEVELS)
        modulus = soft_modulus + (1.0 - soft_modulus) * density * density * density
        movable = 1.0 - sin[p].astype(f32)
        esend[p] = modulus
        esend[2 + p] = movable
        enat[gz, 1 + p] = modulus
        enat[gz, 3 + p] = movable
        mnat.append(movable)
    loads[2].wait()
    for side in range(2):
        for core in range(2):
            for p in range(2):
                ysend[side, core, p, 8:16] = jnp.zeros((8, 128), f32)
                if side == 1:
                    ysend[side, core, p, 12:13] = esend[p, 7:8]
    for case in range(CASES):
        core, k = divmod(case, HALF)
        for comp in range(3):
            for p in range(2):
                t = mnat[p] * xin[case, comp, p]
                xm[core, p * 3 + comp, 8 * k:8 * k + 8] = t
                for side, y in ((0, 0), (1, 7)):
                    ysend[side, core, p, 4 * k + comp:4 * k + comp + 1] = t[y:y + 1]

    mark('send1')

    def view(ref, *index):
        return ref, index

    def descriptor(src, dst, send_index, recv_index, device):
        (a, i), (b, j) = src, dst
        return pltpu.make_async_remote_copy(
            src_ref=a.at[i] if i else a, dst_ref=b.at[j] if j else b,
            send_sem=ss.at[send_index], recv_sem=rs.at[recv_index],
            device_id=device, device_id_type=MESH,
        )

    def guarded_by(cond, go):
        if cond is None:
            go()
        else:
            pl.when(cond)(go)

    def exchange(cond, send_index, recv_index, items):
        def go():
            for src, dst, device in items:
                descriptor(src, dst, send_index, recv_index, device).start()

        guarded_by(cond, go)

    def wait_in(cond, index, ref):
        guarded_by(cond, lambda: descriptor(ref, ref, 0, index, partner).wait_recv())

    def wait_out(cond, index, ref):
        guarded_by(cond, lambda: descriptor(ref, ref, index, 0, partner).wait_send())

    def rows_of(count):
        return view(dummy, pl.ds(0, count))

    slot = {key: i for i, key in enumerate(exists)}
    partner = (grp, gx, gy, oz)

    half_rows = pl.ds(pl.multiple_of(32 * gz, 8), 24)
    half_16 = pl.ds(pl.multiple_of(16 * gz, 8), 16)
    other_rows = pl.ds(pl.multiple_of(32 * oz, 8), 24)
    bytes1 = {}

    def send_start(key):
        dx, dy = key
        items, count = [], 0
        p, there_p = (1, 0) if dx > 0 else (0, 3)
        side, there = (1, 0) if dy > 0 else (0, 1)
        for core in (0, 1):
            device = (grp, gx + dx, gy + dy, core)
            if dy == 0:
                items.append((view(xm, core, pl.ds(3 * p, 3)), view(nat, pl.ds(3 * there_p, 3), half_rows), device))
                count += 72
                if dx > 0:
                    items.append((view(esend, pl.ds(1, 1)), view(enat, gz, pl.ds(0, 1)), device))
                    count += 8
            elif dx == 0:
                items.append((view(ysend, side, core), view(yrow, pl.ds(4 * there + 1, 2), half_16), device))
                count += 32
            else:
                items.append((view(ysend, side, core, p), view(yrow, 4 * there + there_p, half_16), device))
                count += 16
        exchange(exists[key], slot[key], slot[key], items)
        bytes1[key] = count

    order = sorted(exists, key=lambda k: (k[1] == 0, -abs(k[0])))
    for key in order:
        if key[0] < 0:
            send_start(key)
    mark('points')
    for load in loads[3:]:
        load.wait()
    across_z = 128 * 2
    across_y = 8 * ny * across_z
    number = (gy * 8 + sub) * across_z + gz * 128 + lane + (gx * 2) * across_y
    numbers = (number, number + across_y)

    def add_points(l, acc):
        acc = list(acc)
        for case in range(CASES):
            node = nodes[case, l]
            for p in range(2):
                hit = numbers[p] == node
                for comp in range(3):
                    at = (case * 2 + p) * 3 + comp
                    acc[at] = acc[at] + jnp.where(hit, vals[case, comp, l], 0.0)
        return tuple(acc)

    zero = jnp.zeros((8, 128), f32)
    points = lax.fori_loop(0, LOADS, add_points, (zero,) * (CASES * 6))
    for case in range(CASES):
        core, k = divmod(case, HALF)
        for p in range(2):
            m = mnat[p]
            for comp in range(3):
                total = bin_[case, comp, p] + points[(case * 2 + p) * 3 + comp]
                qs[core, p * 3 + comp, 8 * k:8 * k + 8] = m * total - (1.0 - m) * xin[case, comp, p]
    for k in range(6):
        nat[3 + k, half_rows] = xm[gz, k]
        qnat[k, half_rows] = qs[gz, k]

    mark('above')
    wait_heard(0, 2, exists[1, 0])
    send_start((1, 0))
    wait_heard(13, 2, exists[1, -1], exists[1, 1])
    signal_if(gx < nx - 1, 12, gx + 1, gy, gz)
    send_start((1, -1))
    send_start((1, 1))
    wait_heard(12, 1, gx > 0)
    for key in order:
        if key[0] == 0:
            send_start(key)
    exchange(None, 8, 16, [
        (view(xm, oz), view(nat, pl.ds(3, 6), half_rows), partner),
        (view(esend), view(enat, gz, pl.ds(1, 4)), partner),
    ])
    exchange(None, 9, 17, [(view(qs, oz), view(qnat, full, half_rows), partner)])
    tell_x(0)
    tell_y(0)
    mark('wait1')
    wait_in(None, 16, rows_of(176))
    low = sub < 4

    def spread(ref, k, y):
        return jnp.where(low, ref[0, k, y:y + 1], ref[1, k, y:y + 1])

    def at(y):
        return pl.ds(8 * y, 8)

    def start_tile(p, comp, r):
        if r in (0, 9):
            t = yrow[p + 4 * (r == 9), pl.ds(comp, 8, stride=4), :]
        else:
            t = nat[3 * p + comp, pl.ds(r - 1, 8, stride=8), :]
        u0[comp, p, r] = jnp.where(valid, t, 0.0)

    for j in range(1, 9):
        for e in (1, 2):
            em[j, e] = spread(enat, e, j - 1) * (MU / 16.0)
        mob[:, at(j - 1)] = jnp.stack([spread(enat, 3, j - 1), spread(enat, 4, j - 1)])
        for p in (1, 2):
            for comp in range(3):
                start_tile(p, comp, j)

    def em_at(j, *es):
        return em[j, es[0]] if len(es) == 1 else jnp.stack([em[j, e] for e in es])

    def planes_of(u):
        def planes(c, r, which):
            return u[c, 1:3, r] if which == "own" else jnp.stack([u[c, 0, r], u[c, 3, r]])

        return planes

    stiff = Stiffness(planes_of(u0), em_at, lambda y, force: first(y, force), lane, sub)
    stiff.begin()
    for (dx, dy), index in slot.items():
        wait_in(exists[-dx, -dy], index, rows_of(bytes1[dx, dy]))
    hear_x(0)
    tell_x(1)
    hear_y(0)
    tell_y(1)
    mark('build')

    for j in range(9):
        for e in range(3):
            if j == 0:
                em[j, e] = jnp.where(low, yrow[e, 12:13], yrow[e, 28:29]) * (MU / 16.0)
            elif e == 0:
                em[j, e] = spread(enat, e, j - 1) * (MU / 16.0)
    for y in range(8):
        rows = em[y] + em[y + 1]
        around = rows[0:2] + rows[1:3]
        esum = (around + z_dn(around, lane, sub)) * (16.0 / MU)
        m = mob[:, at(y)]
        guarded = jnp.where(m > 0, esum, 1.0)
        scl[:, at(y)] = m / (K00 * guarded) + (1.0 - m)
    for r in range(10):
        for p in range(4):
            if r in (0, 9) or p in (0, 3):
                for comp in range(3):
                    start_tile(p, comp, r)

    mark('waitq')
    wait_in(None, 17, view(qnat, full, other_rows))
    mark('k1')

    def halo_views(u, key, chunk):
        dx, dy = key
        src, dst = (2, 0) if dx > 0 else (1, 3)
        ysrc, ydst = (8, 0) if dy > 0 else (1, 9)
        if dy == 0:
            return [
                (view(u, full, src, pl.ds(k, m)), view(u, full, dst, pl.ds(k, m)))
                for k, m in (((1, 2), (7, 1)) if chunk == 0 else ((3, 3),))
            ]
        if dx == 0:
            return [(view(u, full, pl.ds(1, 2), ysrc), view(u, full, pl.ds(1, 2), ydst))]
        return [(view(u, full, src, ysrc), view(u, full, dst, ydst))]

    halo_rows = {(dx, dy): 8 * 3 * (6 if dy == 0 else 2 if dx == 0 else 1) for dx, dy in exists}

    free = sub % 4 == 3
    chunks = ((1, 2, 7, 8), (3, 4, 5, 6))

    def pack(u, chunk):
        *carriers, last = chunks[chunk]
        t = u[:, 1:3, last]
        for i, k in enumerate(carriers, 1):
            u[:, 1:3, k] = jnp.where(free, pltpu.roll(t, 4 - i, axis=2), u[:, 1:3, k])

    def unpack(u, chunk):
        *carriers, last = chunks[chunk]
        for p in (0, 3):
            a, b, c = (pltpu.roll(u[:, p, k], 4 + i, axis=1) for i, k in enumerate(carriers, 1))
            u[:, p, last] = jnp.where(sub % 4 == 0, a, jnp.where(sub % 4 == 1, b, c))

    def halo_slot(first_slot, key, chunk):
        if chunk == 0:
            return first_slot + slot[key]
        return 23 + 2 * (first_slot == 0) + (key[0] > 0)

    def send_halos(u, first_slot, chunk):
        pack(u, chunk)
        for key in order:
            dx, dy = key
            if chunk == 0 or dy == 0:
                exchange(
                    exists[key], slot[key], halo_slot(first_slot, key, chunk),
                    [(a, b, (grp, gx + dx, gy + dy, gz)) for a, b in halo_views(u, key, chunk)],
                )

    def take_halos(u, first_slot, chunk):
        for key in exists:
            dx, dy = key
            if chunk == 0 or dy == 0:
                rows = halo_rows[key] // 2 if dy == 0 else halo_rows[key]
                wait_in(exists[-dx, -dy], halo_slot(first_slot, key, chunk), rows_of(rows))
        unpack(u, chunk)

    def sent_halos(u):
        for key in exists:
            wait_out(exists[key], slot[key], rows_of(halo_rows[key]))

    def share(buf, send_index, recv_index):
        exchange(None, send_index, recv_index, [(view(buf, gz), view(buf, gz), partner)])

    def first(y, force):
        m = mob[:, at(y)]
        s = scl[:, at(y)]
        for comp in range(3):
            q = jnp.stack([qnat[3 * p + comp, pl.ds(y, 8, stride=8), :] for p in range(2)])
            res = jnp.where(valid, q, 0.0) - m * force[comp]
            rb[gz, comp, :, at(y)] = res
            u1[comp, 1:3, 1 + y] = m * (s * res)

    stiff.rows(0, 7, 1, 6)
    for key in exists:
        wait_out(exists[key], slot[key], rows_of(bytes1[key]))
    wait_out(None, 8, rows_of(176))
    send_halos(u1, 8, 0)
    stiff.rows(2, 3, 4, 5)
    send_halos(u1, 8, 1)
    share(rb, 8, 18)
    stiff = Stiffness(planes_of(u1), em_at, lambda y, force: second(y, force), lane, sub)
    stiff.begin()
    mark('wait2')
    take_halos(u1, 8, 0)
    take_halos(u1, 8, 1)
    mark('k2')

    def second(y, force):
        m = mob[:, at(y)]
        s = scl[:, at(y)]
        for comp in range(3):
            d = s * rb[gz, comp, :, at(y)]
            image = m * force[comp] + (1.0 - m) * d
            ib[gz, comp, :, at(y)] = image
            u2[comp, 1:3, 1 + y] = m * (s * image)

    stiff.rows(0, 7)
    stiff.rows(1, 6)
    sent_halos(u1)
    send_halos(u2, 0, 0)
    stiff.rows(2, 3, 4, 5)
    send_halos(u2, 0, 1)
    mark('send3')
    wait_out(None, 9, view(qs, oz))
    share(ib, 9, 19)
    hear_x(1)
    tell_x(2)
    hear_y(1)
    tell_y(2)
    wait_in(None, 18, view(rb, oz))
    wait_in(None, 19, view(ib, oz))

    mark('grams')
    def grams(make):
        acc = None
        for y in range(8):
            s = scl[:, at(y)]
            for comp in range(3):
                prods = pair_products(*make(comp, y, s), sub)
                acc = prods if acc is None else [a + b for a, b in zip(acc, prods)]
        return [a[0] + a[1] for a in acc]

    def own_other(buf, comp, y):
        return buf[gz, comp, :, at(y)], buf[oz, comp, :, at(y)]

    def make_g(comp, y, s):
        r, ro = own_other(rb, comp, y)
        return s * r, s * ro, ib[gz, comp, :, at(y)]

    def make_h(comp, y, s):
        i, io = own_other(ib, comp, y)
        return i, io, s * i

    def make_p(comp, y, s):
        r, ro = own_other(rb, comp, y)
        return r, ro, s * r

    sums = grams(make_g) + grams(make_h) + grams(make_p)

    stiff = Stiffness(planes_of(u2), em_at, lambda y, force: third(y, force), lane, sub)
    stiff.begin()
    mark('wait3')
    take_halos(u2, 0, 0)
    mark('k3')

    jacc = []

    def third(y, force):
        m = mob[:, at(y)]
        s = scl[:, at(y)]
        for comp in range(3):
            i, io = own_other(ib, comp, y)
            w = s * i
            image = m * force[comp] + (1.0 - m) * w
            yb[gz, comp, :, at(y)] = image
            prods = pair_products(w, s * io, image, sub)
            if jacc:
                jacc[0] = [a + b for a, b in zip(jacc[0], prods)]
            else:
                jacc.append(prods)

    stiff.rows(0, 7)
    take_halos(u2, 0, 1)
    stiff.rows(1, 6, 2, 3, 4, 5)
    wait_out(None, 8, view(rb, gz))
    share(yb, 8, 20)
    sums = sums + [a[0] + a[1] for a in jacc[0]]

    mark('rowsum')
    folded = [a + pltpu.roll(a, 4, axis=0) for a in sums]
    ga[pl.ds(80, 48), :] = jnp.zeros((48, 128), f32)
    for t in range(10):
        ga[pl.ds(8 * t, 8), :] = jnp.where(low, folded[2 * t], folded[2 * t + 1])
    row = lax.dot_general(
        jnp.ones((8, 128), f32), ga[...], (((1,), (1,)), ((), ())),
        precision=lax.Precision.HIGHEST, preferred_element_type=f32,
    )
    hear_y(2)
    mark('reduce_a')
    me = gz * ny + gy
    ag[me] = row[0:1]
    exchange(None, 10, 21, [
        (view(ag, me), view(ag, me), (grp, gx, lax.rem(gy + d, ny), oz if flip else gz))
        for d in sorted(range(ny), key=lambda d: -min(d, ny - d)) for flip in (0, 1) if d or flip
    ])
    hear_x(2)
    tell_x(3)
    wait_in(None, 21, view(ag, pl.ds(0, 2 * ny - 1)))
    for s in (0, 1):
        total = ag[s * ny]
        for k in range(1, ny):
            total = total + ag[s * ny + k]
        bg[gx, s:s + 1] = total
    hear_x(3, above=False)
    mark('reduce_b')
    def send_sum(target, carry):
        descriptor(view(bg, gx), view(bg, gx), 11, 22, (grp, target, gy, gz)).start()
        return carry

    lax.fori_loop(0, gx, send_sum, 0)
    hear_x(3, below=False)
    lax.fori_loop(gx + 1, nx, send_sum, 0)
    wait_in(None, 22, view(bg, pl.ds(0, nx - 1)))
    mark('solve')
    total = bg[0]
    for k in range(1, nx):
        total = total + bg[k]

    rows = [jnp.broadcast_to(total[s:s + 1], (8, 128)) for s in (0, 1)]

    def entry(matrix, i, j):
        ci, ki = divmod(i, HALF)
        cj, kj = divmod(j, HALF)
        if ci == cj:
            if (ki + 1) % 3 == kj:
                acc, k, s = 1, ki, ci
            elif ki == kj:
                acc, k, s = 0, ki, ci
            else:
                acc, k, s = 1, kj, ci
        else:
            if ci == 1:
                ki, kj = kj, ki
            acc, k, s = 2 + (kj - ki) % 3, ki, 0
        number = matrix * 5 + acc
        where = 8 * (number // 2) + 4 * (number % 2) + k
        return jnp.broadcast_to(rows[s][:, where:where + 1], (8, 128))

    n = CASES
    mats = []
    for matrix in range(4):
        m = {}
        for i in range(n):
            for j in range(i + 1):
                m[i, j] = entry(matrix, i, j)
                m[j, i] = m[i, j]
        mats.append(m)
    mg, mh, mp, mj = mats

    lo1, inv1 = cholesky(mg, n)
    zh = [forward(lo1, inv1, [mh[i, j] for i in range(n)], n) for j in range(n)]
    zp = [forward(lo1, inv1, [mp[i, j] for i in range(n)], n) for j in range(n)]
    th = [backward(lo1, inv1, zh[j], n) for j in range(n)]
    al = [backward(lo1, inv1, zp[j], n) for j in range(n)]
    schur, right = {}, []
    for j in range(n):
        col = []
        for i in range(n):
            t = mg[i, j]
            for k in range(n):
                t = t - zh[i][k] * zp[j][k]
            col.append(t)
            if i >= j:
                t = mj[i, j]
                for k in range(n):
                    t = t - zh[i][k] * zh[j][k]
                schur[i, j] = t
        right.append(col)
    lo2, inv2 = cholesky(schur, n)
    cb = [backward(lo2, inv2, forward(lo2, inv2, right[j], n), n) for j in range(n)]
    ca = []
    for j in range(n):
        col = []
        for i in range(n):
            t = al[j][i]
            for k in range(n):
                t = t - th[k][i] * cb[j][k]
            col.append(t)
        ca.append(col)

    mark('combine')
    wait_in(None, 20, view(yb, oz))
    for comp in range(3):
        for p in range(2):
            s = scl[p, pl.ds(4 * gz, 8, stride=8), :]
            fr, fi, fy = [], [], []
            for j in range(n):
                core, k = divmod(j, HALF)
                pick = pl.ds(4 * gz + k, 8, stride=8)
                fr.append(rb[core, comp, p, pick, :])
                fi.append(ib[core, comp, p, pick, :])
                fy.append(yb[core, comp, p, pick, :])
            for i in range(n):
                up = fr[0] * ca[i][0] + fi[0] * cb[i][0]
                dn = fi[0] * ca[i][0] + fy[0] * cb[i][0]
                for j in range(1, n):
                    up = up + fr[j] * ca[i][j] + fi[j] * cb[i][j]
                    dn = dn + fi[j] * ca[i][j] + fy[j] * cb[i][j]
                xout[i, comp, p] = s * up
                rout[i, comp, p] = (fr[i] - dn) + xin[i, comp, p]
        for i, (src, dst) in enumerate(((xout, xo_hbm), (rout, ro_hbm))):
            pltpu.make_async_copy(src.at[:, comp], dst.at[:, comp], out_sem.at[i]).start()
    mark('drain')
    sent_halos(u2)
    wait_out(None, 8, view(yb, gz))
    wait_out(None, 9, view(ib, gz))
    wait_out(None, 10, view(ag, pl.ds(0, 2 * ny - 1)))
    wait_out(None, 11, view(bg, pl.ds(0, nx - 1)))
    for i, (src, dst) in enumerate(((xout, xo_hbm), (rout, ro_hbm))):
        pltpu.make_async_copy(src, dst, out_sem.at[i]).wait()
    mark(None)


def shards(design, supports, body_load, start, load_nodes, load_values):
    nx, ny = lax.axis_size("gx"), lax.axis_size("gy")
    block = body_load.shape
    vmem = lambda *shape: pltpu.VMEM(shape, f32)
    spec = pl.BlockSpec(memory_space=pl.ANY)
    scratch = [
        vmem(*block), vmem(*block), pltpu.VMEM(design.shape, jnp.int32), pltpu.VMEM(design.shape, jnp.int32),
        vmem(2, 6, 24, 128), vmem(2, 2, 2, 16, 128), vmem(4, 8, 128), vmem(2, 6, 24, 128),
        vmem(12, 64, 128), vmem(8, 32, 128), vmem(2, 5, 8, 128), vmem(6, 64, 128),
        vmem(3, 4, 10, 8, 128), vmem(3, 4, 10, 8, 128), vmem(3, 4, 10, 8, 128),
        vmem(9, 3, 8, 128), vmem(2, 64, 128), vmem(2, 64, 128),
        vmem(2, 3, 2, 64, 128), vmem(2, 3, 2, 64, 128), vmem(2, 3, 2, 64, 128),
        vmem(128, 128), vmem(2 * ny, 1, 128), vmem(nx, 2, 128), vmem(176, 128), vmem(*block), vmem(*block),
        pltpu.SMEM(load_nodes.shape, jnp.int32), pltpu.SMEM((CASES, 3, LOADS), f32),
        pltpu.SemaphoreType.DMA((6,)), pltpu.SemaphoreType.DMA((2,)), pltpu.SemaphoreType.DMA((12,)), pltpu.SemaphoreType.DMA((27,)),
        pltpu.SemaphoreType.REGULAR((14,)),
    ]
    out = jax.ShapeDtypeStruct(block, f32)
    change, shifted = pl.pallas_call(
        functools.partial(kernel, nx, ny),
        out_shape=(out, out),
        in_specs=[spec] * 6,
        out_specs=(spec, spec),
        scratch_shapes=scratch,
        compiler_params=pltpu.CompilerParams(collective_id=0, has_side_effects=True),
    )(load_nodes, jnp.transpose(load_values, (0, 2, 1)), start, body_load, design, supports)

    return start + change, shifted - start


def solution(mesh):
    in_specs = (
        P(("grp", "gx"), "gy", "gz"),
        P(("grp", "gx"), "gy", "gz"),
        P("grp", None, "gx", "gy", "gz"),
        P("grp", None, "gx", "gy", "gz"),
        P("grp", None),
        P("grp", None, None),
    )
    out_specs = (P("grp", None, "gx", "gy", "gz"), P("grp", None, "gx", "gy", "gz"))
    return jax.shard_map(shards, mesh=mesh, in_specs=in_specs, out_specs=out_specs, check_vma=False)
```

```python
import functools

import jax
import jax.numpy as jnp
from jax import lax
from jax.experimental import pallas as pl
from jax.experimental.pallas import tpu as pltpu
from jax.sharding import PartitionSpec as P

LEVELS = 16
CASES = 6
LOADS = 16
HALF = 3
soft_modulus = 0.05
poisson_ratio = 0.3
LAM = poisson_ratio / ((1.0 + poisson_ratio) * (1.0 - 2.0 * poisson_ratio))
MU = 1.0 / (2.0 * (1.0 + poisson_ratio))
C11 = LAM + 2.0 * MU
RHO = LAM / MU
KAP = C11 / MU + 1.0
K00 = (C11 + 2.0 * MU) / 9.0
MESH = pl.DeviceIdType.MESH
f32 = jnp.float32


def masks():
    lane = lax.broadcasted_iota(jnp.int32, (8, 128), 1)
    sub = lax.broadcasted_iota(jnp.int32, (8, 128), 0)
    return lane, sub


def z_up(v, lane, sub):
    nd = v.ndim
    sh = pltpu.roll(v, 127, axis=nd - 1)
    fx = pltpu.roll(sh, 4, axis=nd - 2)
    return jnp.where(lane == 127, jnp.where(sub < 4, fx, 0.0), sh)


def z_dn(v, lane, sub):
    nd = v.ndim
    sh = pltpu.roll(v, 1, axis=nd - 1)
    fx = pltpu.roll(sh, 4, axis=nd - 2)
    return jnp.where(lane == 0, jnp.where(sub >= 4, fx, 0.0), sh)


def modal(a, em):
    X, Y, Z = 0, 1, 2
    g = {}
    tr = RHO * (a[X, 1, 0, 0] + a[Y, 0, 1, 0] + a[Z, 0, 0, 1])
    for key in ((X, 1, 0, 0), (Y, 0, 1, 0), (Z, 0, 0, 1)):
        g[key] = em * (a[key] + a[key] + tr)
    for p, q in (
        ((X, 0, 1, 0), (Y, 1, 0, 0)),
        ((X, 0, 0, 1), (Z, 1, 0, 0)),
        ((Y, 0, 0, 1), (Z, 0, 1, 0)),
    ):
        g[p] = g[q] = em * (a[p] + a[q])
    e2 = em * (1.0 / 3.0)
    ek = em * (KAP / 3.0)
    er = em * (RHO / 3.0)
    for p, q in (
        ((X, 1, 1, 0), (Z, 0, 1, 1)),
        ((X, 1, 0, 1), (Y, 0, 1, 1)),
        ((Y, 1, 1, 0), (Z, 1, 0, 1)),
    ):
        g[p] = ek * a[p] + er * a[q]
        g[q] = ek * a[q] + er * a[p]
    three = ((X, 0, 1, 1), (Y, 1, 0, 1), (Z, 1, 1, 0))
    total = a[three[0]] + a[three[1]] + a[three[2]]
    for key in three:
        g[key] = e2 * (a[key] + total)
    e3 = em * ((C11 / MU + 2.0) / 9.0)
    for c in range(3):
        g[c, 1, 1, 1] = e3 * a[c, 1, 1, 1]
    return g


class Stiffness:
    def __init__(self, planes, em_at, emit, lane, sub):
        self.planes, self.em_at, self.emit, self.lane, self.sub = planes, em_at, emit, lane, sub
        self.nodes, self.fields_, self.middles, self.elements = {}, {}, {}, {}

    def node(self, r, which):
        if (r, which) not in self.nodes:
            zs = []
            for c in range(3):
                v = self.planes(c, r, which)
                w = z_up(v, self.lane, self.sub)
                zs.append((v + w, w - v))
            self.nodes[r, which] = zs
        return self.nodes[r, which]

    def fields(self, j, which):
        if (j, which) not in self.fields_:
            low_row, high_row = self.node(j, which), self.node(j + 1, which)
            f = {}
            for c in range(3):
                for z in (0, 1):
                    lo, hi = low_row[c][z], high_row[c][z]
                    f[c, 0, z], f[c, 1, z] = lo + hi, hi - lo
            self.fields_[j, which] = f
        return self.fields_[j, which]

    def middle(self, j):
        if j not in self.middles:
            a = {}
            for (c, y, z), f in self.fields(j, "own").items():
                a[c, 1, y, z] = f[1] - f[0]
                if y or z:
                    a[c, 0, y, z] = f[0] + f[1]
            g = modal(a, self.em_at(j, 1))
            parts = {}
            for c, y, z in self.fields(j, "own"):
                gd = g[c, 1, y, z]
                if y or z:
                    gs = g[c, 0, y, z]
                    parts[c, y, z] = gs - gd, gs + gd
                else:
                    parts[c, y, z] = -gd, gd
            self.middles[j] = parts
        return self.middles[j]

    def begin(self):
        for j in range(1, 8):
            self.middle(j)

    def element(self, j):
        if j not in self.elements:
            own, outer, parts = self.fields(j, "own"), self.fields(j, "outer"), self.middle(j)
            a = {}
            for c, y, z in own:
                fo, fh = own[c, y, z], outer[c, y, z]
                a[c, 1, y, z] = jnp.stack([fo[0] - fh[0], fh[1] - fo[1]])
                if y or z:
                    a[c, 0, y, z] = fo + fh
            g = modal(a, self.em_at(j, 0, 2))
            h = {}
            for c, y, z in own:
                p1, p2 = parts[c, y, z]
                gd = g[c, 1, y, z]
                if y or z:
                    gs = g[c, 0, y, z]
                    p1, p2 = p1 + gs[0], p2 + gs[1]
                h[c, y, z] = jnp.stack([p1 + gd[0], p2 - gd[1]])
            lows = [[h[c, 0, z] - h[c, 1, z] for z in (0, 1)] for c in range(3)]
            highs = [[h[c, 0, z] + h[c, 1, z] for z in (0, 1)] for c in range(3)]
            self.elements[j] = lows, highs
        return self.elements[j]

    def rows(self, *ys):
        for y in ys:
            highs, lows = self.element(y)[1], self.element(y + 1)[0]
            out = []
            for c in range(3):
                ks = highs[c][0] + lows[c][0]
                kd = highs[c][1] + lows[c][1]
                out.append((ks - kd) + z_dn(ks + kd, self.lane, self.sub))
            self.emit(y, out)


def cyc1(v, sub):
    return jnp.where(sub % 4 == 2, pltpu.roll(v, 2, axis=v.ndim - 2), pltpu.roll(v, 7, axis=v.ndim - 2))


def cyc2(v, sub):
    return jnp.where(sub % 4 == 0, pltpu.roll(v, 6, axis=v.ndim - 2), pltpu.roll(v, 1, axis=v.ndim - 2))


def pair_products(own_x, other_x, own_y, sub):
    return [
        own_x * own_y,
        cyc1(own_x, sub) * own_y,
        other_x * own_y,
        cyc1(other_x, sub) * own_y,
        cyc2(other_x, sub) * own_y,
    ]


def cholesky(m, n):
    low = {}
    inv = {}
    for j in range(n):
        s = m[j, j]
        for k in range(j):
            s = s - low[j, k] * low[j, k]
        inv[j] = lax.rsqrt(s)
        for i in range(j + 1, n):
            t = m[i, j]
            for k in range(j):
                t = t - low[i, k] * low[j, k]
            low[i, j] = t * inv[j]
    return low, inv


def forward(low, inv, rhs, n):
    out = []
    for i in range(n):
        t = rhs[i]
        for k in range(i):
            t = t - low[i, k] * out[k]
        out.append(t * inv[i])
    return out


def backward(low, inv, rhs, n):
    out = [None] * n
    for i in reversed(range(n)):
        t = rhs[i]
        for k in range(i + 1, n):
            t = t - low[k, i] * out[k]
        out[i] = t * inv[i]
    return out


def kernel(
    nx, ny,
    n_hbm, v_hbm, x_hbm, b_hbm, d_hbm, s_hbm,
    xo_hbm, ro_hbm,
    xin, bin_, din, sin, xm, ysend, esend, qs,
    nat, yrow, enat, qnat,
    u0, u1, u2, em, mob, scl, rb, ib, yb, ga, ag, bg, ag2, bg2, vout, wout, dummy, xout, rout, nodes, vals,
    in_sem, out_sem, ss, rs, heard,
):
    grp, gx, gy, gz = (lax.axis_index(a) for a in ("grp", "gx", "gy", "gz"))
    oz = 1 - gz
    lane, sub = masks()
    valid = sub % 4 < 3
    scope = [None]

    def mark(name):
        if scope[0] is not None:
            scope[0].__exit__(None, None, None)
        scope[0] = None
        if name is not None:
            scope[0] = jax.named_scope(name)
            scope[0].__enter__()

    mark('entry')

    loads = [
        pltpu.make_async_copy(src, dst, in_sem.at[i])
        for i, (src, dst) in enumerate(((d_hbm, din), (s_hbm, sin), (x_hbm, xin), (b_hbm, bin_), (n_hbm, nodes), (v_hbm, vals)))
    ]
    for load in loads:
        load.start()

    barrier = pltpu.get_barrier_semaphore()

    def greet(cx, cy, cz):
        pl.semaphore_signal(barrier, inc=1, device_id=(grp, cx, cy, cz), device_id_type=MESH)

    exists = {}
    for dx in (-1, 0, 1):
        for dy in (-1, 0, 1):
            conds = []
            if dx:
                conds.append(gx > 0 if dx < 0 else gx < nx - 1)
            if dy:
                conds.append(gy > 0 if dy < 0 else gy < ny - 1)
            if conds:
                exists[dx, dy] = functools.reduce(jnp.logical_and, conds)

    def greet_if(here, targets):
        @pl.when(here)
        def _():
            for target in targets:
                greet(*target)

    bottom = gx == 0
    expected = bottom.astype(jnp.int32)
    for dy in (-1, 0, 1):
        greet_if(exists[1, dy], [(gx + 1, gy + dy, core) for core in (0, 1)])
        expected = expected + 2 * exists[-1, dy].astype(jnp.int32)
        if dy:
            here = jnp.logical_and(bottom, exists[0, dy])
            greet_if(here, [(gx, gy + dy, core) for core in (0, 1)])
            expected = expected + 2 * here.astype(jnp.int32)
        else:
            greet_if(bottom, [(gx, gy, oz)])

    def signal(index, cx, cy, cz):
        pl.semaphore_signal(heard.at[index], inc=1, device_id=(grp, cx, cy, cz), device_id_type=MESH)

    def signal_if(here, index, cx, cy, cz):
        pl.when(here)(lambda: signal(index, cx, cy, cz))

    def count_of(*conds):
        return sum(c.astype(jnp.int32) for c in conds)

    def wait_heard(index, each, *conds):
        @pl.when(functools.reduce(jnp.logical_or, conds))
        def _():
            pl.semaphore_wait(heard.at[index], each * count_of(*conds))

    def tell_y(k):
        step = 2**k
        if step < ny:
            signal_if(gy + step < ny, 1 + k, gx, gy + step, gz)
            signal_if(gy >= step, 1 + k, gx, gy - step, gz)

    def hear_y(k):
        step = 2**k
        if step < ny:
            wait_heard(1 + k, 1, gy + step < ny, gy >= step)

    def tell_x(k):
        step = 2**k
        if step < nx:
            signal_if(gx + step < nx, 4 + k, gx + step, gy, gz)
            signal_if(gx >= step, 8 + k, gx - step, gy, gz)

    def hear_x(k, below=True, above=True):
        step = 2**k
        if step < nx:
            if below:
                wait_heard(4 + k, 1, gx >= step)
            if above:
                wait_heard(8 + k, 1, gx + step < nx)

    def clear(ref, *index):
        ref[index] = jnp.zeros(ref[index].shape, f32)

    full = slice(None)

    @pl.when(gx == 0)
    def _():
        clear(nat, pl.ds(0, 3))
        clear(enat, full, 0)
        for side in (0, 4):
            clear(yrow, side)
        for u in (u1, u2):
            clear(u, full, 0)

    @pl.when(gx == nx - 1)
    def _():
        clear(nat, pl.ds(9, 3))
        for side in (0, 4):
            clear(yrow, side + 3)
        for u in (u1, u2):
            clear(u, full, 3)

    @pl.when(gy == 0)
    def _():
        clear(yrow, pl.ds(0, 4))
        for u in (u1, u2):
            clear(u, full, full, 0)

    @pl.when(gy == ny - 1)
    def _():
        clear(yrow, pl.ds(4, 4))
        for u in (u1, u2):
            clear(u, full, full, 9)

    mark('barrier')
    pl.semaphore_wait(barrier, expected)
    for dy in (0, -1, 1):

        @pl.when(exists[-1, dy])
        def _(dy=dy):
            for core in (0, 1):
                signal(13 if dy else 0, gx - 1, gy + dy, core)

    mark('prep')
    loads[0].wait()
    loads[1].wait()
    mnat = []
    for p in range(2):
        density = (din[p].astype(f32) + 1.0) * (1.0 / LEVELS)
        modulus = soft_modulus + (1.0 - soft_modulus) * density * density * density
        movable = 1.0 - sin[p].astype(f32)
        esend[p] = modulus
        esend[2 + p] = movable
        enat[gz, 1 + p] = modulus
        enat[gz, 3 + p] = movable
        mnat.append(movable)
    loads[2].wait()
    for side in range(2):
        for core in range(2):
            for p in range(2):
                ysend[side, core, p, 8:16] = jnp.zeros((8, 128), f32)
                if side == 1:
                    ysend[side, core, p, 12:13] = esend[p, 7:8]
    for case in range(CASES):
        core, k = divmod(case, HALF)
        for comp in range(3):
            for p in range(2):
                t = mnat[p] * xin[case, comp, p]
                xm[core, p * 3 + comp, 8 * k:8 * k + 8] = t
                for side, y in ((0, 0), (1, 7)):
                    ysend[side, core, p, 4 * k + comp:4 * k + comp + 1] = t[y:y + 1]

    mark('send1')

    def view(ref, *index):
        return ref, index

    def descriptor(src, dst, send_index, recv_index, device):
        (a, i), (b, j) = src, dst
        return pltpu.make_async_remote_copy(
            src_ref=a.at[i] if i else a, dst_ref=b.at[j] if j else b,
            send_sem=ss.at[send_index], recv_sem=rs.at[recv_index],
            device_id=device, device_id_type=MESH,
        )

    def guarded_by(cond, go):
        if cond is None:
            go()
        else:
            pl.when(cond)(go)

    def exchange(cond, send_index, recv_index, items):
        def go():
            for src, dst, device in items:
                descriptor(src, dst, send_index, recv_index, device).start()

        guarded_by(cond, go)

    def wait_in(cond, index, ref):
        guarded_by(cond, lambda: descriptor(ref, ref, 0, index, partner).wait_recv())

    def wait_out(cond, index, ref):
        guarded_by(cond, lambda: descriptor(ref, ref, index, 0, partner).wait_send())

    def rows_of(count):
        return view(dummy, pl.ds(0, count))

    slot = {key: i for i, key in enumerate(exists)}
    partner = (grp, gx, gy, oz)

    half_rows = pl.ds(pl.multiple_of(32 * gz, 8), 24)
    half_16 = pl.ds(pl.multiple_of(16 * gz, 8), 16)
    other_rows = pl.ds(pl.multiple_of(32 * oz, 8), 24)
    bytes1 = {}

    def send_start(key):
        dx, dy = key
        items, count = [], 0
        p, there_p = (1, 0) if dx > 0 else (0, 3)
        side, there = (1, 0) if dy > 0 else (0, 1)
        for core in (0, 1):
            device = (grp, gx + dx, gy + dy, core)
            if dy == 0:
                items.append((view(xm, core, pl.ds(3 * p, 3)), view(nat, pl.ds(3 * there_p, 3), half_rows), device))
                count += 72
                if dx > 0:
                    items.append((view(esend, pl.ds(1, 1)), view(enat, gz, pl.ds(0, 1)), device))
                    count += 8
            elif dx == 0:
                items.append((view(ysend, side, core), view(yrow, pl.ds(4 * there + 1, 2), half_16), device))
                count += 32
            else:
                items.append((view(ysend, side, core, p), view(yrow, 4 * there + there_p, half_16), device))
                count += 16
        exchange(exists[key], slot[key], slot[key], items)
        bytes1[key] = count

    order = sorted(exists, key=lambda k: (k[1] == 0, -abs(k[0])))
    for key in order:
        if key[0] < 0:
            send_start(key)
    mark('points')
    for load in loads[3:]:
        load.wait()
    across_z = 128 * 2
    across_y = 8 * ny * across_z
    number = (gy * 8 + sub) * across_z + gz * 128 + lane + (gx * 2) * across_y
    numbers = (number, number + across_y)

    def add_points(l, acc):
        acc = list(acc)
        for case in range(CASES):
            node = nodes[case, l]
            for p in range(2):
                hit = numbers[p] == node
                for comp in range(3):
                    at = (case * 2 + p) * 3 + comp
                    acc[at] = acc[at] + jnp.where(hit, vals[case, comp, l], 0.0)
        return tuple(acc)

    zero = jnp.zeros((8, 128), f32)
    points = lax.fori_loop(0, LOADS, add_points, (zero,) * (CASES * 6))
    for case in range(CASES):
        core, k = divmod(case, HALF)
        for p in range(2):
            m = mnat[p]
            for comp in range(3):
                total = bin_[case, comp, p] + points[(case * 2 + p) * 3 + comp]
                qs[core, p * 3 + comp, 8 * k:8 * k + 8] = m * total - (1.0 - m) * xin[case, comp, p]
    for k in range(6):
        nat[3 + k, half_rows] = xm[gz, k]
        qnat[k, half_rows] = qs[gz, k]

    mark('above')
    wait_heard(0, 2, exists[1, 0])
    send_start((1, 0))
    wait_heard(13, 2, exists[1, -1], exists[1, 1])
    signal_if(gx < nx - 1, 12, gx + 1, gy, gz)
    send_start((1, -1))
    send_start((1, 1))
    wait_heard(12, 1, gx > 0)
    for key in order:
        if key[0] == 0:
            send_start(key)
    exchange(None, 8, 16, [
        (view(xm, oz), view(nat, pl.ds(3, 6), half_rows), partner),
        (view(esend), view(enat, gz, pl.ds(1, 4)), partner),
    ])
    exchange(None, 9, 17, [(view(qs, oz), view(qnat, full, half_rows), partner)])
    tell_x(0)
    tell_y(0)
    mark('wait1')
    wait_in(None, 16, rows_of(176))
    low = sub < 4

    def spread(ref, k, y):
        return jnp.where(low, ref[0, k, y:y + 1], ref[1, k, y:y + 1])

    def at(y):
        return pl.ds(8 * y, 8)

    def start_tile(p, comp, r):
        if r in (0, 9):
            t = yrow[p + 4 * (r == 9), pl.ds(comp, 8, stride=4), :]
        else:
            t = nat[3 * p + comp, pl.ds(r - 1, 8, stride=8), :]
        u0[comp, p, r] = jnp.where(valid, t, 0.0)

    for j in range(1, 9):
        for e in (1, 2):
            em[j, e] = spread(enat, e, j - 1) * (MU / 16.0)
        mob[:, at(j - 1)] = jnp.stack([spread(enat, 3, j - 1), spread(enat, 4, j - 1)])
        for p in (1, 2):
            for comp in range(3):
                start_tile(p, comp, j)

    def em_at(j, *es):
        return em[j, es[0]] if len(es) == 1 else jnp.stack([em[j, e] for e in es])

    def planes_of(u):
        def planes(c, r, which):
            return u[c, 1:3, r] if which == "own" else jnp.stack([u[c, 0, r], u[c, 3, r]])

        return planes

    stiff = Stiffness(planes_of(u0), em_at, lambda y, force: first(y, force), lane, sub)
    stiff.begin()
    for (dx, dy), index in slot.items():
        wait_in(exists[-dx, -dy], index, rows_of(bytes1[dx, dy]))
    hear_x(0)
    tell_x(1)
    hear_y(0)
    tell_y(1)
    mark('build')

    for j in range(9):
        for e in range(3):
            if j == 0:
                em[j, e] = jnp.where(low, yrow[e, 12:13], yrow[e, 28:29]) * (MU / 16.0)
            elif e == 0:
                em[j, e] = spread(enat, e, j - 1) * (MU / 16.0)
    for y in range(8):
        rows = em[y] + em[y + 1]
        around = rows[0:2] + rows[1:3]
        esum = (around + z_dn(around, lane, sub)) * (16.0 / MU)
        m = mob[:, at(y)]
        guarded = jnp.where(m > 0, esum, 1.0)
        scl[:, at(y)] = m / (K00 * guarded) + (1.0 - m)
    for r in range(10):
        for p in range(4):
            if r in (0, 9) or p in (0, 3):
                for comp in range(3):
                    start_tile(p, comp, r)

    mark('waitq')
    wait_in(None, 17, view(qnat, full, other_rows))
    mark('k1')

    def halo_views(u, key, chunk):
        dx, dy = key
        src, dst = (2, 0) if dx > 0 else (1, 3)
        ysrc, ydst = (8, 0) if dy > 0 else (1, 9)
        if dy == 0:
            return [
                (view(u, full, src, pl.ds(k, m)), view(u, full, dst, pl.ds(k, m)))
                for k, m in ((1 + 3 * chunk, 3),)
            ]
        if dx == 0:
            return [(view(u, full, pl.ds(1, 2), ysrc), view(u, full, pl.ds(1, 2), ydst))]
        return [(view(u, full, src, ysrc), view(u, full, dst, ydst))]

    halo_rows = {(dx, dy): 8 * 3 * (6 if dy == 0 else 2 if dx == 0 else 1) for dx, dy in exists}

    free = sub % 4 == 3
    chunks = ((1, 2, 3, 8), (4, 5, 6, 7))

    def pack(u, chunk):
        *carriers, last = chunks[chunk]
        t = u[:, 1:3, last]
        for i, k in enumerate(carriers, 1):
            u[:, 1:3, k] = jnp.where(free, pltpu.roll(t, 4 - i, axis=2), u[:, 1:3, k])

    def unpack(u, chunk):
        *carriers, last = chunks[chunk]
        for p in (0, 3):
            a, b, c = (pltpu.roll(u[:, p, k], 4 + i, axis=1) for i, k in enumerate(carriers, 1))
            u[:, p, last] = jnp.where(sub % 4 == 0, a, jnp.where(sub % 4 == 1, b, c))

    def halo_slot(first_slot, key, chunk):
        if chunk == 0:
            return first_slot + slot[key]
        return 23 + 2 * (first_slot == 0) + (key[0] > 0)

    def send_halos(u, first_slot, chunk):
        pack(u, chunk)
        for key in order:
            dx, dy = key
            if chunk == 0 or dy == 0:
                exchange(
                    exists[key], slot[key], halo_slot(first_slot, key, chunk),
                    [(a, b, (grp, gx + dx, gy + dy, gz)) for a, b in halo_views(u, key, chunk)],
                )

    def take_halos(u, first_slot, chunk):
        for key in exists:
            dx, dy = key
            if chunk == 0 or dy == 0:
                rows = halo_rows[key] // 2 if dy == 0 else halo_rows[key]
                wait_in(exists[-dx, -dy], halo_slot(first_slot, key, chunk), rows_of(rows))
        unpack(u, chunk)

    def sent_halos(u):
        for key in exists:
            wait_out(exists[key], slot[key], rows_of(halo_rows[key]))

    def share(buf, send_index, recv_index):
        exchange(None, send_index, recv_index, [(view(buf, gz), view(buf, gz), partner)])

    def first(y, force):
        m = mob[:, at(y)]
        s = scl[:, at(y)]
        for comp in range(3):
            q = jnp.stack([qnat[3 * p + comp, pl.ds(y, 8, stride=8), :] for p in range(2)])
            res = jnp.where(valid, q, 0.0) - m * force[comp]
            rb[gz, comp, :, at(y)] = res
            u1[comp, 1:3, 1 + y] = m * (s * res)

    stiff.rows(0, 7, 1, 2)
    for key in exists:
        wait_out(exists[key], slot[key], rows_of(bytes1[key]))
    wait_out(None, 8, rows_of(176))
    send_halos(u1, 8, 0)
    stiff.rows(3, 4, 5, 6)
    send_halos(u1, 8, 1)
    share(rb, 8, 18)
    stiff = Stiffness(planes_of(u1), em_at, lambda y, force: second(y, force), lane, sub)
    stiff.begin()
    hear_x(1)
    tell_x(2)
    hear_y(1)
    tell_y(2)
    mark('wait2')
    take_halos(u1, 8, 0)
    take_halos(u1, 8, 1)
    mark('k2')

    def second(y, force):
        m = mob[:, at(y)]
        s = scl[:, at(y)]
        for comp in range(3):
            d = s * rb[gz, comp, :, at(y)]
            image = m * force[comp] + (1.0 - m) * d
            ib[gz, comp, :, at(y)] = image
            u2[comp, 1:3, 1 + y] = m * (s * image)

    stiff.rows(0, 7, 1, 2)
    sent_halos(u1)
    send_halos(u2, 0, 0)
    stiff.rows(3, 4, 5, 6)
    send_halos(u2, 0, 1)
    mark('send3')
    wait_out(None, 9, view(qs, oz))
    share(ib, 9, 19)
    wait_in(None, 18, view(rb, oz))
    wait_in(None, 19, view(ib, oz))

    mark('grams')
    def grams(make):
        acc = None
        for y in range(8):
            s = scl[:, at(y)]
            for comp in range(3):
                prods = pair_products(*make(comp, y, s), sub)
                acc = prods if acc is None else [a + b for a, b in zip(acc, prods)]
        return [a[0] + a[1] for a in acc]

    def own_other(buf, comp, y):
        return buf[gz, comp, :, at(y)], buf[oz, comp, :, at(y)]

    def make_g(comp, y, s):
        r, ro = own_other(rb, comp, y)
        return s * r, s * ro, ib[gz, comp, :, at(y)]

    def make_h(comp, y, s):
        i, io = own_other(ib, comp, y)
        return i, io, s * i

    def make_p(comp, y, s):
        r, ro = own_other(rb, comp, y)
        return r, ro, s * r

    me = gz * ny + gy

    def send_row(accs, rows_ref, send_index, recv_index):
        folded = [a + pltpu.roll(a, 4, axis=0) for a in accs]
        if len(folded) % 2:
            folded.append(folded[-1])
        for t in range(len(folded) // 2):
            ga[pl.ds(8 * t, 8), :] = jnp.where(low, folded[2 * t], folded[2 * t + 1])
        row = lax.dot_general(
            jnp.ones((8, 128), f32), ga[...], (((1,), (1,)), ((), ())),
            precision=lax.Precision.HIGHEST, preferred_element_type=f32,
        )
        rows_ref[me] = row[0:1]
        exchange(None, send_index, recv_index, [
            (view(rows_ref, me), view(rows_ref, me), (grp, gx, lax.rem(gy + d, ny), oz if flip else gz))
            for d in sorted(range(ny), key=lambda d: -min(d, ny - d)) for flip in (0, 1) if d or flip
        ])

    def sum_rows(rows_ref, recv_index, planes_ref):
        wait_in(None, recv_index, view(rows_ref, pl.ds(0, 2 * ny - 1)))
        for s in (0, 1):
            total = rows_ref[s * ny]
            for k in range(1, ny):
                total = total + rows_ref[s * ny + k]
            planes_ref[gx, s:s + 1] = total

    def send_planes(planes_ref, send_index, recv_index, first_plane, last_plane):
        def send_sum(target, carry):
            mine = view(planes_ref, gx)
            descriptor(mine, mine, send_index, recv_index, (grp, target, gy, gz)).start()
            return carry

        lax.fori_loop(first_plane, last_plane, send_sum, 0)

    def totals(planes_ref, recv_index):
        wait_in(None, recv_index, view(planes_ref, pl.ds(0, nx - 1)))
        total = planes_ref[0]
        for k in range(1, nx):
            total = total + planes_ref[k]
        return [jnp.broadcast_to(total[s:s + 1], (8, 128)) for s in (0, 1)]

    ga[...] = jnp.zeros_like(ga)
    hear_x(2)
    tell_x(3)
    hear_y(2)
    send_row(grams(make_g) + grams(make_h) + grams(make_p), ag2, 12, 27)

    stiff = Stiffness(planes_of(u2), em_at, lambda y, force: third(y, force), lane, sub)
    stiff.begin()
    mark('wait3')
    take_halos(u2, 0, 0)
    mark('k3')

    jacc = []

    def third(y, force):
        m = mob[:, at(y)]
        s = scl[:, at(y)]
        for comp in range(3):
            i, io = own_other(ib, comp, y)
            w = s * i
            image = m * force[comp] + (1.0 - m) * w
            yb[gz, comp, :, at(y)] = image
            prods = pair_products(w, s * io, image, sub)
            if jacc:
                jacc[0] = [a + b for a, b in zip(jacc[0], prods)]
            else:
                jacc.append(prods)

    stiff.rows(0, 1)
    take_halos(u2, 0, 1)
    stiff.rows(7, 2, 3, 4, 5, 6)
    wait_out(None, 8, view(rb, gz))
    share(yb, 8, 20)
    mark('rowsum')
    send_row([a[0] + a[1] for a in jacc[0]], ag, 10, 21)
    mark('reduce_a')
    sum_rows(ag2, 27, bg2)
    hear_x(3, above=False)
    send_planes(bg2, 13, 28, 0, gx)
    sum_rows(ag, 21, bg)
    mark('reduce_b')
    send_planes(bg, 11, 22, 0, gx)
    hear_x(3, below=False)
    send_planes(bg, 11, 22, gx + 1, nx)
    send_planes(bg2, 13, 28, gx + 1, nx)

    def entry(rows, matrix, i, j):
        ci, ki = divmod(i, HALF)
        cj, kj = divmod(j, HALF)
        if ci == cj:
            if (ki + 1) % 3 == kj:
                acc, k, s = 1, ki, ci
            elif ki == kj:
                acc, k, s = 0, ki, ci
            else:
                acc, k, s = 1, kj, ci
        else:
            if ci == 1:
                ki, kj = kj, ki
            acc, k, s = 2 + (kj - ki) % 3, ki, 0
        number = matrix * 5 + acc
        where = 8 * (number // 2) + 4 * (number % 2) + k
        return jnp.broadcast_to(rows[s][:, where:where + 1], (8, 128))

    n = CASES

    def matrix_of(rows, matrix):
        m = {}
        for i in range(n):
            for j in range(i + 1):
                m[i, j] = m[j, i] = entry(rows, matrix, i, j)
        return m

    rows = totals(bg2, 28)
    mg, mh, mp = (matrix_of(rows, matrix) for matrix in range(3))
    lo1, inv1 = cholesky(mg, n)
    zh = [forward(lo1, inv1, [mh[i, j] for i in range(n)], n) for j in range(n)]
    zp = [forward(lo1, inv1, [mp[i, j] for i in range(n)], n) for j in range(n)]
    th = [backward(lo1, inv1, zh[j], n) for j in range(n)]
    al = [backward(lo1, inv1, zp[j], n) for j in range(n)]
    right = []
    for j in range(n):
        col = []
        for i in range(n):
            t = mg[i, j]
            for k in range(n):
                t = t - zh[i][k] * zp[j][k]
            col.append(t)
        right.append(col)
    taken = {}
    for j in range(n):
        for i in range(j, n):
            t = zh[i][0] * zh[j][0]
            for k in range(1, n):
                t = t + zh[i][k] * zh[j][k]
            taken[i, j] = t

    wait_in(None, 20, view(yb, oz))
    for comp in range(3):
        for p in range(2):
            s = scl[p, pl.ds(4 * gz, 8, stride=8), :]
            fr, fi, fy = [], [], []
            for j in range(n):
                core, k = divmod(j, HALF)
                pick = pl.ds(4 * gz + k, 8, stride=8)
                fr.append(rb[core, comp, p, pick, :])
                fi.append(ib[core, comp, p, pick, :])
                fy.append(yb[core, comp, p, pick, :])
            for i in range(n):
                up, dn, v, y = fr[0] * al[i][0], fi[0] * al[i][0], fr[0] * th[i][0], fi[0] * th[i][0]
                for j in range(1, n):
                    up = up + fr[j] * al[i][j]
                    dn = dn + fi[j] * al[i][j]
                    v = v + fr[j] * th[i][j]
                    y = y + fi[j] * th[i][j]
                xout[i, comp, p] = s * up
                rout[i, comp, p] = (fr[i] - dn) + xin[i, comp, p]
                vout[i, comp, p] = s * (fi[i] - v)
                wout[i, comp, p] = fy[i] - y

    mark('solve')
    rows = totals(bg, 22)
    mj = matrix_of(rows, 0)
    schur = {key: mj[key] - t for key, t in taken.items()}
    lo2, inv2 = cholesky(schur, n)
    cb = [backward(lo2, inv2, forward(lo2, inv2, right[j], n), n) for j in range(n)]

    mark('combine')
    for comp in range(3):
        for p in range(2):
            v = [vout[j, comp, p] for j in range(n)]
            w = [wout[j, comp, p] for j in range(n)]
            for i in range(n):
                up, dn = v[0] * cb[i][0], w[0] * cb[i][0]
                for j in range(1, n):
                    up = up + v[j] * cb[i][j]
                    dn = dn + w[j] * cb[i][j]
                xout[i, comp, p] = xout[i, comp, p] + up
                rout[i, comp, p] = rout[i, comp, p] - dn
        for i, (src, dst) in enumerate(((xout, xo_hbm), (rout, ro_hbm))):
            pltpu.make_async_copy(src.at[:, comp], dst.at[:, comp], out_sem.at[i]).start()
    mark('drain')
    sent_halos(u2)
    wait_out(None, 8, view(yb, gz))
    wait_out(None, 9, view(ib, gz))
    wait_out(None, 10, view(ag, pl.ds(0, 2 * ny - 1)))
    wait_out(None, 11, view(bg, pl.ds(0, nx - 1)))
    wait_out(None, 12, view(ag2, pl.ds(0, 2 * ny - 1)))
    wait_out(None, 13, view(bg2, pl.ds(0, nx - 1)))
    for i, (src, dst) in enumerate(((xout, xo_hbm), (rout, ro_hbm))):
        pltpu.make_async_copy(src, dst, out_sem.at[i]).wait()
    mark(None)


def shards(design, supports, body_load, start, load_nodes, load_values):
    nx, ny = lax.axis_size("gx"), lax.axis_size("gy")
    block = body_load.shape
    vmem = lambda *shape: pltpu.VMEM(shape, f32)
    spec = pl.BlockSpec(memory_space=pl.ANY)
    scratch = [
        vmem(*block), vmem(*block), pltpu.VMEM(design.shape, jnp.int32), pltpu.VMEM(design.shape, jnp.int32),
        vmem(2, 6, 24, 128), vmem(2, 2, 2, 16, 128), vmem(4, 8, 128), vmem(2, 6, 24, 128),
        vmem(12, 64, 128), vmem(8, 32, 128), vmem(2, 5, 8, 128), vmem(6, 64, 128),
        vmem(3, 4, 10, 8, 128), vmem(3, 4, 10, 8, 128), vmem(3, 4, 10, 8, 128),
        vmem(9, 3, 8, 128), vmem(2, 64, 128), vmem(2, 64, 128),
        vmem(2, 3, 2, 64, 128), vmem(2, 3, 2, 64, 128), vmem(2, 3, 2, 64, 128),
        vmem(128, 128), vmem(2 * ny, 1, 128), vmem(nx, 2, 128),
        vmem(2 * ny, 1, 128), vmem(nx, 2, 128), vmem(*block), vmem(*block), vmem(176, 128), vmem(*block), vmem(*block),
        pltpu.SMEM(load_nodes.shape, jnp.int32), pltpu.SMEM((CASES, 3, LOADS), f32),
        pltpu.SemaphoreType.DMA((6,)), pltpu.SemaphoreType.DMA((2,)), pltpu.SemaphoreType.DMA((14,)), pltpu.SemaphoreType.DMA((29,)),
        pltpu.SemaphoreType.REGULAR((14,)),
    ]
    out = jax.ShapeDtypeStruct(block, f32)
    change, shifted = pl.pallas_call(
        functools.partial(kernel, nx, ny),
        out_shape=(out, out),
        in_specs=[spec] * 6,
        out_specs=(spec, spec),
        scratch_shapes=scratch,
        compiler_params=pltpu.CompilerParams(collective_id=0, has_side_effects=True),
    )(load_nodes, jnp.transpose(load_values, (0, 2, 1)), start, body_load, design, supports)

    return start + change, shifted - start


def solution(mesh):
    in_specs = (
        P(("grp", "gx"), "gy", "gz"),
        P(("grp", "gx"), "gy", "gz"),
        P("grp", None, "gx", "gy", "gz"),
        P("grp", None, "gx", "gy", "gz"),
        P("grp", None),
        P("grp", None, None),
    )
    out_specs = (P("grp", None, "gx", "gy", "gz"), P("grp", None, "gx", "gy", "gz"))
    return jax.shard_map(shards, mesh=mesh, in_specs=in_specs, out_specs=out_specs, check_vma=False)
```

```python
import functools

import jax
import jax.numpy as jnp
from jax import lax
from jax.experimental import pallas as pl
from jax.experimental.pallas import tpu as pltpu
from jax.sharding import PartitionSpec as P

LEVELS = 16
CASES = 6
LOADS = 16
HALF = 3
soft_modulus = 0.05
poisson_ratio = 0.3
LAM = poisson_ratio / ((1.0 + poisson_ratio) * (1.0 - 2.0 * poisson_ratio))
MU = 1.0 / (2.0 * (1.0 + poisson_ratio))
C11 = LAM + 2.0 * MU
RHO = LAM / MU
KAP = C11 / MU + 1.0
K00 = (C11 + 2.0 * MU) / 9.0
MESH = pl.DeviceIdType.MESH
f32 = jnp.float32


def masks():
    lane = lax.broadcasted_iota(jnp.int32, (8, 128), 1)
    sub = lax.broadcasted_iota(jnp.int32, (8, 128), 0)
    return lane, sub


def z_up(v, lane, sub):
    nd = v.ndim
    sh = pltpu.roll(v, 127, axis=nd - 1)
    fx = pltpu.roll(sh, 4, axis=nd - 2)
    return jnp.where(lane == 127, jnp.where(sub < 4, fx, 0.0), sh)


def z_dn(v, lane, sub):
    nd = v.ndim
    sh = pltpu.roll(v, 1, axis=nd - 1)
    fx = pltpu.roll(sh, 4, axis=nd - 2)
    return jnp.where(lane == 0, jnp.where(sub >= 4, fx, 0.0), sh)


def modal(a, em):
    X, Y, Z = 0, 1, 2
    g = {}
    tr = RHO * (a[X, 1, 0, 0] + a[Y, 0, 1, 0] + a[Z, 0, 0, 1])
    for key in ((X, 1, 0, 0), (Y, 0, 1, 0), (Z, 0, 0, 1)):
        g[key] = em * (a[key] + a[key] + tr)
    for p, q in (
        ((X, 0, 1, 0), (Y, 1, 0, 0)),
        ((X, 0, 0, 1), (Z, 1, 0, 0)),
        ((Y, 0, 0, 1), (Z, 0, 1, 0)),
    ):
        g[p] = g[q] = em * (a[p] + a[q])
    e2 = em * (1.0 / 3.0)
    ek = em * (KAP / 3.0)
    er = em * (RHO / 3.0)
    for p, q in (
        ((X, 1, 1, 0), (Z, 0, 1, 1)),
        ((X, 1, 0, 1), (Y, 0, 1, 1)),
        ((Y, 1, 1, 0), (Z, 1, 0, 1)),
    ):
        g[p] = ek * a[p] + er * a[q]
        g[q] = ek * a[q] + er * a[p]
    three = ((X, 0, 1, 1), (Y, 1, 0, 1), (Z, 1, 1, 0))
    total = a[three[0]] + a[three[1]] + a[three[2]]
    for key in three:
        g[key] = e2 * (a[key] + total)
    e3 = em * ((C11 / MU + 2.0) / 9.0)
    for c in range(3):
        g[c, 1, 1, 1] = e3 * a[c, 1, 1, 1]
    return g


class Stiffness:
    def __init__(self, planes, em_at, emit, lane, sub):
        self.planes, self.em_at, self.emit, self.lane, self.sub = planes, em_at, emit, lane, sub
        self.nodes, self.fields_, self.middles, self.elements = {}, {}, {}, {}

    def node(self, r, which):
        if (r, which) not in self.nodes:
            zs = []
            for c in range(3):
                v = self.planes(c, r, which)
                w = z_up(v, self.lane, self.sub)
                zs.append((v + w, w - v))
            self.nodes[r, which] = zs
        return self.nodes[r, which]

    def fields(self, j, which):
        if (j, which) not in self.fields_:
            low_row, high_row = self.node(j, which), self.node(j + 1, which)
            f = {}
            for c in range(3):
                for z in (0, 1):
                    lo, hi = low_row[c][z], high_row[c][z]
                    f[c, 0, z], f[c, 1, z] = lo + hi, hi - lo
            self.fields_[j, which] = f
        return self.fields_[j, which]

    def middle(self, j):
        if j not in self.middles:
            a = {}
            for (c, y, z), f in self.fields(j, "own").items():
                a[c, 1, y, z] = f[1] - f[0]
                if y or z:
                    a[c, 0, y, z] = f[0] + f[1]
            g = modal(a, self.em_at(j, 1))
            parts = {}
            for c, y, z in self.fields(j, "own"):
                gd = g[c, 1, y, z]
                if y or z:
                    gs = g[c, 0, y, z]
                    parts[c, y, z] = gs - gd, gs + gd
                else:
                    parts[c, y, z] = -gd, gd
            self.middles[j] = parts
        return self.middles[j]

    def begin(self):
        for j in range(1, 8):
            self.middle(j)

    def element(self, j):
        if j not in self.elements:
            own, outer, parts = self.fields(j, "own"), self.fields(j, "outer"), self.middle(j)
            a = {}
            for c, y, z in own:
                fo, fh = own[c, y, z], outer[c, y, z]
                a[c, 1, y, z] = jnp.stack([fo[0] - fh[0], fh[1] - fo[1]])
                if y or z:
                    a[c, 0, y, z] = fo + fh
            g = modal(a, self.em_at(j, 0, 2))
            h = {}
            for c, y, z in own:
                p1, p2 = parts[c, y, z]
                gd = g[c, 1, y, z]
                if y or z:
                    gs = g[c, 0, y, z]
                    p1, p2 = p1 + gs[0], p2 + gs[1]
                h[c, y, z] = jnp.stack([p1 + gd[0], p2 - gd[1]])
            lows = [[h[c, 0, z] - h[c, 1, z] for z in (0, 1)] for c in range(3)]
            highs = [[h[c, 0, z] + h[c, 1, z] for z in (0, 1)] for c in range(3)]
            self.elements[j] = lows, highs
        return self.elements[j]

    def rows(self, *ys):
        for y in ys:
            highs, lows = self.element(y)[1], self.element(y + 1)[0]
            out = []
            for c in range(3):
                ks = highs[c][0] + lows[c][0]
                kd = highs[c][1] + lows[c][1]
                out.append((ks - kd) + z_dn(ks + kd, self.lane, self.sub))
            self.emit(y, out)


def cyc1(v, sub):
    return jnp.where(sub % 4 == 2, pltpu.roll(v, 2, axis=v.ndim - 2), pltpu.roll(v, 7, axis=v.ndim - 2))


def cyc2(v, sub):
    return jnp.where(sub % 4 == 0, pltpu.roll(v, 6, axis=v.ndim - 2), pltpu.roll(v, 1, axis=v.ndim - 2))


def pair_products(own_x, other_x, own_y, sub):
    return [
        own_x * own_y,
        cyc1(own_x, sub) * own_y,
        other_x * own_y,
        cyc1(other_x, sub) * own_y,
        cyc2(other_x, sub) * own_y,
    ]


def cholesky(m, n):
    low = {}
    inv = {}
    for j in range(n):
        s = m[j, j]
        for k in range(j):
            s = s - low[j, k] * low[j, k]
        inv[j] = lax.rsqrt(s)
        for i in range(j + 1, n):
            t = m[i, j]
            for k in range(j):
                t = t - low[i, k] * low[j, k]
            low[i, j] = t * inv[j]
    return low, inv


def forward(low, inv, rhs, n):
    out = []
    for i in range(n):
        t = rhs[i]
        for k in range(i):
            t = t - low[i, k] * out[k]
        out.append(t * inv[i])
    return out


def backward(low, inv, rhs, n):
    out = [None] * n
    for i in reversed(range(n)):
        t = rhs[i]
        for k in range(i + 1, n):
            t = t - low[k, i] * out[k]
        out[i] = t * inv[i]
    return out


def kernel(
    nx, ny,
    n_hbm, v_hbm, x_hbm, b_hbm, d_hbm, s_hbm,
    xo_hbm, ro_hbm,
    xin, bin_, din, sin, xm, ysend, esend, qs,
    nat, yrow, enat, qnat,
    u0, u1, u2, em, mob, scl, rb, ib, yb, ga, ag, bg, ag2, bg2, vout, wout, dummy, xout, rout, nodes, vals,
    in_sem, out_sem, ss, rs, heard,
):
    grp, gx, gy, gz = (lax.axis_index(a) for a in ("grp", "gx", "gy", "gz"))
    oz = 1 - gz
    lane, sub = masks()
    valid = sub % 4 < 3
    scope = [None]

    def mark(name):
        if scope[0] is not None:
            scope[0].__exit__(None, None, None)
        scope[0] = None
        if name is not None:
            scope[0] = jax.named_scope(name)
            scope[0].__enter__()

    mark('entry')

    loads = [
        pltpu.make_async_copy(src, dst, in_sem.at[i])
        for i, (src, dst) in enumerate(((d_hbm, din), (s_hbm, sin), (x_hbm, xin), (b_hbm, bin_), (n_hbm, nodes), (v_hbm, vals)))
    ]
    for load in loads:
        load.start()

    barrier = pltpu.get_barrier_semaphore()

    def greet(cx, cy, cz):
        pl.semaphore_signal(barrier, inc=1, device_id=(grp, cx, cy, cz), device_id_type=MESH)

    exists = {}
    for dx in (-1, 0, 1):
        for dy in (-1, 0, 1):
            conds = []
            if dx:
                conds.append(gx > 0 if dx < 0 else gx < nx - 1)
            if dy:
                conds.append(gy > 0 if dy < 0 else gy < ny - 1)
            if conds:
                exists[dx, dy] = functools.reduce(jnp.logical_and, conds)

    def greet_if(here, targets):
        @pl.when(here)
        def _():
            for target in targets:
                greet(*target)

    bottom = gx == 0
    expected = bottom.astype(jnp.int32)
    for dy in (-1, 0, 1):
        greet_if(exists[1, dy], [(gx + 1, gy + dy, core) for core in (0, 1)])
        expected = expected + 2 * exists[-1, dy].astype(jnp.int32)
        if dy:
            here = jnp.logical_and(bottom, exists[0, dy])
            greet_if(here, [(gx, gy + dy, core) for core in (0, 1)])
            expected = expected + 2 * here.astype(jnp.int32)
        else:
            greet_if(bottom, [(gx, gy, oz)])

    def signal(index, cx, cy, cz):
        pl.semaphore_signal(heard.at[index], inc=1, device_id=(grp, cx, cy, cz), device_id_type=MESH)

    def signal_if(here, index, cx, cy, cz):
        pl.when(here)(lambda: signal(index, cx, cy, cz))

    def count_of(*conds):
        return sum(c.astype(jnp.int32) for c in conds)

    def wait_heard(index, each, *conds):
        @pl.when(functools.reduce(jnp.logical_or, conds))
        def _():
            pl.semaphore_wait(heard.at[index], each * count_of(*conds))

    def tell_y(k):
        step = 2**k
        if step < ny:
            signal_if(gy + step < ny, 1 + k, gx, gy + step, gz)
            signal_if(gy >= step, 1 + k, gx, gy - step, gz)

    def hear_y(k):
        step = 2**k
        if step < ny:
            wait_heard(1 + k, 1, gy + step < ny, gy >= step)

    def tell_x(k):
        step = 2**k
        if step < nx:
            signal_if(gx + step < nx, 4 + k, gx + step, gy, gz)
            signal_if(gx >= step, 8 + k, gx - step, gy, gz)

    def hear_x(k, below=True, above=True):
        step = 2**k
        if step < nx:
            if below:
                wait_heard(4 + k, 1, gx >= step)
            if above:
                wait_heard(8 + k, 1, gx + step < nx)

    def clear(ref, *index):
        ref[index] = jnp.zeros(ref[index].shape, f32)

    full = slice(None)

    @pl.when(gx == 0)
    def _():
        clear(nat, pl.ds(0, 3))
        clear(enat, full, 0)
        for side in (0, 4):
            clear(yrow, side)
        for u in (u1, u2):
            clear(u, full, 0)

    @pl.when(gx == nx - 1)
    def _():
        clear(nat, pl.ds(9, 3))
        for side in (0, 4):
            clear(yrow, side + 3)
        for u in (u1, u2):
            clear(u, full, 3)

    @pl.when(gy == 0)
    def _():
        clear(yrow, pl.ds(0, 4))
        for u in (u1, u2):
            clear(u, full, full, 0)

    @pl.when(gy == ny - 1)
    def _():
        clear(yrow, pl.ds(4, 4))
        for u in (u1, u2):
            clear(u, full, full, 9)

    mark('barrier')
    pl.semaphore_wait(barrier, expected)
    for dy in (0, -1, 1):

        @pl.when(exists[-1, dy])
        def _(dy=dy):
            for core in (0, 1):
                signal(13 if dy else 0, gx - 1, gy + dy, core)

    mark('prep')
    loads[0].wait()
    loads[1].wait()
    mnat = []
    for p in range(2):
        density = (din[p].astype(f32) + 1.0) * (1.0 / LEVELS)
        modulus = soft_modulus + (1.0 - soft_modulus) * density * density * density
        movable = 1.0 - sin[p].astype(f32)
        esend[p] = modulus
        esend[2 + p] = movable
        enat[gz, 1 + p] = modulus
        enat[gz, 3 + p] = movable
        mnat.append(movable)
    loads[2].wait()
    for side in range(2):
        for core in range(2):
            for p in range(2):
                ysend[side, core, p, 8:16] = jnp.zeros((8, 128), f32)
                if side == 1:
                    ysend[side, core, p, 12:13] = esend[p, 7:8]
    for case in range(CASES):
        core, k = divmod(case, HALF)
        for comp in range(3):
            for p in range(2):
                t = mnat[p] * xin[case, comp, p]
                xm[core, p * 3 + comp, 8 * k:8 * k + 8] = t
                for side, y in ((0, 0), (1, 7)):
                    ysend[side, core, p, 4 * k + comp:4 * k + comp + 1] = t[y:y + 1]

    mark('send1')

    def view(ref, *index):
        return ref, index

    def descriptor(src, dst, send_index, recv_index, device):
        (a, i), (b, j) = src, dst
        return pltpu.make_async_remote_copy(
            src_ref=a.at[i] if i else a, dst_ref=b.at[j] if j else b,
            send_sem=ss.at[send_index], recv_sem=rs.at[recv_index],
            device_id=device, device_id_type=MESH,
        )

    def guarded_by(cond, go):
        if cond is None:
            go()
        else:
            pl.when(cond)(go)

    def exchange(cond, send_index, recv_index, items):
        def go():
            for src, dst, device in items:
                descriptor(src, dst, send_index, recv_index, device).start()

        guarded_by(cond, go)

    def wait_in(cond, index, ref):
        guarded_by(cond, lambda: descriptor(ref, ref, 0, index, partner).wait_recv())

    def wait_out(cond, index, ref):
        guarded_by(cond, lambda: descriptor(ref, ref, index, 0, partner).wait_send())

    def rows_of(count):
        return view(dummy, pl.ds(0, count))

    slot = {key: i for i, key in enumerate(exists)}
    partner = (grp, gx, gy, oz)

    half_rows = pl.ds(pl.multiple_of(32 * gz, 8), 24)
    half_16 = pl.ds(pl.multiple_of(16 * gz, 8), 16)
    other_rows = pl.ds(pl.multiple_of(32 * oz, 8), 24)
    bytes1 = {}

    def send_start(key):
        dx, dy = key
        items, count = [], 0
        p, there_p = (1, 0) if dx > 0 else (0, 3)
        side, there = (1, 0) if dy > 0 else (0, 1)
        for core in (0, 1):
            device = (grp, gx + dx, gy + dy, core)
            if dy == 0:
                items.append((view(xm, core, pl.ds(3 * p, 3)), view(nat, pl.ds(3 * there_p, 3), half_rows), device))
                count += 72
                if dx > 0:
                    items.append((view(esend, pl.ds(1, 1)), view(enat, gz, pl.ds(0, 1)), device))
                    count += 8
            elif dx == 0:
                items.append((view(ysend, side, core), view(yrow, pl.ds(4 * there + 1, 2), half_16), device))
                count += 32
            else:
                items.append((view(ysend, side, core, p), view(yrow, 4 * there + there_p, half_16), device))
                count += 16
        exchange(exists[key], slot[key], slot[key], items)
        bytes1[key] = count

    order = sorted(exists, key=lambda k: (k[1] == 0, -abs(k[0])))
    for key in order:
        if key[0] < 0:
            send_start(key)
    mark('points')
    for load in loads[3:]:
        load.wait()
    across_z = 128 * 2
    across_y = 8 * ny * across_z
    number = (gy * 8 + sub) * across_z + gz * 128 + lane + (gx * 2) * across_y
    numbers = (number, number + across_y)

    def add_points(l, acc):
        acc = list(acc)
        for case in range(CASES):
            node = nodes[case, l]
            for p in range(2):
                hit = numbers[p] == node
                for comp in range(3):
                    at = (case * 2 + p) * 3 + comp
                    acc[at] = acc[at] + jnp.where(hit, vals[case, comp, l], 0.0)
        return tuple(acc)

    zero = jnp.zeros((8, 128), f32)
    points = lax.fori_loop(0, LOADS, add_points, (zero,) * (CASES * 6))
    for case in range(CASES):
        core, k = divmod(case, HALF)
        for p in range(2):
            m = mnat[p]
            for comp in range(3):
                total = bin_[case, comp, p] + points[(case * 2 + p) * 3 + comp]
                qs[core, p * 3 + comp, 8 * k:8 * k + 8] = m * total - (1.0 - m) * xin[case, comp, p]
    for k in range(6):
        nat[3 + k, half_rows] = xm[gz, k]
        qnat[k, half_rows] = qs[gz, k]

    mark('above')
    wait_heard(0, 2, exists[1, 0])
    send_start((1, 0))
    wait_heard(13, 2, exists[1, -1], exists[1, 1])
    signal_if(gx < nx - 1, 12, gx + 1, gy, gz)
    send_start((1, -1))
    send_start((1, 1))
    wait_heard(12, 1, gx > 0)
    for key in order:
        if key[0] == 0:
            send_start(key)
    exchange(None, 8, 16, [
        (view(xm, oz), view(nat, pl.ds(3, 6), half_rows), partner),
        (view(esend), view(enat, gz, pl.ds(1, 4)), partner),
    ])
    exchange(None, 9, 17, [(view(qs, oz), view(qnat, full, half_rows), partner)])
    tell_x(0)
    tell_y(0)
    mark('wait1')
    wait_in(None, 16, rows_of(176))
    low = sub < 4

    def spread(ref, k, y):
        return jnp.where(low, ref[0, k, y:y + 1], ref[1, k, y:y + 1])

    def at(y):
        return pl.ds(8 * y, 8)

    def start_tile(p, comp, r):
        if r in (0, 9):
            t = yrow[p + 4 * (r == 9), pl.ds(comp, 8, stride=4), :]
        else:
            t = nat[3 * p + comp, pl.ds(r - 1, 8, stride=8), :]
        u0[comp, p, r] = jnp.where(valid, t, 0.0)

    for j in range(1, 9):
        for e in (1, 2):
            em[j, e] = spread(enat, e, j - 1) * (MU / 16.0)
        mob[:, at(j - 1)] = jnp.stack([spread(enat, 3, j - 1), spread(enat, 4, j - 1)])
        for p in (1, 2):
            for comp in range(3):
                start_tile(p, comp, j)

    def em_at(j, *es):
        return em[j, es[0]] if len(es) == 1 else jnp.stack([em[j, e] for e in es])

    def planes_of(u):
        def planes(c, r, which):
            return u[c, 1:3, r] if which == "own" else jnp.stack([u[c, 0, r], u[c, 3, r]])

        return planes

    stiff = Stiffness(planes_of(u0), em_at, lambda y, force: first(y, force), lane, sub)
    stiff.begin()
    for (dx, dy), index in slot.items():
        wait_in(exists[-dx, -dy], index, rows_of(bytes1[dx, dy]))
    hear_x(0)
    tell_x(1)
    hear_y(0)
    tell_y(1)
    mark('build')

    for j in range(9):
        for e in range(3):
            if j == 0:
                em[j, e] = jnp.where(low, yrow[e, 12:13], yrow[e, 28:29]) * (MU / 16.0)
            elif e == 0:
                em[j, e] = spread(enat, e, j - 1) * (MU / 16.0)
    for y in range(8):
        rows = em[y] + em[y + 1]
        around = rows[0:2] + rows[1:3]
        esum = (around + z_dn(around, lane, sub)) * (16.0 / MU)
        m = mob[:, at(y)]
        guarded = jnp.where(m > 0, esum, 1.0)
        scl[:, at(y)] = m / (K00 * guarded) + (1.0 - m)
    for r in range(10):
        for p in range(4):
            if r in (0, 9) or p in (0, 3):
                for comp in range(3):
                    start_tile(p, comp, r)

    mark('waitq')
    wait_in(None, 17, view(qnat, full, other_rows))
    mark('k1')

    def halo_views(u, key, chunk):
        dx, dy = key
        src, dst = (2, 0) if dx > 0 else (1, 3)
        ysrc, ydst = (8, 0) if dy > 0 else (1, 9)
        if dy == 0:
            return [
                (view(u, full, src, pl.ds(k, m)), view(u, full, dst, pl.ds(k, m)))
                for k, m in ((1 + 3 * chunk, 3),)
            ]
        if dx == 0:
            return [(view(u, full, pl.ds(1, 2), ysrc), view(u, full, pl.ds(1, 2), ydst))]
        return [(view(u, full, src, ysrc), view(u, full, dst, ydst))]

    halo_rows = {(dx, dy): 8 * 3 * (6 if dy == 0 else 2 if dx == 0 else 1) for dx, dy in exists}

    free = sub % 4 == 3
    chunks = ((1, 2, 3, 8), (4, 5, 6, 7))

    def pack(u, chunk):
        *carriers, last = chunks[chunk]
        t = u[:, 1:3, last]
        for i, k in enumerate(carriers, 1):
            u[:, 1:3, k] = jnp.where(free, pltpu.roll(t, 4 - i, axis=2), u[:, 1:3, k])

    def unpack(u, chunk):
        *carriers, last = chunks[chunk]
        for p in (0, 3):
            a, b, c = (pltpu.roll(u[:, p, k], 4 + i, axis=1) for i, k in enumerate(carriers, 1))
            u[:, p, last] = jnp.where(sub % 4 == 0, a, jnp.where(sub % 4 == 1, b, c))

    def halo_slot(first_slot, key, chunk):
        if chunk == 0:
            return first_slot + slot[key]
        return 23 + 2 * (first_slot == 0) + (key[0] > 0)

    def send_halos(u, first_slot, chunk):
        pack(u, chunk)
        for key in order:
            dx, dy = key
            if chunk == 0 or dy == 0:
                exchange(
                    exists[key], slot[key], halo_slot(first_slot, key, chunk),
                    [(a, b, (grp, gx + dx, gy + dy, gz)) for a, b in halo_views(u, key, chunk)],
                )

    def take_halos(u, first_slot, chunk):
        for key in exists:
            dx, dy = key
            if chunk == 0 or dy == 0:
                rows = halo_rows[key] // 2 if dy == 0 else halo_rows[key]
                wait_in(exists[-dx, -dy], halo_slot(first_slot, key, chunk), rows_of(rows))
        unpack(u, chunk)

    def sent_halos(u):
        for key in exists:
            wait_out(exists[key], slot[key], rows_of(halo_rows[key]))

    def share(buf, send_index, recv_index):
        exchange(None, send_index, recv_index, [(view(buf, gz), view(buf, gz), partner)])

    def first(y, force):
        m = mob[:, at(y)]
        s = scl[:, at(y)]
        for comp in range(3):
            q = jnp.stack([qnat[3 * p + comp, pl.ds(y, 8, stride=8), :] for p in range(2)])
            res = jnp.where(valid, q, 0.0) - m * force[comp]
            rb[gz, comp, :, at(y)] = res
            u1[comp, 1:3, 1 + y] = m * (s * res)

    stiff.rows(0, 7, 1, 2)
    for key in exists:
        wait_out(exists[key], slot[key], rows_of(bytes1[key]))
    wait_out(None, 8, rows_of(176))
    send_halos(u1, 8, 0)
    stiff.rows(3, 4, 5, 6)
    send_halos(u1, 8, 1)
    share(rb, 8, 18)
    stiff = Stiffness(planes_of(u1), em_at, lambda y, force: second(y, force), lane, sub)
    stiff.begin()
    hear_x(1)
    tell_x(2)
    hear_y(1)
    tell_y(2)
    mark('wait2')
    take_halos(u1, 8, 0)
    take_halos(u1, 8, 1)
    mark('k2')

    def second(y, force):
        m = mob[:, at(y)]
        s = scl[:, at(y)]
        for comp in range(3):
            d = s * rb[gz, comp, :, at(y)]
            image = m * force[comp] + (1.0 - m) * d
            ib[gz, comp, :, at(y)] = image
            u2[comp, 1:3, 1 + y] = m * (s * image)

    stiff.rows(0, 7, 1, 2)
    sent_halos(u1)
    send_halos(u2, 0, 0)
    stiff.rows(3, 4, 5, 6)
    send_halos(u2, 0, 1)
    mark('send3')
    wait_out(None, 9, view(qs, oz))
    share(ib, 9, 19)
    wait_in(None, 18, view(rb, oz))
    wait_in(None, 19, view(ib, oz))

    mark('grams')
    def grams(make):
        acc = None
        for y in range(8):
            s = scl[:, at(y)]
            for comp in range(3):
                prods = pair_products(*make(comp, y, s), sub)
                acc = prods if acc is None else [a + b for a, b in zip(acc, prods)]
        return [a[0] + a[1] for a in acc]

    def own_other(buf, comp, y):
        return buf[gz, comp, :, at(y)], buf[oz, comp, :, at(y)]

    def make_g(comp, y, s):
        r, ro = own_other(rb, comp, y)
        return s * r, s * ro, ib[gz, comp, :, at(y)]

    def make_h(comp, y, s):
        i, io = own_other(ib, comp, y)
        return i, io, s * i

    def make_p(comp, y, s):
        r, ro = own_other(rb, comp, y)
        return r, ro, s * r

    me = gz * ny + gy

    def send_row(accs, rows_ref, send_index, recv_index):
        folded = [a + pltpu.roll(a, 4, axis=0) for a in accs]
        if len(folded) % 2:
            folded.append(folded[-1])
        for t in range(len(folded) // 2):
            ga[pl.ds(8 * t, 8), :] = jnp.where(low, folded[2 * t], folded[2 * t + 1])
        row = lax.dot_general(
            jnp.ones((8, 128), f32), ga[...], (((1,), (1,)), ((), ())),
            precision=lax.Precision.HIGHEST, preferred_element_type=f32,
        )
        rows_ref[me] = row[0:1]
        exchange(None, send_index, recv_index, [
            (view(rows_ref, me), view(rows_ref, me), (grp, gx, lax.rem(gy + d, ny), oz if flip else gz))
            for d in sorted(range(ny), key=lambda d: -min(d, ny - d)) for flip in (0, 1) if d or flip
        ])

    def sum_rows(rows_ref, recv_index, planes_ref):
        wait_in(None, recv_index, view(rows_ref, pl.ds(0, 2 * ny - 1)))
        for s in (0, 1):
            total = rows_ref[s * ny]
            for k in range(1, ny):
                total = total + rows_ref[s * ny + k]
            planes_ref[gx, s:s + 1] = total

    def send_planes(planes_ref, send_index, recv_index, first_plane, last_plane):
        def send_sum(target, carry):
            mine = view(planes_ref, gx)
            descriptor(mine, mine, send_index, recv_index, (grp, target, gy, gz)).start()
            return carry

        lax.fori_loop(first_plane, last_plane, send_sum, 0)

    def totals(planes_ref, recv_index):
        wait_in(None, recv_index, view(planes_ref, pl.ds(0, nx - 1)))
        total = planes_ref[0]
        for k in range(1, nx):
            total = total + planes_ref[k]
        return [jnp.broadcast_to(total[s:s + 1], (8, 128)) for s in (0, 1)]

    ga[...] = jnp.zeros_like(ga)
    early = grams(make_g) + grams(make_h) + grams(make_p)

    stiff = Stiffness(planes_of(u2), em_at, lambda y, force: third(y, force), lane, sub)
    stiff.begin()
    hear_x(2)
    tell_x(3)
    hear_y(2)
    send_row(early, ag2, 12, 27)
    mark('wait3')
    take_halos(u2, 0, 0)
    mark('k3')

    jacc = []

    def third(y, force):
        m = mob[:, at(y)]
        s = scl[:, at(y)]
        for comp in range(3):
            i, io = own_other(ib, comp, y)
            w = s * i
            image = m * force[comp] + (1.0 - m) * w
            yb[gz, comp, :, at(y)] = image
            prods = pair_products(w, s * io, image, sub)
            if jacc:
                jacc[0] = [a + b for a, b in zip(jacc[0], prods)]
            else:
                jacc.append(prods)

    stiff.rows(0, 1)
    take_halos(u2, 0, 1)
    stiff.rows(7, 2, 3, 4, 5, 6)
    wait_out(None, 8, view(rb, gz))
    share(yb, 8, 20)
    mark('rowsum')
    send_row([a[0] + a[1] for a in jacc[0]], ag, 10, 21)
    mark('reduce_a')
    sum_rows(ag2, 27, bg2)
    hear_x(3, above=False)
    send_planes(bg2, 13, 28, 0, gx)
    sum_rows(ag, 21, bg)
    mark('reduce_b')
    send_planes(bg, 11, 22, 0, gx)
    hear_x(3, below=False)
    send_planes(bg, 11, 22, gx + 1, nx)
    send_planes(bg2, 13, 28, gx + 1, nx)

    def entry(rows, matrix, i, j):
        ci, ki = divmod(i, HALF)
        cj, kj = divmod(j, HALF)
        if ci == cj:
            if (ki + 1) % 3 == kj:
                acc, k, s = 1, ki, ci
            elif ki == kj:
                acc, k, s = 0, ki, ci
            else:
                acc, k, s = 1, kj, ci
        else:
            if ci == 1:
                ki, kj = kj, ki
            acc, k, s = 2 + (kj - ki) % 3, ki, 0
        number = matrix * 5 + acc
        where = 8 * (number // 2) + 4 * (number % 2) + k
        return jnp.broadcast_to(rows[s][:, where:where + 1], (8, 128))

    n = CASES

    def matrix_of(rows, matrix):
        m = {}
        for i in range(n):
            for j in range(i + 1):
                m[i, j] = m[j, i] = entry(rows, matrix, i, j)
        return m

    rows = totals(bg2, 28)
    mg, mh, mp = (matrix_of(rows, matrix) for matrix in range(3))
    lo1, inv1 = cholesky(mg, n)
    zh = [forward(lo1, inv1, [mh[i, j] for i in range(n)], n) for j in range(n)]
    zp = [forward(lo1, inv1, [mp[i, j] for i in range(n)], n) for j in range(n)]
    th = [backward(lo1, inv1, zh[j], n) for j in range(n)]
    al = [backward(lo1, inv1, zp[j], n) for j in range(n)]
    right = []
    for j in range(n):
        col = []
        for i in range(n):
            t = mg[i, j]
            for k in range(n):
                t = t - zh[i][k] * zp[j][k]
            col.append(t)
        right.append(col)
    taken = {}
    for j in range(n):
        for i in range(j, n):
            t = zh[i][0] * zh[j][0]
            for k in range(1, n):
                t = t + zh[i][k] * zh[j][k]
            taken[i, j] = t

    wait_in(None, 20, view(yb, oz))
    for comp in range(3):
        for p in range(2):
            s = scl[p, pl.ds(4 * gz, 8, stride=8), :]
            fr, fi, fy = [], [], []
            for j in range(n):
                core, k = divmod(j, HALF)
                pick = pl.ds(4 * gz + k, 8, stride=8)
                fr.append(rb[core, comp, p, pick, :])
                fi.append(ib[core, comp, p, pick, :])
                fy.append(yb[core, comp, p, pick, :])
            for i in range(n):
                up, dn, v, y = fr[0] * al[i][0], fi[0] * al[i][0], fr[0] * th[i][0], fi[0] * th[i][0]
                for j in range(1, n):
                    up = up + fr[j] * al[i][j]
                    dn = dn + fi[j] * al[i][j]
                    v = v + fr[j] * th[i][j]
                    y = y + fi[j] * th[i][j]
                xout[i, comp, p] = s * up
                rout[i, comp, p] = (fr[i] - dn) + xin[i, comp, p]
                vout[i, comp, p] = s * (fi[i] - v)
                wout[i, comp, p] = fy[i] - y

    mark('solve')
    rows = totals(bg, 22)
    mj = matrix_of(rows, 0)
    schur = {key: mj[key] - t for key, t in taken.items()}
    lo2, inv2 = cholesky(schur, n)
    cb = [backward(lo2, inv2, forward(lo2, inv2, right[j], n), n) for j in range(n)]

    mark('combine')
    for comp in range(3):
        for p in range(2):
            v = [vout[j, comp, p] for j in range(n)]
            w = [wout[j, comp, p] for j in range(n)]
            for i in range(n):
                up, dn = v[0] * cb[i][0], w[0] * cb[i][0]
                for j in range(1, n):
                    up = up + v[j] * cb[i][j]
                    dn = dn + w[j] * cb[i][j]
                xout[i, comp, p] = xout[i, comp, p] + up
                rout[i, comp, p] = rout[i, comp, p] - dn
        for i, (src, dst) in enumerate(((xout, xo_hbm), (rout, ro_hbm))):
            pltpu.make_async_copy(src.at[:, comp], dst.at[:, comp], out_sem.at[i]).start()
    mark('drain')
    sent_halos(u2)
    wait_out(None, 8, view(yb, gz))
    wait_out(None, 9, view(ib, gz))
    wait_out(None, 10, view(ag, pl.ds(0, 2 * ny - 1)))
    wait_out(None, 11, view(bg, pl.ds(0, nx - 1)))
    wait_out(None, 12, view(ag2, pl.ds(0, 2 * ny - 1)))
    wait_out(None, 13, view(bg2, pl.ds(0, nx - 1)))
    for i, (src, dst) in enumerate(((xout, xo_hbm), (rout, ro_hbm))):
        pltpu.make_async_copy(src, dst, out_sem.at[i]).wait()
    mark(None)


def shards(design, supports, body_load, start, load_nodes, load_values):
    nx, ny = lax.axis_size("gx"), lax.axis_size("gy")
    block = body_load.shape
    vmem = lambda *shape: pltpu.VMEM(shape, f32)
    spec = pl.BlockSpec(memory_space=pl.ANY)
    scratch = [
        vmem(*block), vmem(*block), pltpu.VMEM(design.shape, jnp.int32), pltpu.VMEM(design.shape, jnp.int32),
        vmem(2, 6, 24, 128), vmem(2, 2, 2, 16, 128), vmem(4, 8, 128), vmem(2, 6, 24, 128),
        vmem(12, 64, 128), vmem(8, 32, 128), vmem(2, 5, 8, 128), vmem(6, 64, 128),
        vmem(3, 4, 10, 8, 128), vmem(3, 4, 10, 8, 128), vmem(3, 4, 10, 8, 128),
        vmem(9, 3, 8, 128), vmem(2, 64, 128), vmem(2, 64, 128),
        vmem(2, 3, 2, 64, 128), vmem(2, 3, 2, 64, 128), vmem(2, 3, 2, 64, 128),
        vmem(128, 128), vmem(2 * ny, 1, 128), vmem(nx, 2, 128),
        vmem(2 * ny, 1, 128), vmem(nx, 2, 128), vmem(*block), vmem(*block), vmem(176, 128), vmem(*block), vmem(*block),
        pltpu.SMEM(load_nodes.shape, jnp.int32), pltpu.SMEM((CASES, 3, LOADS), f32),
        pltpu.SemaphoreType.DMA((6,)), pltpu.SemaphoreType.DMA((2,)), pltpu.SemaphoreType.DMA((14,)), pltpu.SemaphoreType.DMA((29,)),
        pltpu.SemaphoreType.REGULAR((14,)),
    ]
    out = jax.ShapeDtypeStruct(block, f32)
    change, shifted = pl.pallas_call(
        functools.partial(kernel, nx, ny),
        out_shape=(out, out),
        in_specs=[spec] * 6,
        out_specs=(spec, spec),
        scratch_shapes=scratch,
        compiler_params=pltpu.CompilerParams(collective_id=0, has_side_effects=True),
    )(load_nodes, jnp.transpose(load_values, (0, 2, 1)), start, body_load, design, supports)

    return start + change, shifted - start


def solution(mesh):
    in_specs = (
        P(("grp", "gx"), "gy", "gz"),
        P(("grp", "gx"), "gy", "gz"),
        P("grp", None, "gx", "gy", "gz"),
        P("grp", None, "gx", "gy", "gz"),
        P("grp", None),
        P("grp", None, None),
    )
    out_specs = (P("grp", None, "gx", "gy", "gz"), P("grp", None, "gx", "gy", "gz"))
    return jax.shard_map(shards, mesh=mesh, in_specs=in_specs, out_specs=out_specs, check_vma=False)
```
